8 devices in a mesh: dp: 1 (over z), tp: 8 (over y, x, core).
Axes of the slice: x: 2, y: 2, z: 1, core: 2. Of those that a mesh axis runs over, the one named last changes fastest.
Arguments:
- tokens: int32 [512, 5], P('dp')
- start_pos: int32 [512], P('dp')
- kv_cache: bfloat16 [2, 2, 512, 128, 8, 64], P(None, None, 'dp', None, 'tp')
- expert_ids: int32 [4, 2, 512, 8], P(None, None, 'dp')
- embed: bfloat16 [49152, 1536], P('tp')
- norm_gain: float32 [5, 1536], replicated
- w_query: bfloat16 [2, 1536, 1536], P(None, None, 'tp')
- w_key: bfloat16 [2, 1536, 512], P(None, None, 'tp')
- w_value: bfloat16 [2, 1536, 512], P(None, None, 'tp')
- w_out: bfloat16 [2, 1536, 1536], P(None, 'tp')
- w_router: bfloat16 [2, 1536, 40], replicated
- w_gate: bfloat16 [2, 40, 1536, 512], P(None, 'tp')
- w_up: bfloat16 [2, 40, 1536, 512], P(None, 'tp')
- w_down: bfloat16 [2, 40, 512, 1536], P(None, 'tp')
Outputs:
- output 1: float32 [512, 4], P('dp')
- output 2: float32 [512, 49152], P('dp', 'tp')
- output 3: bfloat16 [2, 2, 512, 128, 8, 64], P(None, None, 'dp', None, 'tp')
All inputs are finite; a program needn't handle non-finite values.
Results may differ from the reference program's by a relative error of at most 0.0112274.
Values are sent between devices in bfloat16 or wider.
A program may use at most 1 GiB of HBM per device.

```python
import jax
import jax.numpy as jnp
from jax import lax

D = 1536
HEADS = 24
KV_HEADS = 8
HEAD = 64
EXPERTS = 40
TOP = 8
FF = 512
VOCAB_ROWS = 49152
BATCH = 512
CACHE_LEN = 128
LAYERS = 2
STEPS = 4
SHARDS = 8

EMBED_MULT = 12.0
ATT_SCALE = 0.015625
RESID_MULT = 0.22
LOGIT_DIV = 6.0
NORM_EPS = 1e-6
ROPE_THETA = 10000.0
Q_GAIN = 3.0 / (HEAD ** 0.5 * ATT_SCALE)
HOT_EXPERTS = EXPERTS // 4


def draw_routing(route_key):
    key_list = jax.random.split(route_key, 4)
    shard_width = VOCAB_ROWS // SHARDS
    rotation = jax.random.randint(key_list[0], (), 0, SHARDS)
    shard_of = (jnp.arange(BATCH)[:, None] + jnp.arange(STEPS + 1)[None, :] + rotation) % SHARDS
    tokens = shard_of * shard_width + jax.random.randint(key_list[1], (BATCH, STEPS + 1), 0, shard_width)
    start_pos = jax.random.randint(key_list[2], (BATCH,), CACHE_LEN // 4, CACHE_LEN - STEPS + 1)
    start_pos = start_pos.at[0].set(CACHE_LEN - STEPS).at[1].set(CACHE_LEN // 4)
    scores = jax.random.randint(key_list[3], (STEPS, LAYERS, BATCH, EXPERTS), 0, 1024)
    scores = scores + jnp.where(jnp.arange(EXPERTS) < HOT_EXPERTS, 384, 0)
    scores = scores * EXPERTS + jnp.arange(EXPERTS)
    expert_ids = lax.top_k(scores, TOP)[1]
    return tokens.astype(jnp.int32), start_pos.astype(jnp.int32), expert_ids.astype(jnp.int32)


def setup_inputs(seed: int = 0, part: int = 0) -> dict:
    own_key = jax.random.fold_in(jax.random.key(seed), part)
    key_list = jax.random.split(own_key, 2)
    tokens, start_pos, expert_ids = draw_routing(key_list[0])
    kv_cache = jax.random.normal(key_list[1], (LAYERS, 2, BATCH, CACHE_LEN, KV_HEADS, HEAD), jnp.float32)
    weight_keys = jax.random.split(jax.random.key(seed + 1), 10)
    embed = jax.random.normal(weight_keys[0], (VOCAB_ROWS, D), jnp.float32) / EMBED_MULT
    norm_gain = 1.0 + 0.3 * jax.random.normal(weight_keys[1], (2 * LAYERS + 1, D), jnp.float32)
    w_query = jax.random.normal(weight_keys[2], (LAYERS, D, HEADS * HEAD), jnp.float32) * (Q_GAIN / D ** 0.5)
    w_key = jax.random.normal(weight_keys[3], (LAYERS, D, KV_HEADS * HEAD), jnp.float32) / D ** 0.5
    w_value = jax.random.normal(weight_keys[4], (LAYERS, D, KV_HEADS * HEAD), jnp.float32) / D ** 0.5
    w_out = jax.random.normal(weight_keys[5], (LAYERS, HEADS * HEAD, D), jnp.float32) * (1.5 / (HEADS * HEAD) ** 0.5)
    w_router = jax.random.normal(weight_keys[6], (LAYERS, D, EXPERTS), jnp.float32) / D ** 0.5
    w_gate = jax.random.normal(weight_keys[7], (LAYERS, EXPERTS, D, FF), jnp.float32) / D ** 0.5
    w_up = jax.random.normal(weight_keys[8], (LAYERS, EXPERTS, D, FF), jnp.float32) / D ** 0.5
    w_down = jax.random.normal(weight_keys[9], (LAYERS, EXPERTS, FF, D), jnp.float32) * (2.0 * TOP ** 0.5 / FF ** 0.5)
    return {'tokens': tokens, 'start_pos': start_pos, 'kv_cache': kv_cache.astype(jnp.bfloat16), 'expert_ids': expert_ids, 'embed': embed.astype(jnp.bfloat16), 'norm_gain': norm_gain, 'w_query': w_query.astype(jnp.bfloat16), 'w_key': w_key.astype(jnp.bfloat16), 'w_value': w_value.astype(jnp.bfloat16), 'w_out': w_out.astype(jnp.bfloat16), 'w_router': w_router.astype(jnp.bfloat16), 'w_gate': w_gate.astype(jnp.bfloat16), 'w_up': w_up.astype(jnp.bfloat16), 'w_down': w_down.astype(jnp.bfloat16)}


def rms_norm(hidden, gain):
    mean_sq = jnp.mean(hidden * hidden, axis=-1, keepdims=True)
    return (hidden * lax.rsqrt(mean_sq + NORM_EPS) * gain).astype(jnp.bfloat16)


def rotary(values, positions):
    half_dim = HEAD // 2
    inv_freq = ROPE_THETA ** (-2.0 * jnp.arange(half_dim, dtype=jnp.float32) / HEAD)
    angles = positions.astype(jnp.float32)[:, None, None] * inv_freq
    cos_part = jnp.cos(angles)
    sin_part = jnp.sin(angles)
    first_half = values[..., :half_dim]
    second_half = values[..., half_dim:]
    return jnp.concatenate([first_half * cos_part - second_half * sin_part, second_half * cos_part + first_half * sin_part], axis=-1)


def attend(query, cache_keys, cache_vals, fresh_keys, fresh_vals, old_mask):
    query_wide = query.astype(jnp.float32)
    old_scores = jnp.einsum('bkgh,bskh->bkgs', query_wide, cache_keys.astype(jnp.float32)) * ATT_SCALE
    old_scores = jnp.where(old_mask[:, None, None, :], old_scores, -jnp.inf)
    new_scores = jnp.einsum('bkgh,jbkh->bkgj', query_wide, fresh_keys.astype(jnp.float32)) * ATT_SCALE
    peak = jnp.maximum(jnp.max(old_scores, axis=-1, keepdims=True), jnp.max(new_scores, axis=-1, keepdims=True))
    old_weights = jnp.exp(old_scores - peak)
    new_weights = jnp.exp(new_scores - peak)
    total = jnp.sum(old_weights, axis=-1, keepdims=True) + jnp.sum(new_weights, axis=-1, keepdims=True)
    old_probs = (old_weights / total).astype(jnp.bfloat16)
    new_probs = (new_weights / total).astype(jnp.bfloat16)
    mixed = jnp.einsum('bkgs,bskh->bkgh', old_probs.astype(jnp.float32), cache_vals.astype(jnp.float32)) + jnp.einsum('bkgj,jbkh->bkgh', new_probs.astype(jnp.float32), fresh_vals.astype(jnp.float32))
    return mixed.astype(jnp.bfloat16).reshape(mixed.shape[0], -1)


def mixture(normed, router_w, gate_w, up_w, down_w, chosen_ids):
    router = jnp.dot(normed, router_w, preferred_element_type=jnp.float32)
    chosen = jnp.any(chosen_ids[:, :, None] == jnp.arange(EXPERTS)[None, None, :], axis=1)
    masked = jnp.where(chosen, router, -jnp.inf)
    weights = jnp.exp(masked - jnp.max(masked, axis=-1, keepdims=True))
    gates = weights / jnp.sum(weights, axis=-1, keepdims=True)
    normed_wide = normed.astype(jnp.float32)
    gate_act = jnp.einsum('bd,edf->ebf', normed_wide, gate_w.astype(jnp.float32))
    up_act = jnp.einsum('bd,edf->ebf', normed_wide, up_w.astype(jnp.float32))
    gated_hidden = (jax.nn.silu(gate_act) * up_act * gates.T[:, :, None]).astype(jnp.bfloat16)
    expert_sum = jnp.einsum('ebf,efd->bd', gated_hidden.astype(jnp.float32), down_w.astype(jnp.float32))
    return expert_sum.astype(jnp.bfloat16)


def reference(tokens, start_pos, kv_cache, expert_ids, embed, norm_gain, w_query, w_key, w_value, w_out, w_router, w_gate, w_up, w_down):
    groups = HEADS // KV_HEADS
    positions = jnp.arange(CACHE_LEN)
    old_mask = positions[None, :] < start_pos[:, None]
    fresh_keys = [[] for index in range(LAYERS)]
    fresh_vals = [[] for index in range(LAYERS)]
    log_list = []
    logits = None
    for step in range(STEPS):
        hidden = EMBED_MULT * embed[tokens[:, step]].astype(jnp.float32)
        rot_pos = start_pos + step
        for layer in range(LAYERS):
            normed = rms_norm(hidden, norm_gain[2 * layer])
            query = rotary(jnp.dot(normed, w_query[layer], preferred_element_type=jnp.float32).reshape(BATCH, HEADS, HEAD), rot_pos)
            key_new = rotary(jnp.dot(normed, w_key[layer], preferred_element_type=jnp.float32).reshape(BATCH, KV_HEADS, HEAD), rot_pos)
            val_new = jnp.dot(normed, w_value[layer], preferred_element_type=jnp.float32).reshape(BATCH, KV_HEADS, HEAD)
            fresh_keys[layer].append(key_new.astype(jnp.bfloat16))
            fresh_vals[layer].append(val_new.astype(jnp.bfloat16))
            mixed = attend(query.astype(jnp.bfloat16).reshape(BATCH, KV_HEADS, groups, HEAD), kv_cache[layer, 0], kv_cache[layer, 1], jnp.stack(fresh_keys[layer]), jnp.stack(fresh_vals[layer]), old_mask)
            attn_out = jnp.dot(mixed, w_out[layer], preferred_element_type=jnp.float32).astype(jnp.bfloat16)
            hidden = hidden + RESID_MULT * attn_out.astype(jnp.float32)
            normed = rms_norm(hidden, norm_gain[2 * layer + 1])
            moe_out = mixture(normed, w_router[layer], w_gate[layer], w_up[layer], w_down[layer], expert_ids[step, layer])
            hidden = hidden + RESID_MULT * moe_out.astype(jnp.float32)
        final_norm = rms_norm(hidden, norm_gain[2 * LAYERS])
        logits = jnp.dot(final_norm, embed.T, preferred_element_type=jnp.float32) / LOGIT_DIV
        peak = jnp.max(logits, axis=-1, keepdims=True)
        log_norm = peak[:, 0] + jnp.log(jnp.sum(jnp.exp(logits - peak), axis=-1))
        picked = jnp.take_along_axis(logits, tokens[:, step + 1][:, None], axis=1)[:, 0]
        log_list.append(picked - log_norm)
    offset = positions[None, :] - start_pos[:, None]
    new_cache = kv_cache
    for step in range(STEPS):
        entry = jnp.stack([jnp.stack([fresh_keys[layer][step], fresh_vals[layer][step]]) for layer in range(LAYERS)])
        new_cache = jnp.where((offset == step)[None, None, :, :, None, None], entry[:, :, :, None], new_cache)
    return jnp.stack(log_list, axis=1), logits, new_cache
```

```python
import functools

import jax
import jax.numpy as jnp
from jax import lax
from jax.experimental import pallas as pl
from jax.experimental.pallas import tpu as pltpu
from jax.sharding import PartitionSpec as P

EMBED_MULT = 12.0
ATT_SCALE = 0.015625
RESID_MULT = 0.22
LOGIT_DIV = 6.0
NORM_EPS = 1e-6
ROPE_THETA = 10000.0

D = 1536
HEAD = 64
BATCH = 512
STEPS = 4
LAYERS = 2
CACHE = 128
EXPERTS = 40
LOCAL_EXPERTS = 5
FF = 512
VOCAB = 6144
N = 8
SEQS = BATCH // N
ROWS = SEQS * STEPS
MESH = pl.DeviceIdType.MESH
F32 = jnp.float32
BF16 = jnp.bfloat16
VMEM_LIMIT = 60 * 1024 * 1024

ORDER_RS = ("me", "sib", "bs", "a", "ds", "dg", "as", "b")
ORDER_AG = ("me", "sib", "bs", "a", "as", "b", "ds", "dg")


def places():
    me = lax.axis_index("tp")
    k = lax.rem(me, 2)
    x = lax.rem(lax.div(me, 2), 2)
    y = lax.div(me, 4)
    step_x = 2 - 4 * x
    step_y = 4 - 8 * y
    a = me + step_x + k * (step_y - step_x)
    b = me + step_y + k * (step_x - step_y)
    dg = me + step_x + step_y
    s = 1 - 2 * k
    return {"me": me, "sib": me + s, "a": a, "as": a + s, "b": b, "bs": b + s, "dg": dg, "ds": dg + s}


def entry_barrier(at):
    barrier = pltpu.get_barrier_semaphore()
    for name in ("sib", "a", "b"):
        pl.semaphore_signal(barrier, inc=1, device_id={"tp": at[name]}, device_id_type=MESH)
    pl.semaphore_wait(barrier, 3)


def pick(pos, order, at):
    total = jnp.int32(0)
    for i, name in enumerate(order):
        total = total + jnp.where(pos == i, at[name], 0)
    return total


class Gather:
    def __init__(self, at, own, ubuf, send, recv):
        self.at, self.own, self.ubuf, self.send, self.recv = at, own, ubuf, send, recv

    def copy(self, src, origin, target, slot):
        return pltpu.make_async_remote_copy(
            src_ref=src, dst_ref=self.ubuf.at[origin], send_sem=self.send.at[slot], recv_sem=self.recv.at[origin],
            device_id={"tp": target}, device_id_type=MESH)

    def item(self, slot):
        at = self.at
        if slot < 3:
            return self.copy(self.own, at["me"], at[("a", "b", "sib")[slot]], slot)
        name, target = (("a", "b"), ("a", "sib"), ("b", "sib"), ("dg", "sib"))[slot - 3]
        return self.copy(self.ubuf.at[at[name]], at[name], at[target], slot)

    def start(self, *slots):
        for slot in slots:
            self.item(slot).start()

    def arrive(self, name):
        origin = self.at[name]
        self.copy(self.own, origin, self.at["sib"], 0).wait_recv()

    def before(self, pos, rs):
        @pl.when(pos == 1)
        def _():
            self.start(1)
            self.arrive("sib")

        @pl.when(pos == 2)
        def _():
            self.arrive("a")
            self.start(3, 4)
            self.arrive("bs")

        @pl.when(pos == 4)
        def _():
            self.arrive("b")
            self.start(5)
            if rs:
                self.arrive("dg")
                self.start(6)
                self.arrive("ds")
            else:
                self.arrive("as")

        @pl.when(pos == 6)
        def _():
            if rs:
                self.arrive("as")
            else:
                self.arrive("dg")
                self.start(6)
                self.arrive("ds")

    def finish(self):
        for slot in range(7):
            self.item(slot).wait_send()


class Scatter:
    def __init__(self, at, tbuf, rbuf, send, recv):
        self.at, self.tbuf, self.rbuf, self.send, self.recv = at, tbuf, rbuf, send, recv

    def copy(self, slot, target):
        return pltpu.make_async_remote_copy(
            src_ref=self.tbuf.at[slot], dst_ref=self.rbuf.at[slot], send_sem=self.send.at[slot],
            recv_sem=self.recv.at[slot], device_id={"tp": target}, device_id_type=MESH)

    def arrive(self, slot):
        self.copy(slot, self.at["sib"]).wait_recv()

    def after(self, pos, acc, fin):
        at = self.at

        @pl.when(pos == 0)
        def _():
            fin[...] = acc[...]

        @pl.when((pos == 1) | (pos == 2) | (pos == 4) | (pos == 6))
        def _():
            slot = lax.div(pos, 2)
            self.tbuf[slot] = acc[...].astype(BF16)
            self.copy(slot, at["sib"]).start()

        @pl.when((pos == 3) | (pos == 5))
        def _():
            slot = lax.div(pos, 2)
            out = slot + 3
            self.arrive(slot)
            self.tbuf[out] = (acc[...] + self.rbuf[slot].astype(F32)).astype(BF16)
            self.copy(out, at["a"]).start()

        @pl.when(pos == 7)
        def _():
            self.arrive(3)
            self.arrive(5)
            self.tbuf[6] = (acc[...] + self.rbuf[3].astype(F32) + self.rbuf[5].astype(F32)).astype(BF16)
            self.copy(6, at["b"]).start()

    def finish(self, fin, out_ref):
        self.arrive(0)
        self.arrive(4)
        self.arrive(6)
        total = fin[...] + self.rbuf[0].astype(F32) + self.rbuf[4].astype(F32) + self.rbuf[6].astype(F32)
        out_ref[...] = total.astype(BF16)
        for slot in range(7):
            self.copy(slot, self.at["sib"]).wait_send()


def gather_scratch():
    return [pltpu.VMEM((N, ROWS, D), BF16), pltpu.SemaphoreType.DMA((7,)), pltpu.SemaphoreType.DMA((N,))]


def scatter_scratch():
    return [pltpu.VMEM((ROWS, D), F32), pltpu.VMEM((ROWS, D), F32), pltpu.VMEM((7, ROWS, D), BF16),
            pltpu.VMEM((7, ROWS, D), BF16), pltpu.SemaphoreType.DMA((7,)), pltpu.SemaphoreType.DMA((7,))]


VM = pl.BlockSpec(memory_space=pltpu.VMEM)
ANY = pl.BlockSpec(memory_space=pl.ANY)


def comm_params(ident):
    return pltpu.CompilerParams(collective_id=ident, has_side_effects=True, vmem_limit_bytes=VMEM_LIMIT)


def rows_kernel(count_ref, token_ref, row_ref, embed_ref, out_ref, buf, wide, sem):
    wide[...] = jnp.zeros_like(wide)
    count = count_ref[0]
    slots = buf.shape[0]

    def chunk(c, carry):
        base = c * slots
        width = jnp.minimum(slots, count - base)

        def issue(j, carry):
            pltpu.make_async_copy(embed_ref.at[lax.div(row_ref[base + j], 8)], buf.at[j], sem).start()
            return carry

        def place(j, carry):
            pltpu.make_async_copy(embed_ref.at[0], buf.at[j], sem).wait()
            return carry

        def move(j, carry):
            sub = lax.rem(row_ref[base + j], 8)
            block = buf[j].astype(F32)
            keep = lax.broadcasted_iota(jnp.int32, block.shape, 0) == sub
            line = jnp.sum(jnp.where(keep, block, 0.0), axis=0, keepdims=True)
            wide[pl.ds(token_ref[base + j], 1), :] = line
            return carry

        lax.fori_loop(0, width, issue, 0)
        lax.fori_loop(0, width, place, 0)
        lax.fori_loop(0, width, move, 0)
        return carry

    lax.fori_loop(0, lax.div(count + slots - 1, slots), chunk, 0)
    out_ref[...] = wide[...].astype(BF16)


def local_rows(ids, shard, embed):
    total = N * ROWS
    local = ids - shard * VOCAB
    inside = (local >= 0) & (local < VOCAB)
    rank = jnp.cumsum(inside.astype(jnp.int32)) - 1
    rank = jnp.where(inside, rank, -1)
    hit = rank[None, :] == jnp.arange(total)[:, None]
    token = jnp.sum(jnp.where(hit, jnp.arange(total)[None, :], 0), axis=1)
    row = jnp.sum(jnp.where(hit, local[None, :], 0), axis=1)
    count = jnp.sum(inside.astype(jnp.int32)).reshape(1)
    return pl.pallas_call(
        rows_kernel,
        out_shape=jax.ShapeDtypeStruct((total, D), BF16),
        grid_spec=pltpu.PrefetchScalarGridSpec(
            num_scalar_prefetch=3, grid=(1,),
            in_specs=[ANY],
            out_specs=pl.BlockSpec((total, D), lambda i, *_: (0, 0)),
            scratch_shapes=[pltpu.VMEM((256, 8, D), BF16), pltpu.VMEM((total, D), F32), pltpu.SemaphoreType.DMA]),
        compiler_params=pltpu.CompilerParams(vmem_limit_bytes=VMEM_LIMIT),
    )(count, token, row, embed.reshape(VOCAB // 8, 8, D))


def embed_kernel(rows_ref, out_ref, acc, fin, tbuf, rbuf, send, recv):
    at = places()
    entry_barrier(at)
    scatter = Scatter(at, tbuf, rbuf, send, recv)

    def body(pos, carry):
        acc[...] = rows_ref[pick(pos, ORDER_RS, at)].astype(F32)
        scatter.after(pos, acc, fin)
        return carry

    lax.fori_loop(0, N, body, 0)
    scatter.finish(fin, out_ref)


def embed_sum(rows, ident):
    return pl.pallas_call(
        embed_kernel,
        out_shape=jax.ShapeDtypeStruct((ROWS, D), BF16),
        in_specs=[VM], out_specs=VM,
        scratch_shapes=scatter_scratch(),
        compiler_params=comm_params(ident),
    )(rows.reshape(N, ROWS, D))


def qkv_kernel(u_ref, w_ref, cos_ref, sin_ref, qk_ref, v_ref, ubuf, send, recv):
    at = places()
    entry_barrier(at)
    gather = Gather(at, u_ref, ubuf, send, recv)
    gather.start(0, 2)
    ubuf[at["me"]] = u_ref[...]
    weights = w_ref[...]

    def body(pos, carry):
        gather.before(pos, False)
        blk = pick(pos, ORDER_AG, at)
        out = lax.dot_general(ubuf[blk], weights, (((1,), (1,)), ((), ())), preferred_element_type=F32)
        cos = cos_ref[blk]
        sin = sin_ref[blk]
        low = lax.rem(lax.broadcasted_iota(jnp.int32, (ROWS, 128), 1), HEAD) < HEAD // 2
        for half in range(2):
            part = out[:, half * 128:(half + 1) * 128]
            swapped = jnp.where(low, pltpu.roll(part, 128 - HEAD // 2, 1), pltpu.roll(part, HEAD // 2, 1))
            qk_ref[blk, :, half * 128:(half + 1) * 128] = (part * cos + swapped * sin).astype(BF16)
        v_ref[blk] = out[:, 256:384].astype(BF16)
        return carry

    lax.fori_loop(0, N, body, 0)
    gather.finish()


def project(u, weights, cos, sin, ident):
    return pl.pallas_call(
        qkv_kernel,
        out_shape=(jax.ShapeDtypeStruct((N, ROWS, 256), BF16), jax.ShapeDtypeStruct((N, ROWS, 128), BF16)),
        in_specs=[VM] * 4, out_specs=(VM, VM),
        scratch_shapes=gather_scratch(),
        compiler_params=comm_params(ident),
    )(u, weights, cos, sin)


ATT_SEQS = 32


def attend_kernel(qk_ref, v_ref, start_ref, cache_ref, *rest):
    o_ref, new_ref, wide = rest[-3:]
    lane = lax.broadcasted_iota(jnp.int32, (8, 128), 1)
    row = lax.broadcasted_iota(jnp.int32, (8, 128), 0)
    first = lane < HEAD
    own = [(2 * j + lax.div(lane, HEAD)) == row for j in range(4)]

    def spread(twice):
        return jnp.concatenate([jnp.where(own[j], twice, 0.0) for j in range(4)], axis=1)

    for g in range(ATT_SEQS // 8):
        span = slice(8 * g, 8 * g + 8)
        start = start_ref[span, :]
        queries, keys, vals, hot = [], [], [], []
        for s in range(STEPS):
            qk = qk_ref[0, s].astype(F32)[span, :]
            left, right = qk[:, :128], qk[:, 128:]
            left_r, right_r = pltpu.roll(left, HEAD, 1), pltpu.roll(right, HEAD, 1)
            queries += [spread(jnp.where(first, left, left_r)), spread(jnp.where(first, left_r, left)),
                        spread(jnp.where(first, right, right_r))]
            keys.append(spread(jnp.where(first, right_r, right)))
            vals.append(spread(v_ref[0, s].astype(F32)[span, :]))
            hot.append(jnp.where(lane == start + s, 1.0, 0.0))
        query = jnp.concatenate(queries, axis=0).astype(BF16)
        hot_all = jnp.concatenate(hot, axis=0).astype(BF16)
        fresh = jnp.where((lane >= start) & (lane < start + STEPS), 1.0, 0.0)
        fresh = jnp.broadcast_to(fresh[:, None, :], (8, HEAD, 128)) > 0.5
        planes = []
        for kind, entry in enumerate((keys, vals)):
            entry_all = jnp.concatenate(entry, axis=0).astype(BF16)
            update = lax.dot_general(entry_all, hot_all, (((0,), (0,)), ((), ())), preferred_element_type=F32)
            old = cache_ref[0, kind, span].astype(F32)
            plane = jnp.where(fresh, update.reshape(8, HEAD, 128), old).astype(BF16)
            new_ref[0, kind, span] = plane
            planes.append(plane.reshape(8 * HEAD, 128))
        score = jnp.dot(query, planes[0], preferred_element_type=F32) * ATT_SCALE
        valid = jnp.concatenate([jnp.where(lane <= start + s, 0.0, -jnp.inf) for s in range(STEPS) for h in range(3)], axis=0)
        score = score + valid
        weight = jnp.exp(score - jnp.max(score, axis=1, keepdims=True))
        prob = (weight / jnp.sum(weight, axis=1, keepdims=True)).astype(BF16)
        mixed = lax.dot_general(prob, planes[1], (((1,), (1,)), ((), ())), preferred_element_type=F32)
        for s in range(STEPS):
            heads = []
            for h in range(3):
                part = mixed[8 * (3 * s + h):8 * (3 * s + h) + 8, :]
                total = sum(jnp.where(own[j], part[:, 128 * j:128 * j + 128], 0.0) for j in range(4))
                heads.append(total + pltpu.roll(total, HEAD, 1))
            wide[s, span, 0:128] = jnp.where(first, heads[0], heads[1])
            wide[s, span, 128:256] = heads[2]
    o_ref[0] = wide[...].astype(BF16)


def attention(layer, qk, v, start_wide, cache, new_cache):
    per = SEQS // ATT_SEQS
    token_map = lambda i: (lax.div(i, per), 0, lax.rem(i, per), 0)
    plane_map = lambda i: (layer, 0, i, 0, 0)
    plane_spec = pl.BlockSpec((1, 2, ATT_SEQS, HEAD, CACHE), plane_map)
    args = [qk.reshape(N, STEPS, SEQS, 256), v.reshape(N, STEPS, SEQS, 128), start_wide, cache]
    in_specs = [pl.BlockSpec((1, STEPS, ATT_SEQS, 256), token_map), pl.BlockSpec((1, STEPS, ATT_SEQS, 128), token_map),
                pl.BlockSpec((ATT_SEQS, 128), lambda i: (i, 0)), plane_spec]
    aliases = {}
    if new_cache is not None:
        args.append(new_cache)
        in_specs.append(ANY)
        aliases = {4: 1}
    return pl.pallas_call(
        attend_kernel,
        out_shape=(jax.ShapeDtypeStruct((N, STEPS, SEQS, 256), BF16), jax.ShapeDtypeStruct(cache.shape, BF16)),
        grid=(BATCH // ATT_SEQS,),
        in_specs=in_specs,
        out_specs=(pl.BlockSpec((1, STEPS, ATT_SEQS, 256), token_map), plane_spec),
        scratch_shapes=[pltpu.VMEM((STEPS, ATT_SEQS, 256), F32)],
        input_output_aliases=aliases,
        compiler_params=pltpu.CompilerParams(dimension_semantics=("arbitrary",), vmem_limit_bytes=VMEM_LIMIT),
    )(*args)


def out_kernel(o_ref, w_ref, out_ref, acc, fin, tbuf, rbuf, send, recv):
    at = places()
    entry_barrier(at)
    scatter = Scatter(at, tbuf, rbuf, send, recv)

    def body(pos, carry):
        acc[...] = jnp.dot(o_ref[pick(pos, ORDER_RS, at)], w_ref[...], preferred_element_type=F32)
        scatter.after(pos, acc, fin)
        return carry

    lax.fori_loop(0, N, body, 0)
    scatter.finish(fin, out_ref)


def out_project(mixed, weights, ident):
    return pl.pallas_call(
        out_kernel,
        out_shape=jax.ShapeDtypeStruct((ROWS, D), BF16),
        in_specs=[VM, VM], out_specs=VM,
        scratch_shapes=scatter_scratch(),
        compiler_params=comm_params(ident),
    )(mixed.reshape(N, ROWS, 256), weights)


def moe_kernel(layer, u_ref, router_ref, chosen_ref, gate_hbm, up_hbm, down_hbm, out_ref, ubuf, ag_send, ag_recv,
               acc, fin, tbuf, rbuf, rs_send, rs_recv, gate_v, up_v, down_v, hidden, gates, w_sem):
    down_load = pltpu.make_async_copy(down_hbm.at[layer], down_v, w_sem.at[2, 0])
    for e in range(LOCAL_EXPERTS):
        pltpu.make_async_copy(gate_hbm.at[layer, e], gate_v.at[e], w_sem.at[0, e]).start()
        pltpu.make_async_copy(up_hbm.at[layer, e], up_v.at[e], w_sem.at[1, e]).start()
    down_load.start()
    at = places()
    entry_barrier(at)
    gather = Gather(at, u_ref, ubuf, ag_send, ag_recv)
    scatter = Scatter(at, tbuf, rbuf, rs_send, rs_recv)
    gather.start(0, 2)
    ubuf[at["me"]] = u_ref[...]

    def body(pos, carry):
        gather.before(pos, True)
        blk = pick(pos, ORDER_RS, at)
        route = jnp.dot(ubuf[blk], router_ref[...], preferred_element_type=F32)
        masked = jnp.where(chosen_ref[blk] > 0.5, route, -jnp.inf)
        weight = jnp.exp(masked - jnp.max(masked, axis=1, keepdims=True))
        gates[...] = weight / jnp.sum(weight, axis=1, keepdims=True)

        def expert(e, carry):
            @pl.when(pos == 0)
            def _():
                pltpu.make_async_copy(gate_hbm.at[layer, e], gate_v.at[e], w_sem.at[0, e]).wait()
                pltpu.make_async_copy(up_hbm.at[layer, e], up_v.at[e], w_sem.at[1, e]).wait()
            lane = lax.broadcasted_iota(jnp.int32, (ROWS, 128), 1)
            share = jnp.sum(jnp.where(lane == e, gates[...], 0.0), axis=1, keepdims=True)
            gate_act = jnp.dot(ubuf[blk], gate_v[e], preferred_element_type=F32)
            up_act = jnp.dot(ubuf[blk], up_v[e], preferred_element_type=F32)
            z = gate_act * jax.nn.sigmoid(gate_act) * up_act * share
            hidden[:, pl.ds(pl.multiple_of(e * FF, FF), FF)] = z.astype(BF16)
            return carry

        lax.fori_loop(0, LOCAL_EXPERTS, expert, 0)

        @pl.when(pos == 0)
        def _():
            down_load.wait()

        def column(c, carry):
            cols = pl.ds(pl.multiple_of(c * 512, 512), 512)
            acc[:, cols] = jnp.dot(hidden[...], down_v[:, cols], preferred_element_type=F32)
            return carry

        lax.fori_loop(0, D // 512, column, 0)
        scatter.after(pos, acc, fin)
        return carry

    lax.fori_loop(0, N, body, 0)
    gather.finish()
    scatter.finish(fin, out_ref)


def experts(layer, u, router, chosen, w_gate, w_up, w_down, ident):
    width = LOCAL_EXPERTS * FF
    return pl.pallas_call(
        functools.partial(moe_kernel, layer),
        out_shape=jax.ShapeDtypeStruct((ROWS, D), BF16),
        in_specs=[VM, VM, VM, ANY, ANY, ANY], out_specs=VM,
        scratch_shapes=gather_scratch() + scatter_scratch() + [
            pltpu.VMEM((LOCAL_EXPERTS, D, FF), BF16), pltpu.VMEM((LOCAL_EXPERTS, D, FF), BF16),
            pltpu.VMEM((width, D), BF16), pltpu.VMEM((ROWS, width), BF16), pltpu.VMEM((ROWS, 128), F32),
            pltpu.SemaphoreType.DMA((3, LOCAL_EXPERTS))],
        compiler_params=comm_params(ident),
    )(u, router, chosen, w_gate, w_up, w_down.reshape(LAYERS, width, D))


HEAD_ROWS = SEQS * (STEPS - 1)
TILE = 512
TILES = VOCAB // TILE


def fold(logits, column, target, peak, total, picked):
    parts = [logits[:, 128 * j:128 * j + 128] for j in range(TILE // 128)]
    top = functools.reduce(jnp.maximum, parts, peak)
    total = total * jnp.exp(peak - top)
    lane = lax.broadcasted_iota(jnp.int32, parts[0].shape, 1) + column
    for j, part in enumerate(parts):
        total = total + jnp.exp(part - top)
        picked = picked + jnp.where(lane + 128 * j == target, part, 0.0)
    return top, total, picked


def summary(peak, total, picked):
    top = jnp.max(peak, axis=1, keepdims=True)
    total = jnp.sum(total * jnp.exp(peak - top), axis=1, keepdims=True)
    picked = jnp.sum(picked, axis=1, keepdims=True)
    lane = lax.broadcasted_iota(jnp.int32, peak.shape, 1)
    return jnp.where(lane == 0, top, jnp.where(lane == 1, total, picked))


def head_kernel(f_ref, target_ref, embed_ref, stats_ref, last_ref, ubuf, send, recv, table, peak, total, picked, sem):
    def load(c):
        rows = pl.ds(pl.multiple_of(c * TILE, TILE), TILE)
        return pltpu.make_async_copy(embed_ref.at[rows], table.at[rows], sem.at[c])

    for c in range(TILES):
        load(c).start()
    at = places()
    entry_barrier(at)
    gather = Gather(at, f_ref, ubuf, send, recv)
    gather.start(0, 2)
    ubuf[at["me"]] = f_ref[...]

    def body(pos, carry):
        gather.before(pos, False)
        blk = pick(pos, ORDER_AG, at)
        peak[...] = jnp.full_like(peak, -1e30)
        total[...] = jnp.zeros_like(total)
        picked[...] = jnp.zeros_like(picked)

        def tile(c, carry):
            @pl.when(pos == 0)
            def _():
                load(c).wait()
            rows = pl.ds(pl.multiple_of(c * TILE, TILE), TILE)
            logits = lax.dot_general(ubuf[blk, 0:HEAD_ROWS, :], table[rows, :], (((1,), (1,)), ((), ())),
                                     preferred_element_type=F32) * (1.0 / LOGIT_DIV)
            peak[...], total[...], picked[...] = fold(logits, c * TILE, target_ref[blk], peak[...], total[...], picked[...])
            return carry

        lax.fori_loop(0, TILES, tile, 0)
        stats_ref[blk] = summary(peak[...], total[...], picked[...])
        last_ref[blk] = ubuf[blk, HEAD_ROWS:ROWS, :]
        return carry

    lax.fori_loop(0, N, body, 0)
    gather.finish()


def head_stats(f, target_wide, embed, ident):
    return pl.pallas_call(
        head_kernel,
        out_shape=(jax.ShapeDtypeStruct((N, HEAD_ROWS, 128), F32), jax.ShapeDtypeStruct((N, SEQS, D), BF16)),
        in_specs=[VM, VM, ANY], out_specs=(VM, VM),
        scratch_shapes=gather_scratch() + [pltpu.VMEM((VOCAB, D), BF16)] + [pltpu.VMEM((HEAD_ROWS, 128), F32)] * 3 + [
            pltpu.SemaphoreType.DMA((TILES,))],
        compiler_params=comm_params(ident),
    )(f, target_wide, embed)


def last_kernel(f_ref, target_ref, embed_ref, logits_ref, stats_ref, peak, total, picked):
    c = pl.program_id(0)

    @pl.when(c == 0)
    def _():
        peak[...] = jnp.full_like(peak, -1e30)
        total[...] = jnp.zeros_like(total)
        picked[...] = jnp.zeros_like(picked)

    logits = lax.dot_general(f_ref[...], embed_ref[...], (((1,), (1,)), ((), ())),
                             preferred_element_type=F32) * (1.0 / LOGIT_DIV)
    logits_ref[...] = logits
    peak[...], total[...], picked[...] = fold(logits, c * TILE, target_ref[...], peak[...], total[...], picked[...])

    @pl.when(c == TILES - 1)
    def _():
        stats_ref[...] = summary(peak[...], total[...], picked[...])


def last_step(f, target_wide, embed):
    return pl.pallas_call(
        last_kernel,
        out_shape=(jax.ShapeDtypeStruct((BATCH, VOCAB), F32), jax.ShapeDtypeStruct((BATCH, 128), F32)),
        grid=(TILES,),
        in_specs=[pl.BlockSpec((BATCH, D), lambda c: (0, 0)), pl.BlockSpec((BATCH, 128), lambda c: (0, 0)),
                  pl.BlockSpec((TILE, D), lambda c: (c, 0))],
        out_specs=(pl.BlockSpec((BATCH, TILE), lambda c: (0, c)), pl.BlockSpec((BATCH, 128), lambda c: (0, 0))),
        scratch_shapes=[pltpu.VMEM((BATCH, 128), F32)] * 3,
        compiler_params=pltpu.CompilerParams(dimension_semantics=("arbitrary",), vmem_limit_bytes=VMEM_LIMIT),
    )(f, target_wide, embed)


def share_kernel(in_ref, out_ref, send, recv):
    me = lax.axis_index("tp")
    barrier = pltpu.get_barrier_semaphore()
    for shift in range(1, N):
        pl.semaphore_signal(barrier, inc=1, device_id={"tp": lax.rem(me + shift, N)}, device_id_type=MESH)
    pl.semaphore_wait(barrier, N - 1)
    copies = [pltpu.make_async_remote_copy(
        src_ref=in_ref, dst_ref=out_ref.at[shift], send_sem=send.at[shift], recv_sem=recv.at[shift],
        device_id={"tp": lax.rem(me + shift, N)}, device_id_type=MESH) for shift in range(1, N)]
    for item in copies:
        item.start()
    out_ref[0] = in_ref[...]
    for item in copies:
        item.wait()


def share(values, ident):
    return pl.pallas_call(
        share_kernel,
        out_shape=jax.ShapeDtypeStruct((N,) + values.shape, F32),
        in_specs=[VM], out_specs=VM,
        scratch_shapes=[pltpu.SemaphoreType.DMA((N,)), pltpu.SemaphoreType.DMA((N,))],
        compiler_params=comm_params(ident),
    )(values)


def rms_norm(hidden, gain):
    mean_sq = jnp.mean(hidden * hidden, axis=-1, keepdims=True)
    return (hidden * lax.rsqrt(mean_sq + NORM_EPS) * gain).astype(BF16)


def by_block(values):
    return values.reshape(N, SEQS, values.shape[1]).transpose(0, 2, 1)


def solution(mesh):
    cache_spec = P(None, None, 'dp', None, 'tp', None)
    expert_spec = P(None, 'tp', None, None)
    in_specs = (P('dp', None), P('dp'), cache_spec, P(None, None, 'dp', None), P('tp', None), P(None, None), P(None, None, 'tp'), P(None, None, 'tp'), P(None, None, 'tp'), P(None, 'tp', None), P(None, None, None), expert_spec, expert_spec, expert_spec)
    out_specs = (P('dp', None), P('dp', 'tp'), cache_spec)

    def decode_local(tokens, start_pos, kv_cache, expert_ids, embed, norm_gain, w_query, w_key, w_value, w_out, w_router, w_gate, w_up, w_down):
        shard = lax.axis_index('tp')
        cache = kv_cache.transpose(0, 1, 2, 4, 5, 3).reshape(LAYERS, 2, BATCH, HEAD, CACHE)

        ids = by_block(tokens[:, :STEPS]).reshape(-1)
        rows = local_rows(ids, shard, embed)
        hidden = EMBED_MULT * embed_sum(rows, 0).astype(F32)

        pos = by_block(start_pos[:, None] + jnp.arange(STEPS)[None, :]).reshape(N, ROWS)
        inv_freq = ROPE_THETA ** (-2.0 * jnp.arange(HEAD // 2, dtype=F32) / HEAD)
        angles = pos.astype(F32)[:, :, None] * inv_freq
        cos, sin = jnp.cos(angles), jnp.sin(angles)
        cos = jnp.concatenate([cos] * 4, axis=-1)
        sin = jnp.concatenate([-sin, sin, -sin, sin], axis=-1)
        start_wide = jnp.broadcast_to(start_pos[:, None], (BATCH, 128))

        wq, wk, wv = (w.transpose(0, 2, 1) for w in (w_query, w_key, w_value))
        w_qkv = jnp.concatenate([wq, wk, wv, wv], axis=1)
        w_out_wide = jnp.concatenate([w_out, jnp.zeros((LAYERS, 64, D), BF16)], axis=1)

        first_expert = shard * LOCAL_EXPERTS
        turned = lax.rem(jnp.arange(EXPERTS) + first_expert, EXPERTS)
        router = jnp.take(w_router, turned, axis=2)
        router = jnp.concatenate([router, jnp.zeros((LAYERS, D, 128 - EXPERTS), BF16)], axis=2)
        lanes = jnp.concatenate([turned, jnp.full((128 - EXPERTS,), -1, turned.dtype)])
        chosen = jnp.any(expert_ids[..., None] == lanes, axis=3).astype(F32)
        chosen = chosen.reshape(STEPS, LAYERS, N, SEQS, 128).transpose(1, 2, 0, 3, 4).reshape(LAYERS, N, ROWS, 128)

        new_cache = None
        for layer in range(LAYERS):
            u = rms_norm(hidden, norm_gain[2 * layer])
            qk, v = project(u, w_qkv[layer], cos, sin, 1 + 3 * layer)
            mixed, new_cache = attention(layer, qk, v, start_wide, cache, new_cache)
            attn = out_project(mixed, w_out_wide[layer], 2 + 3 * layer)
            hidden = hidden + RESID_MULT * attn.astype(F32)
            u = rms_norm(hidden, norm_gain[2 * layer + 1])
            y = experts(layer, u, router[layer], chosen[layer], w_gate, w_up, w_down, 3 + 3 * layer)
            hidden = hidden + RESID_MULT * y.astype(F32)

        f = rms_norm(hidden, norm_gain[2 * LAYERS])
        target = tokens[:, 1:] - shard * VOCAB
        early = by_block(target[:, :STEPS - 1]).reshape(N, HEAD_ROWS, 1)
        stats, f_last = head_stats(f, jnp.broadcast_to(early, (N, HEAD_ROWS, 128)), embed, 7)
        last = jnp.broadcast_to(target[:, STEPS - 1:], (BATCH, 128))
        logits, last_stats = last_step(f_last.reshape(BATCH, D), last, embed)
        stats = stats[:, :, :8].reshape(N, STEPS - 1, SEQS, 8).transpose(3, 1, 0, 2).reshape(8, (STEPS - 1) * BATCH)
        packed = jnp.concatenate([stats, last_stats[:, :8].T], axis=1)
        shared = share(packed, 8)
        peak = jnp.max(shared[:, 0], axis=0)
        total = jnp.sum(shared[:, 1] * jnp.exp(shared[:, 0] - peak), axis=0)
        log_probs = jnp.sum(shared[:, 2], axis=0) - peak - jnp.log(total)
        log_probs = log_probs.reshape(STEPS, BATCH).T
        new_cache = new_cache.reshape(LAYERS, 2, BATCH, 1, HEAD, CACHE).transpose(0, 1, 2, 5, 3, 4)
        return log_probs, logits, new_cache

    return jax.shard_map(decode_local, mesh=mesh, in_specs=in_specs, out_specs=out_specs, check_vma=False)
```

```python
import functools

import jax
import jax.numpy as jnp
from jax import lax
from jax.experimental import pallas as pl
from jax.experimental.pallas import tpu as pltpu
from jax.sharding import PartitionSpec as P

EMBED_MULT = 12.0
ATT_SCALE = 0.015625
RESID_MULT = 0.22
LOGIT_DIV = 6.0
NORM_EPS = 1e-6
ROPE_THETA = 10000.0

D = 1536
HEAD = 64
BATCH = 512
STEPS = 4
LAYERS = 2
CACHE = 128
EXPERTS = 40
LOCAL_EXPERTS = 5
FF = 512
VOCAB = 6144
N = 8
SEQS = BATCH // N
ROWS = SEQS * STEPS
MESH = pl.DeviceIdType.MESH
F32 = jnp.float32
BF16 = jnp.bfloat16
VMEM_LIMIT = 60 * 1024 * 1024

ORDER_RS = ("me", "sib", "bs", "a", "ds", "dg", "as", "b")
ORDER_AG = ("me", "sib", "bs", "a", "as", "b", "ds", "dg")


def places():
    me = lax.axis_index("tp")
    k = lax.rem(me, 2)
    x = lax.rem(lax.div(me, 2), 2)
    y = lax.div(me, 4)
    step_x = 2 - 4 * x
    step_y = 4 - 8 * y
    a = me + step_x + k * (step_y - step_x)
    b = me + step_y + k * (step_x - step_y)
    dg = me + step_x + step_y
    s = 1 - 2 * k
    return {"me": me, "sib": me + s, "a": a, "as": a + s, "b": b, "bs": b + s, "dg": dg, "ds": dg + s}


def entry_barrier(at, names=("sib", "a", "b")):
    barrier = pltpu.get_barrier_semaphore()
    for name in names:
        pl.semaphore_signal(barrier, inc=1, device_id={"tp": at[name]}, device_id_type=MESH)
    pl.semaphore_wait(barrier, len(names))


def pick(pos, order, at):
    total = jnp.int32(0)
    for i, name in enumerate(order):
        total = total + jnp.where(pos == i, at[name], 0)
    return total


class Gather:
    def __init__(self, at, own, ubuf, send, recv):
        self.at, self.own, self.ubuf, self.send, self.recv = at, own, ubuf, send, recv

    def copy(self, src, origin, target, slot):
        return pltpu.make_async_remote_copy(
            src_ref=src, dst_ref=self.ubuf.at[origin], send_sem=self.send.at[slot], recv_sem=self.recv.at[origin],
            device_id={"tp": target}, device_id_type=MESH)

    def item(self, slot):
        at = self.at
        if slot < 3:
            return self.copy(self.own, at["me"], at[("a", "b", "sib")[slot]], slot)
        name, target = (("a", "b"), ("a", "sib"), ("b", "sib"), ("dg", "sib"))[slot - 3]
        return self.copy(self.ubuf.at[at[name]], at[name], at[target], slot)

    def start(self, *slots):
        for slot in slots:
            self.item(slot).start()

    def arrive(self, name):
        origin = self.at[name]
        self.copy(self.own, origin, self.at["sib"], 0).wait_recv()

    def before(self, pos, rs):
        @pl.when(pos == 1)
        def _():
            self.start(1)
            self.arrive("sib")

        @pl.when(pos == 2)
        def _():
            self.arrive("a")
            self.start(3, 4)
            self.arrive("bs")

        @pl.when(pos == 4)
        def _():
            self.arrive("b")
            self.start(5)
            if rs:
                self.arrive("dg")
                self.start(6)
                self.arrive("ds")
            else:
                self.arrive("as")

        @pl.when(pos == 6)
        def _():
            if rs:
                self.arrive("as")
            else:
                self.arrive("dg")
                self.start(6)
                self.arrive("ds")

    def finish(self):
        for slot in range(7):
            self.item(slot).wait_send()


class Scatter:
    def __init__(self, at, tbuf, rbuf, send, recv):
        self.at, self.tbuf, self.rbuf, self.send, self.recv = at, tbuf, rbuf, send, recv

    def copy(self, slot, target):
        return pltpu.make_async_remote_copy(
            src_ref=self.tbuf.at[slot], dst_ref=self.rbuf.at[slot], send_sem=self.send.at[slot],
            recv_sem=self.recv.at[slot], device_id={"tp": target}, device_id_type=MESH)

    def arrive(self, slot):
        self.copy(slot, self.at["sib"]).wait_recv()

    def after(self, pos, acc, fin):
        at = self.at

        @pl.when(pos == 0)
        def _():
            fin[...] = acc[...]

        @pl.when((pos == 1) | (pos == 2) | (pos == 4) | (pos == 6))
        def _():
            slot = lax.div(pos, 2)
            self.tbuf[slot] = acc[...].astype(BF16)
            self.copy(slot, at["sib"]).start()

        @pl.when((pos == 3) | (pos == 5))
        def _():
            slot = lax.div(pos, 2)
            out = slot + 3
            self.arrive(slot)
            self.tbuf[out] = (acc[...] + self.rbuf[slot].astype(F32)).astype(BF16)
            self.copy(out, at["a"]).start()

        @pl.when(pos == 7)
        def _():
            self.arrive(3)
            self.arrive(5)
            self.tbuf[6] = (acc[...] + self.rbuf[3].astype(F32) + self.rbuf[5].astype(F32)).astype(BF16)
            self.copy(6, at["b"]).start()

    def finish(self, fin, hidden_in, gain_ref, hidden_ref, normed_ref):
        self.arrive(0)
        self.arrive(4)
        self.arrive(6)

        def chunk(c, carry):
            rows = pl.ds(pl.multiple_of(c * 32, 32), 32)
            total = fin[rows, :]
            for slot in (0, 4, 6):
                total = total + self.rbuf[slot, rows, :].astype(F32)
            total = total.astype(BF16).astype(F32)
            if hidden_in is None:
                hidden = EMBED_MULT * total
            else:
                hidden = hidden_in[rows, :] + RESID_MULT * total
            hidden_ref[rows, :] = hidden
            mean_sq = jnp.mean(hidden * hidden, axis=1, keepdims=True)
            normed_ref[rows, :] = (hidden * lax.rsqrt(mean_sq + NORM_EPS) * gain_ref[...]).astype(BF16)
            return carry

        lax.fori_loop(0, ROWS // 32, chunk, 0)
        for slot in range(7):
            self.copy(slot, self.at["sib"]).wait_send()


def gather_scratch():
    return [pltpu.VMEM((N, ROWS, D), BF16), pltpu.SemaphoreType.DMA((7,)), pltpu.SemaphoreType.DMA((N,))]


def scatter_scratch():
    return [pltpu.VMEM((ROWS, D), F32), pltpu.VMEM((ROWS, D), F32), pltpu.VMEM((7, ROWS, D), BF16),
            pltpu.VMEM((7, ROWS, D), BF16), pltpu.SemaphoreType.DMA((7,)), pltpu.SemaphoreType.DMA((7,))]


VM = pl.BlockSpec(memory_space=pltpu.VMEM)
RESIDUAL = (jax.ShapeDtypeStruct((ROWS, D), F32), jax.ShapeDtypeStruct((ROWS, D), BF16))
ANY = pl.BlockSpec(memory_space=pl.ANY)


def comm_params(ident):
    return pltpu.CompilerParams(collective_id=ident, has_side_effects=True, vmem_limit_bytes=VMEM_LIMIT)


def rows_kernel(count_ref, token_ref, row_ref, embed_ref, out_ref, buf, wide, sem):
    wide[...] = jnp.zeros_like(wide)
    count = count_ref[0]
    slots = buf.shape[0]

    def chunk(c, carry):
        base = c * slots
        width = jnp.minimum(slots, count - base)

        def issue(j, carry):
            pltpu.make_async_copy(embed_ref.at[lax.div(row_ref[base + j], 8)], buf.at[j], sem).start()
            return carry

        def place(j, carry):
            pltpu.make_async_copy(embed_ref.at[0], buf.at[j], sem).wait()
            return carry

        def move(j, carry):
            sub = lax.rem(row_ref[base + j], 8)
            block = buf[j].astype(F32)
            keep = lax.broadcasted_iota(jnp.int32, block.shape, 0) == sub
            line = jnp.sum(jnp.where(keep, block, 0.0), axis=0, keepdims=True)
            wide[pl.ds(token_ref[base + j], 1), :] = line
            return carry

        lax.fori_loop(0, width, issue, 0)
        lax.fori_loop(0, width, place, 0)
        lax.fori_loop(0, width, move, 0)
        return carry

    lax.fori_loop(0, lax.div(count + slots - 1, slots), chunk, 0)
    out_ref[...] = wide[...].astype(BF16)


def local_rows(ids, shard, embed):
    total = N * ROWS
    local = ids - shard * VOCAB
    inside = (local >= 0) & (local < VOCAB)
    rank = jnp.cumsum(inside.astype(jnp.int32)) - 1
    rank = jnp.where(inside, rank, -1)
    hit = rank[None, :] == jnp.arange(total)[:, None]
    token = jnp.sum(jnp.where(hit, jnp.arange(total)[None, :], 0), axis=1)
    row = jnp.sum(jnp.where(hit, local[None, :], 0), axis=1)
    count = jnp.sum(inside.astype(jnp.int32)).reshape(1)
    return pl.pallas_call(
        rows_kernel,
        out_shape=jax.ShapeDtypeStruct((total, D), BF16),
        grid_spec=pltpu.PrefetchScalarGridSpec(
            num_scalar_prefetch=3, grid=(1,),
            in_specs=[ANY],
            out_specs=pl.BlockSpec((total, D), lambda i, *_: (0, 0)),
            scratch_shapes=[pltpu.VMEM((256, 8, D), BF16), pltpu.VMEM((total, D), F32), pltpu.SemaphoreType.DMA]),
        compiler_params=pltpu.CompilerParams(vmem_limit_bytes=VMEM_LIMIT),
    )(count, token, row, embed.reshape(VOCAB // 8, 8, D))


def embed_kernel(rows_ref, gain_ref, hidden_ref, normed_ref, acc, fin, tbuf, rbuf, send, recv):
    at = places()
    entry_barrier(at)
    scatter = Scatter(at, tbuf, rbuf, send, recv)

    def body(pos, carry):
        acc[...] = rows_ref[pick(pos, ORDER_RS, at)].astype(F32)
        scatter.after(pos, acc, fin)
        return carry

    lax.fori_loop(0, N, body, 0)
    scatter.finish(fin, None, gain_ref, hidden_ref, normed_ref)


def embed_sum(rows, gain, ident):
    return pl.pallas_call(
        embed_kernel,
        out_shape=RESIDUAL,
        in_specs=[VM, VM], out_specs=(VM, VM),
        scratch_shapes=scatter_scratch(),
        compiler_params=comm_params(ident),
    )(rows.reshape(N, ROWS, D), gain)


HALF = 32
SLOTS = 4


def attend_half(base, start_ref, first_seq, qk, vv, planes, mixed_out):
    lane = lax.broadcasted_iota(jnp.int32, (8, 128), 1)
    row = lax.broadcasted_iota(jnp.int32, (8, 128), 0)
    first = lane < HEAD
    own = [(2 * j + lax.div(lane, HEAD)) == row for j in range(4)]
    groups = range(HALF // 8)

    def spread(twice):
        return jnp.concatenate([jnp.where(own[j], twice, 0.0) for j in range(4)], axis=1)

    starts = [start_ref[pl.ds(pl.multiple_of(first_seq + base + 8 * g, 8), 8), :] for g in groups]
    query, updates = [], []
    for g in groups:
        queries, keys, vals, hot = [], [], [], []
        for s in range(STEPS):
            span = pl.ds(pl.multiple_of(s * SEQS + base + 8 * g, 8), 8)
            left, right = qk[span, 0:128], qk[span, 128:256]
            left_r, right_r = pltpu.roll(left, HEAD, 1), pltpu.roll(right, HEAD, 1)
            queries += [spread(jnp.where(first, left, left_r)), spread(jnp.where(first, left_r, left)),
                        spread(jnp.where(first, right, right_r))]
            keys.append(spread(jnp.where(first, right_r, right)))
            vals.append(spread(vv[span, :]))
            hot.append(jnp.where(lane == starts[g] + s, 1.0, 0.0))
        query.append(jnp.concatenate(queries, axis=0).astype(BF16))
        hot_all = jnp.concatenate(hot, axis=0).astype(BF16)
        updates.append([
            lax.dot_general(jnp.concatenate(entry, axis=0).astype(BF16), hot_all, (((0,), (0,)), ((), ())),
                            preferred_element_type=F32) for entry in (keys, vals)])
    for g in groups:
        span = pl.ds(base + 8 * g, 8)
        fresh = jnp.where((lane >= starts[g]) & (lane < starts[g] + STEPS), 1.0, 0.0)
        fresh = jnp.broadcast_to(fresh[:, None, :], (8, HEAD, 128)) > 0.5
        for kind in range(2):
            old = planes[kind, span].astype(F32)
            planes[kind, span] = jnp.where(fresh, updates[g][kind].reshape(8, HEAD, 128), old).astype(BF16)
    scores = [jnp.dot(query[g], planes[0, pl.ds(base + 8 * g, 8)].reshape(8 * HEAD, 128), preferred_element_type=F32)
              for g in groups]
    probs = []
    for g in groups:
        valid = [jnp.where(lane <= starts[g] + s, 0.0, -jnp.inf) for s in range(STEPS)]
        score = scores[g] * ATT_SCALE + jnp.concatenate([valid[s] for s in range(STEPS) for h in range(3)], axis=0)
        weight = jnp.exp(score - jnp.max(score, axis=1, keepdims=True))
        probs.append((weight / jnp.sum(weight, axis=1, keepdims=True)).astype(BF16))
    mixed = [lax.dot_general(probs[g], planes[1, pl.ds(base + 8 * g, 8)].reshape(8 * HEAD, 128),
                             (((1,), (1,)), ((), ())), preferred_element_type=F32) for g in groups]
    for g in groups:
        for s in range(STEPS):
            span = pl.ds(pl.multiple_of(s * SEQS + base + 8 * g, 8), 8)
            heads = []
            for h in range(3):
                part = mixed[g][8 * (3 * s + h):8 * (3 * s + h) + 8, :]
                total = sum(jnp.where(own[j], part[:, 128 * j:128 * j + 128], 0.0) for j in range(4))
                heads.append(total + pltpu.roll(total, HEAD, 1))
            mixed_out[span, 0:128] = jnp.where(first, heads[0], heads[1])
            mixed_out[span, 128:256] = heads[2]


def attn_kernel(layer, u_ref, w_ref, cos_ref, sin_ref, start_ref, w_out_ref, hidden_in, gain_ref, cache_ref, *rest):
    if layer > 0:
        rest = rest[1:]
    (hidden_ref, normed_ref, new_ref, ubuf, ag_send, ag_recv, acc, fin, tbuf, rbuf, rs_send, rs_recv,
     qk, vv, mixed, planes, in_sem, out_sem) = rest
    at = places()

    def plane_span(pos):
        return pl.ds(pick(pos, ORDER_RS, at) * SEQS, SEQS)

    def load(pos):
        slot = lax.rem(pos, SLOTS)
        return pltpu.make_async_copy(cache_ref.at[layer, :, plane_span(pos)], planes.at[slot], in_sem.at[slot])

    def store(pos):
        slot = lax.rem(pos, SLOTS)
        return pltpu.make_async_copy(planes.at[slot], new_ref.at[layer, :, plane_span(pos)], out_sem.at[slot])

    load(jnp.int32(0)).start()
    load(jnp.int32(1)).start()
    entry_barrier(at)
    gather = Gather(at, u_ref, ubuf, ag_send, ag_recv)
    scatter = Scatter(at, tbuf, rbuf, rs_send, rs_recv)
    gather.start(0, 2)
    ubuf[at["me"]] = u_ref[...]

    def body(pos, carry):
        gather.before(pos, True)
        blk = pick(pos, ORDER_RS, at)

        @pl.when(pos >= 2)
        def _():
            store(pos - 2).wait()

        @pl.when(pos < N - 2)
        def _():
            load(pos + 2).start()

        out = lax.dot_general(ubuf[blk], w_ref[...], (((1,), (1,)), ((), ())), preferred_element_type=F32)
        cos = cos_ref[blk]
        sin = sin_ref[blk]
        low = lax.rem(lax.broadcasted_iota(jnp.int32, (ROWS, 128), 1), HEAD) < HEAD // 2
        for half in range(2):
            part = out[:, half * 128:(half + 1) * 128]
            swapped = jnp.where(low, pltpu.roll(part, 128 - HEAD // 2, 1), pltpu.roll(part, HEAD // 2, 1))
            qk[:, half * 128:(half + 1) * 128] = (part * cos + swapped * sin).astype(BF16).astype(F32)
        vv[...] = out[:, 256:384].astype(BF16).astype(F32)
        load(pos).wait()

        def half_block(i, carry):
            attend_half(i * HALF, start_ref, blk * SEQS, qk, vv, planes.at[lax.rem(pos, SLOTS)], mixed)
            return carry

        lax.fori_loop(0, SEQS // HALF, half_block, 0)
        store(pos).start()
        acc[...] = jnp.dot(mixed[...].astype(BF16), w_out_ref[...], preferred_element_type=F32)
        scatter.after(pos, acc, fin)
        return carry

    lax.fori_loop(0, N, body, 0)
    store(jnp.int32(N - 2)).wait()
    store(jnp.int32(N - 1)).wait()
    gather.finish()
    scatter.finish(fin, hidden_in, gain_ref, hidden_ref, normed_ref)


def attention(layer, u, w_qkv, cos, sin, start_wide, w_out, hidden, gain, cache, new_cache, ident):
    args = [u, w_qkv, cos, sin, start_wide, w_out, hidden, gain, cache]
    in_specs = [VM] * 8 + [ANY]
    aliases = {}
    if new_cache is not None:
        args.append(new_cache)
        in_specs.append(ANY)
        aliases = {9: 2}
    return pl.pallas_call(
        functools.partial(attn_kernel, layer),
        out_shape=RESIDUAL + (jax.ShapeDtypeStruct(cache.shape, BF16),),
        in_specs=in_specs, out_specs=(VM, VM, ANY),
        scratch_shapes=gather_scratch() + scatter_scratch() + [
            pltpu.VMEM((ROWS, 256), F32), pltpu.VMEM((ROWS, 128), F32), pltpu.VMEM((ROWS, 256), F32),
            pltpu.VMEM((SLOTS, 2, SEQS, HEAD, CACHE), BF16), pltpu.SemaphoreType.DMA((SLOTS,)),
            pltpu.SemaphoreType.DMA((SLOTS,))],
        input_output_aliases=aliases,
        compiler_params=comm_params(ident),
    )(*args)


def moe_kernel(layer, u_ref, router_ref, ids_ref, hidden_in, gain_ref, gate_hbm, up_hbm, down_hbm, hidden_ref, normed_ref,
               ubuf, ag_send, ag_recv, acc, fin, tbuf, rbuf, rs_send, rs_recv, gate_v, up_v, down_v, hidden, gates, w_sem):
    def load(kind, e):
        src, dst = ((gate_hbm, gate_v), (up_hbm, up_v))[kind]
        return pltpu.make_async_copy(src.at[layer, e], dst.at[e], w_sem.at[kind, e])

    down_load = pltpu.make_async_copy(down_hbm.at[layer], down_v, w_sem.at[2, 0])
    for e in range(LOCAL_EXPERTS):
        load(0, e).start()
        load(1, e).start()
    down_load.start()
    at = places()
    entry_barrier(at)
    gather = Gather(at, u_ref, ubuf, ag_send, ag_recv)
    scatter = Scatter(at, tbuf, rbuf, rs_send, rs_recv)
    gather.start(0, 2)
    ubuf[at["me"]] = u_ref[...]
    lane = lax.broadcasted_iota(jnp.int32, (ROWS, 128), 1)

    def route(blk):
        ids = ids_ref[blk]
        chosen = lane == ids[:, 0:1]
        for j in range(1, 8):
            chosen = chosen | (lane == ids[:, j:j + 1])
        score = jnp.dot(ubuf[blk], router_ref[...], preferred_element_type=F32)
        masked = jnp.where(chosen, score, -jnp.inf)
        weight = jnp.exp(masked - jnp.max(masked, axis=1, keepdims=True))
        gates[...] = weight / jnp.sum(weight, axis=1, keepdims=True)

    def expert(blk, e):
        share = jnp.sum(jnp.where(lane == e, gates[...], 0.0), axis=1, keepdims=True)
        gate_act = jnp.dot(ubuf[blk], gate_v[e], preferred_element_type=F32)
        up_act = jnp.dot(ubuf[blk], up_v[e], preferred_element_type=F32)
        z = gate_act * jax.nn.sigmoid(gate_act) * up_act * share
        start = e * FF if isinstance(e, int) else pl.multiple_of(e * FF, FF)
        hidden[:, pl.ds(start, FF)] = z.astype(BF16)

    def down():
        for c in range(D // 512):
            cols = slice(c * 512, c * 512 + 512)
            acc[:, cols] = jnp.dot(hidden[...], down_v[:, cols], preferred_element_type=F32)

    def first_expert(e, carry):
        load(0, e).wait()
        load(1, e).wait()
        expert(at["me"], e)
        return carry

    route(at["me"])
    lax.fori_loop(0, LOCAL_EXPERTS, first_expert, 0)
    down_load.wait()
    down()
    fin[...] = acc[...]

    def body(pos, carry):
        gather.before(pos, True)
        blk = pick(pos, ORDER_RS, at)
        route(blk)
        for e in range(LOCAL_EXPERTS):
            expert(blk, e)
        down()
        scatter.after(pos, acc, fin)
        return carry

    lax.fori_loop(1, N, body, 0)
    gather.finish()
    scatter.finish(fin, hidden_in, gain_ref, hidden_ref, normed_ref)


def experts(layer, u, router, ids, hidden, gain, w_gate, w_up, w_down, ident):
    width = LOCAL_EXPERTS * FF
    return pl.pallas_call(
        functools.partial(moe_kernel, layer),
        out_shape=RESIDUAL,
        in_specs=[VM] * 5 + [ANY] * 3, out_specs=(VM, VM),
        scratch_shapes=gather_scratch() + scatter_scratch() + [
            pltpu.VMEM((LOCAL_EXPERTS, D, FF), BF16), pltpu.VMEM((LOCAL_EXPERTS, D, FF), BF16),
            pltpu.VMEM((width, D), BF16), pltpu.VMEM((ROWS, width), BF16), pltpu.VMEM((ROWS, 128), F32),
            pltpu.SemaphoreType.DMA((3, LOCAL_EXPERTS))],
        compiler_params=comm_params(ident),
    )(u, router, ids, hidden, gain, w_gate, w_up, w_down.reshape(LAYERS, width, D))


TILE = 1024
TILES = VOCAB // TILE
LAST_TILE = 512


def fold(logits, column, target, stat):
    part = (logits * (1.0 / LOGIT_DIV)).reshape(TILE // 8, 8, ROWS)
    peak = stat[0]
    top = jnp.maximum(peak, jnp.max(part, axis=0))
    row = 8 * lax.broadcasted_iota(jnp.int32, part.shape, 0) + lax.broadcasted_iota(jnp.int32, part.shape, 1)
    stat[0] = top
    stat[1] = stat[1] * jnp.exp(peak - top) + jnp.sum(jnp.exp(part - top), axis=0)
    stat[2] = stat[2] + jnp.sum(jnp.where(row == target - column, part, 0.0), axis=0)


def head_kernel(f_ref, target_ref, embed_ref, probs_ref, last_ref, ubuf, send, recv, table, even, odd, stat, mine, theirs,
                share_send, share_recv, sem):
    def load(c):
        rows = pl.ds(pl.multiple_of(c * TILE, TILE), TILE)
        return pltpu.make_async_copy(embed_ref.at[rows], table.at[rows], sem.at[c])

    for c in range(TILES):
        load(c).start()
    at = places()
    entry_barrier(at, ORDER_AG[1:])
    gather = Gather(at, f_ref, ubuf, send, recv)
    gather.start(0, 2)
    ubuf[at["me"]] = f_ref[...]

    def tile_logits(blk, start):
        return lax.dot_general(table[pl.ds(start, TILE), :], ubuf[blk], (((1,), (1,)), ((), ())), preferred_element_type=F32)

    def begin():
        stat[0] = jnp.full((8, ROWS), -1e30, F32)
        stat[1] = jnp.zeros((8, ROWS), F32)
        stat[2] = jnp.zeros((8, ROWS), F32)

    def end(blk):
        peak = stat[0]
        top = jnp.max(peak, axis=0, keepdims=True)
        mine[0, pl.ds(blk, 1), :] = top
        mine[1, pl.ds(blk, 1), :] = jnp.sum(stat[1] * jnp.exp(peak - top), axis=0, keepdims=True)
        mine[2, pl.ds(blk, 1), :] = jnp.sum(stat[2], axis=0, keepdims=True)
        last_ref[blk] = ubuf[blk, ROWS - SEQS:ROWS, :]

    def first_tile(c, carry):
        load(c).wait()
        even[...] = tile_logits(at["me"], pl.multiple_of(c * TILE, TILE))
        fold(even[...], c * TILE, target_ref[at["me"]], stat)
        return carry

    begin()
    lax.fori_loop(0, TILES, first_tile, 0)
    end(at["me"])

    def body(pos, carry):
        gather.before(pos, False)
        blk = pick(pos, ORDER_AG, at)
        target = target_ref[blk]
        begin()
        bufs = (even, odd)
        even[...] = tile_logits(blk, 0)
        for c in range(1, TILES + 1):
            if c < TILES:
                bufs[c % 2][...] = tile_logits(blk, c * TILE)
            fold(bufs[(c - 1) % 2][...], (c - 1) * TILE, target, stat)
        end(blk)
        return carry

    lax.fori_loop(1, N, body, 0)
    gather.finish()
    me = at["me"]
    copies = [pltpu.make_async_remote_copy(
        src_ref=mine, dst_ref=theirs.at[shift], send_sem=share_send.at[shift], recv_sem=share_recv.at[shift],
        device_id={"tp": lax.rem(me + shift, N)}, device_id_type=MESH) for shift in range(1, N)]
    for item in copies:
        item.start()
    theirs[0] = mine[...]
    for item in copies:
        item.wait()
    peak = functools.reduce(jnp.maximum, [theirs[i, 0] for i in range(N)])
    total = sum(theirs[i, 1] * jnp.exp(theirs[i, 0] - peak) for i in range(N))
    picked = sum(theirs[i, 2] for i in range(N))
    probs_ref[...] = picked - peak - jnp.log(total)


def head(f, target, embed, ident):
    return pl.pallas_call(
        head_kernel,
        out_shape=(jax.ShapeDtypeStruct((N, ROWS), F32), jax.ShapeDtypeStruct((N, SEQS, D), BF16)),
        in_specs=[VM, VM, ANY], out_specs=(VM, VM),
        scratch_shapes=gather_scratch() + [
            pltpu.VMEM((VOCAB, D), BF16), pltpu.VMEM((TILE, ROWS), F32), pltpu.VMEM((TILE, ROWS), F32),
            pltpu.VMEM((3, 8, ROWS), F32), pltpu.VMEM((3, N, ROWS), F32), pltpu.VMEM((N, 3, N, ROWS), F32),
            pltpu.SemaphoreType.DMA((N,)), pltpu.SemaphoreType.DMA((N,)), pltpu.SemaphoreType.DMA((TILES,))],
        compiler_params=comm_params(ident),
    )(f, target, embed)


def last_kernel(f_ref, embed_ref, logits_ref):
    logits_ref[...] = lax.dot_general(f_ref[...], embed_ref[...], (((1,), (1,)), ((), ())),
                                      preferred_element_type=F32) * (1.0 / LOGIT_DIV)


def last_step(f, embed):
    return pl.pallas_call(
        last_kernel,
        out_shape=jax.ShapeDtypeStruct((BATCH, VOCAB), F32),
        grid=(VOCAB // LAST_TILE,),
        in_specs=[pl.BlockSpec((BATCH, D), lambda c: (0, 0)), pl.BlockSpec((LAST_TILE, D), lambda c: (c, 0))],
        out_specs=pl.BlockSpec((BATCH, LAST_TILE), lambda c: (0, c)),
        compiler_params=pltpu.CompilerParams(dimension_semantics=("arbitrary",), vmem_limit_bytes=VMEM_LIMIT),
    )(f, embed)


def by_block(values):
    return values.reshape(N, SEQS, values.shape[1]).transpose(0, 2, 1)


def solution(mesh):
    cache_spec = P(None, None, 'dp', None, 'tp', None)
    expert_spec = P(None, 'tp', None, None)
    in_specs = (P('dp', None), P('dp'), cache_spec, P(None, None, 'dp', None), P('tp', None), P(None, None), P(None, None, 'tp'), P(None, None, 'tp'), P(None, None, 'tp'), P(None, 'tp', None), P(None, None, None), expert_spec, expert_spec, expert_spec)
    out_specs = (P('dp', None), P('dp', 'tp'), cache_spec)

    def decode_local(tokens, start_pos, kv_cache, expert_ids, embed, norm_gain, w_query, w_key, w_value, w_out, w_router, w_gate, w_up, w_down):
        shard = lax.axis_index('tp')
        cache = kv_cache.transpose(0, 1, 2, 4, 5, 3).reshape(LAYERS, 2, BATCH, HEAD, CACHE)

        gains = norm_gain[:, None, :]
        ids = by_block(tokens[:, :STEPS]).reshape(-1)
        rows = local_rows(ids, shard, embed)
        hidden, normed = embed_sum(rows, gains[0], 0)

        pos = by_block(start_pos[:, None] + jnp.arange(STEPS)[None, :]).reshape(N, ROWS)
        inv_freq = ROPE_THETA ** (-2.0 * jnp.arange(HEAD // 2, dtype=F32) / HEAD)
        angles = pos.astype(F32)[:, :, None] * inv_freq
        cos, sin = jnp.cos(angles), jnp.sin(angles)
        cos = jnp.concatenate([cos] * 4, axis=-1)
        sin = jnp.concatenate([-sin, sin, -sin, sin], axis=-1)
        start_wide = jnp.broadcast_to(start_pos[:, None], (BATCH, 128))

        wq, wk, wv = (w.transpose(0, 2, 1) for w in (w_query, w_key, w_value))
        w_qkv = jnp.concatenate([wq, wk, wv, wv], axis=1)
        w_out_wide = jnp.concatenate([w_out, jnp.zeros((LAYERS, 64, D), BF16)], axis=1)

        first_expert = shard * LOCAL_EXPERTS
        turned = lax.rem(jnp.arange(EXPERTS) + first_expert, EXPERTS)
        router = jnp.take(w_router, turned, axis=2)
        router = jnp.concatenate([router, jnp.zeros((LAYERS, D, 128 - EXPERTS), BF16)], axis=2)
        routed = lax.rem(expert_ids + (EXPERTS - first_expert), EXPERTS)
        routed = routed.reshape(STEPS, LAYERS, N, SEQS, 8).transpose(1, 2, 0, 3, 4).reshape(LAYERS, N, ROWS, 8)

        new_cache = None
        for layer in range(LAYERS):
            hidden, normed, new_cache = attention(layer, normed, w_qkv[layer], cos, sin, start_wide, w_out_wide[layer], hidden,
                                                  gains[2 * layer + 1], cache, new_cache, 1 + 2 * layer)
            hidden, normed = experts(layer, normed, router[layer], routed[layer], hidden, gains[2 * layer + 2],
                                     w_gate, w_up, w_down, 2 + 2 * layer)

        target = by_block(tokens[:, 1:] - shard * VOCAB).reshape(N, 1, ROWS)
        log_probs, f_last = head(normed, target, embed, 5)
        logits = last_step(f_last.reshape(BATCH, D), embed)
        log_probs = log_probs.reshape(N, STEPS, SEQS).transpose(0, 2, 1).reshape(BATCH, STEPS)
        new_cache = new_cache.reshape(LAYERS, 2, BATCH, 1, HEAD, CACHE).transpose(0, 1, 2, 5, 3, 4)
        return log_probs, logits, new_cache

    return jax.shard_map(decode_local, mesh=mesh, in_specs=in_specs, out_specs=out_specs, check_vma=False)
```

```python
import functools

import jax
import jax.numpy as jnp
from jax import lax
from jax.experimental import pallas as pl
from jax.experimental.pallas import tpu as pltpu
from jax.sharding import PartitionSpec as P

EMBED_MULT = 12.0
ATT_SCALE = 0.015625
RESID_MULT = 0.22
LOGIT_DIV = 6.0
NORM_EPS = 1e-6
ROPE_THETA = 10000.0

D = 1536
HEAD = 64
BATCH = 512
STEPS = 4
LAYERS = 2
CACHE = 128
EXPERTS = 40
LOCAL_EXPERTS = 5
FF = 512
VOCAB = 6144
N = 8
SEQS = BATCH // N
ROWS = SEQS * STEPS
MESH = pl.DeviceIdType.MESH
F32 = jnp.float32
BF16 = jnp.bfloat16
VMEM_LIMIT = 60 * 1024 * 1024

ORDER_RS = ("sib", "bs", "a", "ds", "dg", "as", "b", "me")
ORDER_AG = ("me", "sib", "bs", "a", "ds", "dg", "as", "b")
ORDER_EMBED = ("sib", "ds", "dg", "bs", "a", "as", "b", "me")


def places():
    me = lax.axis_index("tp")
    k = lax.rem(me, 2)
    x = lax.rem(lax.div(me, 2), 2)
    y = lax.div(me, 4)
    step_x = 2 - 4 * x
    step_y = 4 - 8 * y
    a = me + step_x + k * (step_y - step_x)
    b = me + step_y + k * (step_x - step_y)
    dg = me + step_x + step_y
    s = 1 - 2 * k
    return {"me": me, "sib": me + s, "a": a, "as": a + s, "b": b, "bs": b + s, "dg": dg, "ds": dg + s}


def entry_barrier(at, names=("sib", "a", "b")):
    barrier = pltpu.get_barrier_semaphore()
    for name in names:
        pl.semaphore_signal(barrier, inc=1, device_id={"tp": at[name]}, device_id_type=MESH)
    pl.semaphore_wait(barrier, len(names))


def pick(pos, order, at):
    total = jnp.int32(0)
    for i, name in enumerate(order):
        total = total + jnp.where(pos == i, at[name], 0)
    return total


class Gather:
    def __init__(self, at, own, ubuf, send, recv):
        self.at, self.own, self.ubuf, self.send, self.recv = at, own, ubuf, send, recv

    def copy(self, src, origin, target, slot):
        return pltpu.make_async_remote_copy(
            src_ref=src, dst_ref=self.ubuf.at[origin], send_sem=self.send.at[slot], recv_sem=self.recv.at[origin],
            device_id={"tp": target}, device_id_type=MESH)

    def item(self, slot):
        at = self.at
        if slot < 3:
            return self.copy(self.own, at["me"], at[("a", "b", "sib")[slot]], slot)
        name, target = (("a", "b"), ("a", "sib"), ("b", "sib"), ("dg", "sib"))[slot - 3]
        return self.copy(self.ubuf.at[at[name]], at[name], at[target], slot)

    def start(self, *slots):
        for slot in slots:
            self.item(slot).start()

    def arrive(self, name):
        origin = self.at[name]
        self.copy(self.own, origin, self.at["sib"], 0).wait_recv()

    def before(self, pos, order):
        @pl.when(pos == order.index("sib"))
        def _():
            self.arrive("sib")

        @pl.when(pos == order.index("bs"))
        def _():
            self.arrive("a")
            self.start(3, 4, 1)
            self.arrive("bs")

        @pl.when(pos == order.index("ds"))
        def _():
            self.arrive("dg")
            self.start(6)
            self.arrive("ds")

        @pl.when(pos == order.index("as"))
        def _():
            self.arrive("b")
            self.start(5)
            self.arrive("as")

    def finish(self):
        for slot in range(7):
            self.item(slot).wait_send()


class Scatter:
    def __init__(self, at, tbuf, rbuf, send, recv):
        self.at, self.tbuf, self.rbuf, self.send, self.recv = at, tbuf, rbuf, send, recv

    def copy(self, slot, target):
        return pltpu.make_async_remote_copy(
            src_ref=self.tbuf.at[slot], dst_ref=self.rbuf.at[slot], send_sem=self.send.at[slot],
            recv_sem=self.recv.at[slot], device_id={"tp": target}, device_id_type=MESH)

    def arrive(self, slot):
        self.copy(slot, self.at["sib"]).wait_recv()

    def after(self, pos, acc, far_first=False):
        at = self.at

        @pl.when((pos == 0) | (pos == 1) | (pos == 3) | (pos == 5))
        def _():
            slot = lax.div(pos + 1, 2)
            self.tbuf[slot] = acc[...].astype(BF16)
            self.copy(slot, at["sib"]).start()

        @pl.when((pos == 2) | (pos == 4))
        def _():
            slot = lax.div(pos, 2)
            out = 6 - slot if far_first else slot + 3
            self.arrive(slot)
            self.tbuf[out] = (acc[...] + self.rbuf[slot].astype(F32)).astype(BF16)
            self.copy(out, at["a"]).start()

        @pl.when(pos == 6)
        def _():
            self.arrive(3)
            self.arrive(5)
            self.tbuf[6] = (acc[...] + self.rbuf[3].astype(F32) + self.rbuf[5].astype(F32)).astype(BF16)
            self.copy(6, at["b"]).start()

    def finish(self, acc, hidden_in, gain, hidden_ref, normed_ref):
        self.arrive(0)
        self.arrive(4)
        self.arrive(6)

        def chunk(c, carry):
            rows = pl.ds(pl.multiple_of(c * 32, 32), 32)
            total = acc[rows, :]
            for slot in (0, 4, 6):
                total = total + self.rbuf[slot, rows, :].astype(F32)
            total = total.astype(BF16).astype(F32)
            if hidden_in is None:
                hidden = EMBED_MULT * total
            else:
                hidden = hidden_in[rows, :] + RESID_MULT * total
            hidden_ref[rows, :] = hidden
            mean_sq = jnp.mean(hidden * hidden, axis=1, keepdims=True)
            normed_ref[rows, :] = (hidden * lax.rsqrt(mean_sq + NORM_EPS) * gain).astype(BF16)
            return carry

        lax.fori_loop(0, ROWS // 32, chunk, 0)
        for slot in range(7):
            self.copy(slot, self.at["sib"]).wait_send()


def gather_scratch():
    return [pltpu.VMEM((N, ROWS, D), BF16), pltpu.SemaphoreType.DMA((7,)), pltpu.SemaphoreType.DMA((N,))]


def scatter_scratch():
    return [pltpu.VMEM((ROWS, D), F32), pltpu.VMEM((7, ROWS, D), BF16),
            pltpu.VMEM((7, ROWS, D), BF16), pltpu.SemaphoreType.DMA((7,)), pltpu.SemaphoreType.DMA((7,))]


VM = pl.BlockSpec(memory_space=pltpu.VMEM)
RESIDUAL = (jax.ShapeDtypeStruct((ROWS, D), F32), jax.ShapeDtypeStruct((ROWS, D), BF16))
ANY = pl.BlockSpec(memory_space=pl.ANY)


def comm_params(ident):
    return pltpu.CompilerParams(collective_id=ident, has_side_effects=True, vmem_limit_bytes=VMEM_LIMIT)


def rows_kernel(count_ref, token_ref, row_ref, embed_ref, out_ref, buf, wide, sem):
    wide[...] = jnp.zeros_like(wide)
    count = count_ref[0]
    slots = buf.shape[0]

    def chunk(c, carry):
        base = c * slots
        width = jnp.minimum(slots, count - base)

        def issue(j, carry):
            pltpu.make_async_copy(embed_ref.at[lax.div(row_ref[base + j], 8)], buf.at[j], sem).start()
            return carry

        def place(j, carry):
            pltpu.make_async_copy(embed_ref.at[0], buf.at[j], sem).wait()
            return carry

        def move(i, carry):
            for j in range(4):
                spot = base + 4 * i + j
                sub = lax.rem(row_ref[spot], 8)
                block = buf[4 * i + j].astype(F32)
                keep = lax.broadcasted_iota(jnp.int32, block.shape, 0) == sub
                line = jnp.sum(jnp.where(keep, block, 0.0), axis=0, keepdims=True)
                wide[pl.ds(token_ref[spot], 1), :] = line
            return carry

        lax.fori_loop(0, width, issue, 0)
        lax.fori_loop(0, width, place, 0)
        lax.fori_loop(0, lax.div(width + 3, 4), move, 0)
        return carry

    lax.fori_loop(0, lax.div(count + slots - 1, slots), chunk, 0)
    out_ref[...] = wide[0:N * ROWS, :].astype(BF16)


def local_rows(ids, shard, embed):
    total = N * ROWS
    local = ids - shard * VOCAB
    inside = (local >= 0) & (local < VOCAB)
    rank = jnp.cumsum(inside.astype(jnp.int32)) - 1
    rank = jnp.where(inside, rank, -1)
    hit = rank[None, :] == jnp.arange(total)[:, None]
    token = jnp.sum(jnp.where(hit, jnp.arange(total)[None, :] - total, 0), axis=1) + total
    row = jnp.sum(jnp.where(hit, local[None, :], 0), axis=1)
    count = jnp.sum(inside.astype(jnp.int32)).reshape(1)
    return pl.pallas_call(
        rows_kernel,
        out_shape=jax.ShapeDtypeStruct((total, D), BF16),
        grid_spec=pltpu.PrefetchScalarGridSpec(
            num_scalar_prefetch=3, grid=(1,),
            in_specs=[ANY],
            out_specs=pl.BlockSpec((total, D), lambda i, *_: (0, 0)),
            scratch_shapes=[pltpu.VMEM((256, 8, D), BF16), pltpu.VMEM((total + 8, D), F32), pltpu.SemaphoreType.DMA]),
        compiler_params=pltpu.CompilerParams(vmem_limit_bytes=VMEM_LIMIT),
    )(count, token, row, embed.reshape(VOCAB // 8, 8, D))


def embed_kernel(rows_ref, gains_ref, hidden_ref, normed_ref, acc, tbuf, rbuf, send, recv):
    at = places()
    entry_barrier(at)
    scatter = Scatter(at, tbuf, rbuf, send, recv)

    def body(pos, carry):
        acc[...] = rows_ref[pick(pos, ORDER_EMBED, at)].astype(F32)
        scatter.after(pos, acc, far_first=True)
        return carry

    lax.fori_loop(0, N, body, 0)
    scatter.finish(acc, None, gains_ref[0:1, :], hidden_ref, normed_ref)


def embed_sum(rows, gains, ident):
    return pl.pallas_call(
        embed_kernel,
        out_shape=RESIDUAL,
        in_specs=[VM, VM], out_specs=(VM, VM),
        scratch_shapes=scatter_scratch(),
        compiler_params=comm_params(ident),
    )(rows.reshape(N, ROWS, D), gains)


HALF = 32
SLOTS = 4


def attend_half(base, start_ref, first_seq, qk, vv, planes, mixed_out):
    lane = lax.broadcasted_iota(jnp.int32, (8, 128), 1)
    row = lax.broadcasted_iota(jnp.int32, (8, 128), 0)
    first = lane < HEAD
    own = [(2 * j + lax.div(lane, HEAD)) == row for j in range(4)]
    groups = range(HALF // 8)

    def spread(twice):
        return jnp.concatenate([jnp.where(own[j], twice, 0.0) for j in range(4)], axis=1)

    starts = [start_ref[pl.ds(pl.multiple_of(first_seq + base + 8 * g, 8), 8), :] for g in groups]
    query, updates = [], []
    for g in groups:
        queries, keys, vals, hot = [], [], [], []
        for s in range(STEPS):
            span = pl.ds(pl.multiple_of(s * SEQS + base + 8 * g, 8), 8)
            left, right = qk[span, 0:128], qk[span, 128:256]
            left_r, right_r = pltpu.roll(left, HEAD, 1), pltpu.roll(right, HEAD, 1)
            queries += [spread(jnp.where(first, left, left_r)), spread(jnp.where(first, left_r, left)),
                        spread(jnp.where(first, right, right_r))]
            keys.append(spread(jnp.where(first, right_r, right)))
            vals.append(spread(vv[span, :]))
            hot.append(jnp.where(lane == starts[g] + s, 1.0, 0.0))
        query.append(jnp.concatenate(queries, axis=0).astype(BF16))
        hot_all = jnp.concatenate(hot, axis=0).astype(BF16)
        updates.append([
            lax.dot_general(jnp.concatenate(entry, axis=0).astype(BF16), hot_all, (((0,), (0,)), ((), ())),
                            preferred_element_type=F32) for entry in (keys, vals)])
    for g in groups:
        span = pl.ds(base + 8 * g, 8)
        fresh = jnp.where((lane >= starts[g]) & (lane < starts[g] + STEPS), 1.0, 0.0)
        fresh = jnp.broadcast_to(fresh[:, None, :], (8, HEAD, 128)) > 0.5
        for kind in range(2):
            old = planes[kind, span].astype(F32)
            planes[kind, span] = jnp.where(fresh, updates[g][kind].reshape(8, HEAD, 128), old).astype(BF16)
    scores = [jnp.dot(query[g], planes[0, pl.ds(base + 8 * g, 8)].reshape(8 * HEAD, 128), preferred_element_type=F32)
              for g in groups]
    probs = []
    for g in groups:
        valid = [jnp.where(lane <= starts[g] + s, 0.0, -jnp.inf) for s in range(STEPS)]
        score = scores[g] * ATT_SCALE + jnp.concatenate([valid[s] for s in range(STEPS) for h in range(3)], axis=0)
        weight = jnp.exp(score - jnp.max(score, axis=1, keepdims=True))
        probs.append((weight / jnp.sum(weight, axis=1, keepdims=True)).astype(BF16))
    mixed = [lax.dot_general(probs[g], planes[1, pl.ds(base + 8 * g, 8)].reshape(8 * HEAD, 128),
                             (((1,), (1,)), ((), ())), preferred_element_type=F32) for g in groups]
    for g in groups:
        for s in range(STEPS):
            span = pl.ds(pl.multiple_of(s * SEQS + base + 8 * g, 8), 8)
            heads = []
            for h in range(3):
                part = mixed[g][8 * (3 * s + h):8 * (3 * s + h) + 8, :]
                total = sum(jnp.where(own[j], part[:, 128 * j:128 * j + 128], 0.0) for j in range(4))
                heads.append(total + pltpu.roll(total, HEAD, 1))
            mixed_out[span, 0:128] = jnp.where(first, heads[0], heads[1])
            mixed_out[span, 128:256] = heads[2]


def attn_kernel(layer, u_ref, cos_ref, sin_ref, start_ref, hidden_in, gains_ref, wq_ref, wk_ref, wv_ref, wo_ref, cache_ref,
                *rest):
    if layer > 0:
        rest = rest[1:]
    (hidden_ref, normed_ref, new_ref, ubuf, ag_send, ag_recv, acc, tbuf, rbuf, rs_send, rs_recv,
     qk, vv, mixed, planes, w_qkv, w_out, in_sem, out_sem, w_sem) = rest
    at = places()
    weights = [
        pltpu.make_async_copy(wq_ref.at[layer], w_qkv.at[0:192], w_sem.at[0]),
        pltpu.make_async_copy(wk_ref.at[layer], w_qkv.at[192:256], w_sem.at[1]),
        pltpu.make_async_copy(wv_ref.at[layer], w_qkv.at[256:320], w_sem.at[2]),
        pltpu.make_async_copy(wv_ref.at[layer], w_qkv.at[320:384], w_sem.at[3]),
        pltpu.make_async_copy(wo_ref.at[layer], w_out.at[0:192], w_sem.at[4])]
    for item in weights:
        item.start()
    w_out[192:256, :] = jnp.zeros((64, D), BF16)

    def plane_span(pos):
        return pl.ds(pick(pos, ORDER_RS, at) * SEQS, SEQS)

    def load(pos):
        slot = lax.rem(pos, SLOTS)
        return pltpu.make_async_copy(cache_ref.at[layer, :, plane_span(pos)], planes.at[slot], in_sem.at[slot])

    def store(pos):
        slot = lax.rem(pos, SLOTS)
        return pltpu.make_async_copy(planes.at[slot], new_ref.at[layer, :, plane_span(pos)], out_sem.at[slot])

    load(jnp.int32(0)).start()
    load(jnp.int32(1)).start()
    entry_barrier(at)
    gather = Gather(at, u_ref, ubuf, ag_send, ag_recv)
    scatter = Scatter(at, tbuf, rbuf, rs_send, rs_recv)
    gather.start(0, 2)
    ubuf[at["me"]] = u_ref[...]
    for item in weights:
        item.wait()

    def body(pos, carry):
        gather.before(pos, ORDER_RS)
        blk = pick(pos, ORDER_RS, at)

        @pl.when(pos >= 2)
        def _():
            store(pos - 2).wait()

        @pl.when(pos < N - 2)
        def _():
            load(pos + 2).start()

        out = lax.dot_general(ubuf[blk], w_qkv[...], (((1,), (1,)), ((), ())), preferred_element_type=F32)
        cos = cos_ref[blk]
        sin = sin_ref[blk]
        low = lax.rem(lax.broadcasted_iota(jnp.int32, (ROWS, 128), 1), HEAD) < HEAD // 2
        for half in range(2):
            part = out[:, half * 128:(half + 1) * 128]
            swapped = jnp.where(low, pltpu.roll(part, 128 - HEAD // 2, 1), pltpu.roll(part, HEAD // 2, 1))
            qk[:, half * 128:(half + 1) * 128] = (part * cos + swapped * sin).astype(BF16).astype(F32)
        vv[...] = out[:, 256:384].astype(BF16).astype(F32)
        load(pos).wait()

        def half_block(i, carry):
            attend_half(i * HALF, start_ref, blk * SEQS, qk, vv, planes.at[lax.rem(pos, SLOTS)], mixed)
            return carry

        lax.fori_loop(0, SEQS // HALF, half_block, 0)
        store(pos).start()
        acc[...] = jnp.dot(mixed[...].astype(BF16), w_out[...], preferred_element_type=F32)
        scatter.after(pos, acc)
        return carry

    lax.fori_loop(0, N, body, 0)
    store(jnp.int32(N - 2)).wait()
    store(jnp.int32(N - 1)).wait()
    gather.finish()
    scatter.finish(acc, hidden_in, gains_ref[2 * layer + 1:2 * layer + 2, :], hidden_ref, normed_ref)


def attention(layer, u, cos, sin, start_wide, hidden, gains, weights, cache, new_cache, ident):
    args = [u, cos, sin, start_wide, hidden, gains, *weights, cache]
    in_specs = [VM] * 6 + [ANY] * 5
    aliases = {}
    if new_cache is not None:
        args.append(new_cache)
        in_specs.append(ANY)
        aliases = {11: 2}
    return pl.pallas_call(
        functools.partial(attn_kernel, layer),
        out_shape=RESIDUAL + (jax.ShapeDtypeStruct(cache.shape, BF16),),
        in_specs=in_specs, out_specs=(VM, VM, ANY),
        scratch_shapes=gather_scratch() + scatter_scratch() + [
            pltpu.VMEM((ROWS, 256), F32), pltpu.VMEM((ROWS, 128), F32), pltpu.VMEM((ROWS, 256), F32),
            pltpu.VMEM((SLOTS, 2, SEQS, HEAD, CACHE), BF16), pltpu.VMEM((384, D), BF16), pltpu.VMEM((256, D), BF16),
            pltpu.SemaphoreType.DMA((SLOTS,)), pltpu.SemaphoreType.DMA((SLOTS,)), pltpu.SemaphoreType.DMA((5,))],
        input_output_aliases=aliases,
        compiler_params=comm_params(ident),
    )(*args)


def moe_kernel(layer, u_ref, router_ref, ids_ref, hidden_in, gains_ref, gate_hbm, up_hbm, down_hbm, hidden_ref, normed_ref,
               ubuf, ag_send, ag_recv, acc, tbuf, rbuf, rs_send, rs_recv, gate_v, up_v, down_v, hidden, gates, w_sem):
    def load(kind, e):
        src, dst = ((gate_hbm, gate_v), (up_hbm, up_v))[kind]
        return pltpu.make_async_copy(src.at[layer, e], dst.at[e], w_sem.at[kind, e])

    down_load = pltpu.make_async_copy(down_hbm.at[layer], down_v, w_sem.at[2, 0])
    for e in range(LOCAL_EXPERTS):
        load(0, e).start()
        load(1, e).start()
    down_load.start()
    at = places()
    entry_barrier(at)
    gather = Gather(at, u_ref, ubuf, ag_send, ag_recv)
    scatter = Scatter(at, tbuf, rbuf, rs_send, rs_recv)
    gather.start(0, 2)
    ubuf[at["me"]] = u_ref[...]
    lane = lax.broadcasted_iota(jnp.int32, (ROWS, EXPERTS), 1)

    def route(blk):
        ids = ids_ref[blk]
        chosen = lane == ids[:, 0:1]
        for j in range(1, 8):
            chosen = chosen | (lane == ids[:, j:j + 1])
        score = lax.dot_general(ubuf[blk], router_ref[layer], (((1,), (1,)), ((), ())), preferred_element_type=F32)
        masked = jnp.where(chosen, score, -jnp.inf)
        weight = jnp.exp(masked - jnp.max(masked, axis=1, keepdims=True))
        gates[...] = weight / jnp.sum(weight, axis=1, keepdims=True)

    def inner(blk, e):
        return (jnp.dot(ubuf[blk], gate_v[e], preferred_element_type=F32),
                jnp.dot(ubuf[blk], up_v[e], preferred_element_type=F32))

    def activate(e, gate_act, up_act):
        share = jnp.sum(jnp.where(lane == at["me"] * LOCAL_EXPERTS + e, gates[...], 0.0), axis=1, keepdims=True)
        z = gate_act * jax.nn.sigmoid(gate_act) * up_act * share
        start = e * FF if isinstance(e, int) else pl.multiple_of(e * FF, FF)
        hidden[:, pl.ds(start, FF)] = z.astype(BF16)

    def down():
        for c in range(D // 512):
            cols = slice(c * 512, c * 512 + 512)
            acc[:, cols] = jnp.dot(hidden[...], down_v[:, cols], preferred_element_type=F32)

    def first_expert(e, carry):
        load(0, e).wait()
        load(1, e).wait()
        activate(e, *inner(at["sib"], e))
        return carry

    gather.before(jnp.int32(0), ORDER_RS)
    route(at["sib"])
    lax.fori_loop(0, LOCAL_EXPERTS, first_expert, 0)
    down_load.wait()
    down()
    scatter.after(jnp.int32(0), acc)

    def body(pos, carry):
        gather.before(pos, ORDER_RS)
        blk = pick(pos, ORDER_RS, at)
        acts = inner(blk, 0)
        route(blk)
        for e in range(LOCAL_EXPERTS):
            following = inner(blk, e + 1) if e + 1 < LOCAL_EXPERTS else None
            activate(e, *acts)
            acts = following
        down()
        scatter.after(pos, acc)
        return carry

    lax.fori_loop(1, N, body, 0)
    gather.finish()
    scatter.finish(acc, hidden_in, gains_ref[2 * layer + 2:2 * layer + 3, :], hidden_ref, normed_ref)


def experts(layer, u, router, ids, hidden, gains, w_gate, w_up, w_down, ident):
    width = LOCAL_EXPERTS * FF
    return pl.pallas_call(
        functools.partial(moe_kernel, layer),
        out_shape=RESIDUAL,
        in_specs=[VM] * 5 + [ANY] * 3, out_specs=(VM, VM),
        scratch_shapes=gather_scratch() + scatter_scratch() + [
            pltpu.VMEM((LOCAL_EXPERTS, D, FF), BF16), pltpu.VMEM((LOCAL_EXPERTS, D, FF), BF16),
            pltpu.VMEM((width, D), BF16), pltpu.VMEM((ROWS, width), BF16), pltpu.VMEM((ROWS, EXPERTS), F32),
            pltpu.SemaphoreType.DMA((3, LOCAL_EXPERTS))],
        compiler_params=comm_params(ident),
    )(u, router, ids, hidden, gains, w_gate, w_up, w_down.reshape(LAYERS, width, D))


TILE = 1024
TILES = VOCAB // TILE
LAST_TILE = 384


def fold(logits, column, target, stat):
    part = (logits * (1.0 / LOGIT_DIV)).reshape(TILE // 8, 8, ROWS)
    peak = stat[0]
    top = jnp.maximum(peak, jnp.max(part, axis=0))
    row = 8 * lax.broadcasted_iota(jnp.int32, part.shape, 0) + lax.broadcasted_iota(jnp.int32, part.shape, 1)
    stat[0] = top
    stat[1] = stat[1] * jnp.exp(peak - top) + jnp.sum(jnp.exp(part - top), axis=0)
    stat[2] = stat[2] + jnp.sum(jnp.where(row == target - column, part, 0.0), axis=0)


def head_kernel(f_ref, target_ref, embed_ref, probs_ref, last_ref, ubuf, send, recv, table, even, odd, stat, mine, theirs,
                share_send, share_recv, sem):
    def load(c):
        rows = pl.ds(pl.multiple_of(c * TILE, TILE), TILE)
        return pltpu.make_async_copy(embed_ref.at[rows], table.at[rows], sem.at[c])

    for c in range(TILES):
        load(c).start()
    at = places()
    entry_barrier(at, ORDER_AG[1:])
    gather = Gather(at, f_ref, ubuf, send, recv)
    gather.start(0, 2)
    ubuf[at["me"]] = f_ref[...]

    def tile_logits(blk, start):
        return lax.dot_general(table[pl.ds(start, TILE), :], ubuf[blk], (((1,), (1,)), ((), ())), preferred_element_type=F32)

    def begin():
        stat[0] = jnp.full((8, ROWS), -1e30, F32)
        stat[1] = jnp.zeros((8, ROWS), F32)
        stat[2] = jnp.zeros((8, ROWS), F32)

    def end(blk):
        peak = stat[0]
        top = jnp.max(peak, axis=0, keepdims=True)
        mine[0, pl.ds(blk, 1), :] = top
        mine[1, pl.ds(blk, 1), :] = jnp.sum(stat[1] * jnp.exp(peak - top), axis=0, keepdims=True)
        mine[2, pl.ds(blk, 1), :] = jnp.sum(stat[2], axis=0, keepdims=True)
        last_ref[blk] = ubuf[blk, ROWS - SEQS:ROWS, :]

    def first_tile(c, carry):
        load(c).wait()
        even[...] = tile_logits(at["me"], pl.multiple_of(c * TILE, TILE))
        fold(even[...], c * TILE, target_ref[at["me"]], stat)
        return carry

    begin()
    lax.fori_loop(0, TILES, first_tile, 0)
    end(at["me"])

    def body(pos, carry):
        gather.before(pos, ORDER_AG)
        blk = pick(pos, ORDER_AG, at)
        target = target_ref[blk]
        begin()
        bufs = (even, odd)
        even[...] = tile_logits(blk, 0)
        for c in range(1, TILES + 1):
            if c < TILES:
                bufs[c % 2][...] = tile_logits(blk, c * TILE)
            fold(bufs[(c - 1) % 2][...], (c - 1) * TILE, target, stat)
        end(blk)
        return carry

    lax.fori_loop(1, N, body, 0)
    gather.finish()
    me = at["me"]
    copies = [pltpu.make_async_remote_copy(
        src_ref=mine, dst_ref=theirs.at[shift], send_sem=share_send.at[shift], recv_sem=share_recv.at[shift],
        device_id={"tp": lax.rem(me + shift, N)}, device_id_type=MESH) for shift in range(1, N)]
    for item in copies:
        item.start()
    theirs[0] = mine[...]
    for item in copies:
        item.wait()
    peak = functools.reduce(jnp.maximum, [theirs[i, 0] for i in range(N)])
    total = sum(theirs[i, 1] * jnp.exp(theirs[i, 0] - peak) for i in range(N))
    picked = sum(theirs[i, 2] for i in range(N))
    probs_ref[...] = picked - peak - jnp.log(total)


def head(f, target, embed, ident):
    return pl.pallas_call(
        head_kernel,
        out_shape=(jax.ShapeDtypeStruct((N, ROWS), F32), jax.ShapeDtypeStruct((N, SEQS, D), BF16)),
        in_specs=[VM, VM, ANY], out_specs=(VM, VM),
        scratch_shapes=gather_scratch() + [
            pltpu.VMEM((VOCAB, D), BF16), pltpu.VMEM((TILE, ROWS), F32), pltpu.VMEM((TILE, ROWS), F32),
            pltpu.VMEM((3, 8, ROWS), F32), pltpu.VMEM((3, N, ROWS), F32), pltpu.VMEM((N, 3, N, ROWS), F32),
            pltpu.SemaphoreType.DMA((N,)), pltpu.SemaphoreType.DMA((N,)), pltpu.SemaphoreType.DMA((TILES,))],
        compiler_params=comm_params(ident),
    )(f, target, embed)


def last_kernel(f_ref, embed_ref, cache_ref, logits_ref, new_ref):
    logits_ref[...] = lax.dot_general(f_ref[...], embed_ref[...], (((1,), (1,)), ((), ())),
                                      preferred_element_type=F32) * (1.0 / LOGIT_DIV)
    new_ref[...] = cache_ref[...]


def last_step(f, embed, cache):
    steps = VOCAB // LAST_TILE
    flat = cache.reshape(LAYERS * 2 * BATCH, HEAD, CACHE)
    plane_spec = pl.BlockSpec((flat.shape[0] // steps, HEAD, CACHE), lambda c: (c, 0, 0))
    logits, flat = pl.pallas_call(
        last_kernel,
        out_shape=(jax.ShapeDtypeStruct((BATCH, VOCAB), F32), jax.ShapeDtypeStruct(flat.shape, BF16)),
        grid=(steps,),
        in_specs=[pl.BlockSpec((BATCH, D), lambda c: (0, 0)), pl.BlockSpec((LAST_TILE, D), lambda c: (c, 0)), plane_spec],
        out_specs=(pl.BlockSpec((BATCH, LAST_TILE), lambda c: (0, c)), plane_spec),
        compiler_params=pltpu.CompilerParams(dimension_semantics=("arbitrary",), vmem_limit_bytes=VMEM_LIMIT),
    )(f, embed, flat)
    return logits, flat.reshape(cache.shape)


def by_block(values):
    return values.reshape(N, SEQS, values.shape[1]).transpose(0, 2, 1)


def solution(mesh):
    cache_spec = P(None, None, 'dp', None, 'tp', None)
    expert_spec = P(None, 'tp', None, None)
    in_specs = (P('dp', None), P('dp'), cache_spec, P(None, None, 'dp', None), P('tp', None), P(None, None), P(None, None, 'tp'), P(None, None, 'tp'), P(None, None, 'tp'), P(None, 'tp', None), P(None, None, None), expert_spec, expert_spec, expert_spec)
    out_specs = (P('dp', None), P('dp', 'tp'), cache_spec)

    def decode_local(tokens, start_pos, kv_cache, expert_ids, embed, norm_gain, w_query, w_key, w_value, w_out, w_router, w_gate, w_up, w_down):
        shard = lax.axis_index('tp')
        cache = kv_cache.transpose(0, 1, 2, 4, 5, 3).reshape(LAYERS, 2, BATCH, HEAD, CACHE)

        ids = by_block(tokens[:, :STEPS]).reshape(-1)
        rows = local_rows(ids, shard, embed)
        hidden, normed = embed_sum(rows, norm_gain, 0)

        pos = by_block(start_pos[:, None] + jnp.arange(STEPS)[None, :]).reshape(N, ROWS)
        inv_freq = ROPE_THETA ** (-2.0 * jnp.arange(HEAD // 2, dtype=F32) / HEAD)
        angles = pos.astype(F32)[:, :, None] * inv_freq
        cos, sin = jnp.cos(angles), jnp.sin(angles)
        cos = jnp.concatenate([cos] * 4, axis=-1)
        sin = jnp.concatenate([-sin, sin, -sin, sin], axis=-1)
        start_wide = jnp.broadcast_to(start_pos[:, None], (BATCH, 128))

        weights = [w.transpose(0, 2, 1) for w in (w_query, w_key, w_value)] + [w_out]
        router = w_router.transpose(0, 2, 1)
        routed = expert_ids.reshape(STEPS, LAYERS, N, SEQS, 8).transpose(1, 2, 0, 3, 4).reshape(LAYERS, N, ROWS, 8)

        new_cache = None
        for layer in range(LAYERS):
            hidden, normed, new_cache = attention(layer, normed, cos, sin, start_wide, hidden, norm_gain, weights, cache, new_cache,
                                                  1 + 2 * layer)
            hidden, normed = experts(layer, normed, router, routed[layer], hidden, norm_gain, w_gate, w_up, w_down, 2 + 2 * layer)

        target = by_block(tokens[:, 1:] - shard * VOCAB).reshape(N, 1, ROWS)
        log_probs, f_last = head(normed, target, embed, 5)
        logits, new_cache = last_step(f_last.reshape(BATCH, D), embed, new_cache)
        log_probs = log_probs.reshape(N, STEPS, SEQS).transpose(0, 2, 1).reshape(BATCH, STEPS)
        new_cache = new_cache.reshape(LAYERS, 2, BATCH, 1, HEAD, CACHE).transpose(0, 1, 2, 5, 3, 4)
        return log_probs, logits, new_cache

    return jax.shard_map(decode_local, mesh=mesh, in_specs=in_specs, out_specs=out_specs, check_vma=False)
```

```python
import functools

import jax
import jax.numpy as jnp
from jax import lax
from jax.experimental import pallas as pl
from jax.experimental.pallas import tpu as pltpu
from jax.sharding import PartitionSpec as P

EMBED_MULT = 12.0
ATT_SCALE = 0.015625
RESID_MULT = 0.22
LOGIT_DIV = 6.0
NORM_EPS = 1e-6
ROPE_THETA = 10000.0

D = 1536
HEAD = 64
BATCH = 512
STEPS = 4
LAYERS = 2
CACHE = 128
EXPERTS = 40
LOCAL_EXPERTS = 5
FF = 512
VOCAB = 6144
N = 8
SEQS = BATCH // N
ROWS = SEQS * STEPS
MESH = pl.DeviceIdType.MESH
F32 = jnp.float32
BF16 = jnp.bfloat16
VMEM_LIMIT = 60 * 1024 * 1024

ORDER_RS = ("sib", "bs", "a", "ds", "dg", "as", "b", "me")
ORDER_AG = ("me", "sib", "bs", "a", "ds", "dg", "as", "b")
ORDER_EMBED = ("sib", "ds", "dg", "bs", "a", "as", "b", "me")


def places():
    me = lax.axis_index("tp")
    k = lax.rem(me, 2)
    x = lax.rem(lax.div(me, 2), 2)
    y = lax.div(me, 4)
    step_x = 2 - 4 * x
    step_y = 4 - 8 * y
    a = me + step_x + k * (step_y - step_x)
    b = me + step_y + k * (step_x - step_y)
    dg = me + step_x + step_y
    s = 1 - 2 * k
    return {"me": me, "sib": me + s, "a": a, "as": a + s, "b": b, "bs": b + s, "dg": dg, "ds": dg + s}


def entry_barrier(at, names=("sib", "a", "b")):
    barrier = pltpu.get_barrier_semaphore()
    for name in names:
        pl.semaphore_signal(barrier, inc=1, device_id={"tp": at[name]}, device_id_type=MESH)
    pl.semaphore_wait(barrier, len(names))


def pick(pos, order, at):
    total = jnp.int32(0)
    for i, name in enumerate(order):
        total = total + jnp.where(pos == i, at[name], 0)
    return total


class Gather:
    def __init__(self, at, own, ubuf, send, recv):
        self.at, self.own, self.ubuf, self.send, self.recv = at, own, ubuf, send, recv

    def copy(self, src, origin, target, slot):
        return pltpu.make_async_remote_copy(
            src_ref=src, dst_ref=self.ubuf.at[origin], send_sem=self.send.at[slot], recv_sem=self.recv.at[origin],
            device_id={"tp": target}, device_id_type=MESH)

    def item(self, slot):
        at = self.at
        if slot < 3:
            return self.copy(self.own, at["me"], at[("a", "b", "sib")[slot]], slot)
        name, target = (("a", "b"), ("a", "sib"), ("b", "sib"), ("dg", "sib"))[slot - 3]
        return self.copy(self.ubuf.at[at[name]], at[name], at[target], slot)

    def start(self, *slots):
        for slot in slots:
            self.item(slot).start()

    def arrive(self, name):
        origin = self.at[name]
        self.copy(self.own, origin, self.at["sib"], 0).wait_recv()

    def before(self, pos, order):
        @pl.when(pos == order.index("sib"))
        def _():
            self.arrive("sib")

        @pl.when(pos == order.index("bs"))
        def _():
            self.arrive("a")
            self.start(3, 4, 1)
            self.arrive("bs")

        @pl.when(pos == order.index("ds"))
        def _():
            self.arrive("dg")
            self.start(6)
            self.arrive("ds")

        @pl.when(pos == order.index("as"))
        def _():
            self.arrive("b")
            self.start(5)
            self.arrive("as")

    def finish(self):
        for slot in range(7):
            self.item(slot).wait_send()


class Scatter:
    def __init__(self, at, tbuf, rbuf, send, recv):
        self.at, self.tbuf, self.rbuf, self.send, self.recv = at, tbuf, rbuf, send, recv

    def copy(self, slot, target):
        return pltpu.make_async_remote_copy(
            src_ref=self.tbuf.at[slot], dst_ref=self.rbuf.at[slot], send_sem=self.send.at[slot],
            recv_sem=self.recv.at[slot], device_id={"tp": target}, device_id_type=MESH)

    def arrive(self, slot):
        self.copy(slot, self.at["sib"]).wait_recv()

    def after(self, pos, acc, far_first=False):
        at = self.at

        @pl.when((pos == 0) | (pos == 1) | (pos == 3) | (pos == 5))
        def _():
            slot = lax.div(pos + 1, 2)
            self.tbuf[slot] = acc[...].astype(BF16)
            self.copy(slot, at["sib"]).start()

        @pl.when((pos == 2) | (pos == 4))
        def _():
            slot = lax.div(pos, 2)
            out = 6 - slot if far_first else slot + 3
            self.arrive(slot)
            self.tbuf[out] = (acc[...] + self.rbuf[slot].astype(F32)).astype(BF16)
            self.copy(out, at["a"]).start()

        @pl.when(pos == 6)
        def _():
            self.arrive(3)
            self.arrive(5)
            self.tbuf[6] = (acc[...] + self.rbuf[3].astype(F32) + self.rbuf[5].astype(F32)).astype(BF16)
            self.copy(6, at["b"]).start()

    def finish(self, acc, hidden_in, gain, hidden_ref, normed_ref):
        self.arrive(0)
        self.arrive(4)
        self.arrive(6)

        def chunk(c, carry):
            rows = pl.ds(pl.multiple_of(c * 32, 32), 32)
            total = acc[rows, :]
            for slot in (0, 4, 6):
                total = total + self.rbuf[slot, rows, :].astype(F32)
            total = total.astype(BF16).astype(F32)
            if hidden_in is None:
                hidden = EMBED_MULT * total
            else:
                hidden = hidden_in[rows, :] + RESID_MULT * total
            hidden_ref[rows, :] = hidden
            mean_sq = jnp.mean(hidden * hidden, axis=1, keepdims=True)
            normed_ref[rows, :] = (hidden * lax.rsqrt(mean_sq + NORM_EPS) * gain).astype(BF16)
            return carry

        lax.fori_loop(0, ROWS // 32, chunk, 0)
        for slot in range(7):
            self.copy(slot, self.at["sib"]).wait_send()


def gather_scratch():
    return [pltpu.VMEM((N, ROWS, D), BF16), pltpu.SemaphoreType.DMA((7,)), pltpu.SemaphoreType.DMA((N,))]


def scatter_scratch():
    return [pltpu.VMEM((ROWS, D), F32), pltpu.VMEM((7, ROWS, D), BF16),
            pltpu.VMEM((7, ROWS, D), BF16), pltpu.SemaphoreType.DMA((7,)), pltpu.SemaphoreType.DMA((7,))]


VM = pl.BlockSpec(memory_space=pltpu.VMEM)
RESIDUAL = (jax.ShapeDtypeStruct((ROWS, D), F32), jax.ShapeDtypeStruct((ROWS, D), BF16))
ANY = pl.BlockSpec(memory_space=pl.ANY)


def comm_params(ident):
    return pltpu.CompilerParams(collective_id=ident, has_side_effects=True, vmem_limit_bytes=VMEM_LIMIT)


CAP = 64


def pack_kernel(group_ref, place_ref, embed_ref, out_ref, buf, sem):
    def issue(d, carry):
        for j in range(CAP):
            pltpu.make_async_copy(embed_ref.at[group_ref[d * CAP + j]], buf.at[d, j], sem.at[d]).start()
        return carry

    def place(d, carry):
        pltpu.make_async_copy(embed_ref.at[0:CAP], buf.at[d], sem.at[d]).wait()
        lane = lax.broadcasted_iota(jnp.int32, (CAP, 8 * CAP), 1)
        one_hot = jnp.where(lane == place_ref[d], 1.0, 0.0).astype(BF16)
        out_ref[d] = jnp.dot(one_hot, buf[d].reshape(8 * CAP, D), preferred_element_type=F32).astype(BF16)
        return carry

    lax.fori_loop(0, N, issue, 0)
    lax.fori_loop(0, N, place, 0)


def pack_rows(owned, embed):
    group = lax.div(owned, 8).reshape(-1)
    place = (8 * jnp.arange(CAP) + lax.rem(owned, 8)).reshape(N, CAP, 1)
    return pl.pallas_call(
        pack_kernel,
        out_shape=jax.ShapeDtypeStruct((N, CAP, D), BF16),
        grid_spec=pltpu.PrefetchScalarGridSpec(
            num_scalar_prefetch=1, grid=(1,),
            in_specs=[pl.BlockSpec((N, CAP, 1), lambda i, *_: (0, 0, 0)), ANY],
            out_specs=pl.BlockSpec((N, CAP, D), lambda i, *_: (0, 0, 0)),
            scratch_shapes=[pltpu.VMEM((N, CAP, 8, D), BF16), pltpu.SemaphoreType.DMA((N,))]),
        compiler_params=pltpu.CompilerParams(vmem_limit_bytes=VMEM_LIMIT),
    )(group, place, embed.reshape(VOCAB // 8, 8, D))


def exchange_kernel(packed_ref, slot_ref, gains_ref, hidden_ref, normed_ref, held, send, recv):
    me = lax.axis_index("tp")
    barrier = pltpu.get_barrier_semaphore()
    for shift in range(1, N):
        pl.semaphore_signal(barrier, inc=1, device_id={"tp": lax.rem(me + shift, N)}, device_id_type=MESH)
    pl.semaphore_wait(barrier, N - 1)

    def copy(target, origin, shift):
        return pltpu.make_async_remote_copy(
            src_ref=packed_ref.at[target], dst_ref=held.at[origin], send_sem=send.at[shift], recv_sem=recv.at[shift],
            device_id={"tp": target}, device_id_type=MESH)

    for shift in range(1, N):
        copy(lax.rem(me + shift, N), me, shift).start()
    held[me] = packed_ref[me]
    for shift in range(1, N):
        copy(lax.rem(me + shift, N), lax.rem(me + N - shift, N), shift).wait()

    def chunk(c, carry):
        rows = pl.ds(pl.multiple_of(c * 64, 64), 64)
        lane = lax.broadcasted_iota(jnp.int32, (64, N * CAP), 1)
        one_hot = jnp.where(lane == slot_ref[rows, :], 1.0, 0.0).astype(BF16)
        hidden = EMBED_MULT * jnp.dot(one_hot, held[...].reshape(N * CAP, D), preferred_element_type=F32)
        hidden_ref[rows, :] = hidden
        mean_sq = jnp.mean(hidden * hidden, axis=1, keepdims=True)
        normed_ref[rows, :] = (hidden * lax.rsqrt(mean_sq + NORM_EPS) * gains_ref[0:1, :]).astype(BF16)
        return carry

    lax.fori_loop(0, ROWS // 64, chunk, 0)


def exchange_rows(packed, slot, gains, ident):
    return pl.pallas_call(
        exchange_kernel,
        out_shape=RESIDUAL,
        in_specs=[VM] * 3, out_specs=(VM, VM),
        scratch_shapes=[pltpu.VMEM((N, CAP, D), BF16), pltpu.SemaphoreType.DMA((N,)), pltpu.SemaphoreType.DMA((N,))],
        compiler_params=comm_params(ident),
    )(packed, slot, gains)


def embed_tokens(ids, shard, embed, gains):
    owner = lax.div(ids, VOCAB)
    earlier = jnp.arange(ROWS)[:, None] > jnp.arange(ROWS)[None, :]
    rank = jnp.sum(((owner[:, :, None] == owner[:, None, :]) & earlier).astype(jnp.int32), axis=2)
    local = ids - shard * VOCAB

    def packed(gains):
        mine = jnp.where(owner == shard, rank, -1)
        hit = mine[:, None, :] == jnp.arange(CAP)[None, :, None]
        owned = jnp.sum(jnp.where(hit, local[:, None, :], 0), axis=2)
        slot = lax.dynamic_index_in_dim(owner * CAP + rank, shard, 0, keepdims=False)
        return exchange_rows(pack_rows(owned, embed), slot[:, None], gains, 0)

    def general(gains):
        flat = local.reshape(-1)
        inside = (flat >= 0) & (flat < VOCAB)
        rows = jnp.take(embed, jnp.clip(flat, 0, VOCAB - 1), axis=0)
        return embed_sum(jnp.where(inside[:, None], rows, jnp.zeros_like(rows)), gains, 6)

    return lax.cond(jnp.max(rank) < CAP, packed, general, gains)


def embed_kernel(rows_ref, gains_ref, hidden_ref, normed_ref, acc, tbuf, rbuf, send, recv):
    at = places()
    entry_barrier(at)
    scatter = Scatter(at, tbuf, rbuf, send, recv)

    def body(pos, carry):
        acc[...] = rows_ref[pick(pos, ORDER_EMBED, at)].astype(F32)
        scatter.after(pos, acc, far_first=True)
        return carry

    lax.fori_loop(0, N, body, 0)
    scatter.finish(acc, None, gains_ref[0:1, :], hidden_ref, normed_ref)


def embed_sum(rows, gains, ident):
    return pl.pallas_call(
        embed_kernel,
        out_shape=RESIDUAL,
        in_specs=[VM, VM], out_specs=(VM, VM),
        scratch_shapes=scatter_scratch(),
        compiler_params=comm_params(ident),
    )(rows.reshape(N, ROWS, D), gains)


HALF = 32
SLOTS = 4


def attend_half(base, start_ref, first_seq, qk, vv, planes, mixed_out):
    lane = lax.broadcasted_iota(jnp.int32, (8, 128), 1)
    row = lax.broadcasted_iota(jnp.int32, (8, 128), 0)
    first = lane < HEAD
    own = [(2 * j + lax.div(lane, HEAD)) == row for j in range(4)]
    groups = range(HALF // 8)

    def spread(twice):
        return jnp.concatenate([jnp.where(own[j], twice, 0.0) for j in range(4)], axis=1)

    starts = [start_ref[pl.ds(pl.multiple_of(first_seq + base + 8 * g, 8), 8), :] for g in groups]
    query, updates = [], []
    for g in groups:
        queries, keys, vals, hot = [], [], [], []
        for s in range(STEPS):
            span = pl.ds(pl.multiple_of(s * SEQS + base + 8 * g, 8), 8)
            left, right = qk[span, 0:128], qk[span, 128:256]
            left_r, right_r = pltpu.roll(left, HEAD, 1), pltpu.roll(right, HEAD, 1)
            queries += [spread(jnp.where(first, left, left_r)), spread(jnp.where(first, left_r, left)),
                        spread(jnp.where(first, right, right_r))]
            keys.append(spread(jnp.where(first, right_r, right)))
            vals.append(spread(vv[span, :]))
            hot.append(jnp.where(lane == starts[g] + s, 1.0, 0.0))
        query.append(jnp.concatenate(queries, axis=0).astype(BF16))
        hot_all = jnp.concatenate(hot, axis=0).astype(BF16)
        updates.append([
            lax.dot_general(jnp.concatenate(entry, axis=0).astype(BF16), hot_all, (((0,), (0,)), ((), ())),
                            preferred_element_type=F32) for entry in (keys, vals)])
    for g in groups:
        span = pl.ds(base + 8 * g, 8)
        fresh = jnp.where((lane >= starts[g]) & (lane < starts[g] + STEPS), 1.0, 0.0)
        fresh = jnp.broadcast_to(fresh[:, None, :], (8, HEAD, 128)) > 0.5
        for kind in range(2):
            old = planes[kind, span].astype(F32)
            planes[kind, span] = jnp.where(fresh, updates[g][kind].reshape(8, HEAD, 128), old).astype(BF16)
    scores = [jnp.dot(query[g], planes[0, pl.ds(base + 8 * g, 8)].reshape(8 * HEAD, 128), preferred_element_type=F32)
              for g in groups]
    probs = []
    for g in groups:
        valid = [jnp.where(lane <= starts[g] + s, 0.0, -jnp.inf) for s in range(STEPS)]
        score = scores[g] * ATT_SCALE + jnp.concatenate([valid[s] for s in range(STEPS) for h in range(3)], axis=0)
        weight = jnp.exp(score - jnp.max(score, axis=1, keepdims=True))
        probs.append((weight / jnp.sum(weight, axis=1, keepdims=True)).astype(BF16))
    mixed = [lax.dot_general(probs[g], planes[1, pl.ds(base + 8 * g, 8)].reshape(8 * HEAD, 128),
                             (((1,), (1,)), ((), ())), preferred_element_type=F32) for g in groups]
    for g in groups:
        for s in range(STEPS):
            span = pl.ds(pl.multiple_of(s * SEQS + base + 8 * g, 8), 8)
            heads = []
            for h in range(3):
                part = mixed[g][8 * (3 * s + h):8 * (3 * s + h) + 8, :]
                total = sum(jnp.where(own[j], part[:, 128 * j:128 * j + 128], 0.0) for j in range(4))
                heads.append(total + pltpu.roll(total, HEAD, 1))
            mixed_out[span, 0:128] = jnp.where(first, heads[0], heads[1])
            mixed_out[span, 128:256] = heads[2]


def attn_kernel(layer, u_ref, cos_ref, sin_ref, start_ref, hidden_in, gains_ref, wq_ref, wk_ref, wv_ref, wo_ref, cache_ref,
                *rest):
    if layer > 0:
        rest = rest[1:]
    (hidden_ref, normed_ref, new_ref, ubuf, ag_send, ag_recv, acc, tbuf, rbuf, rs_send, rs_recv,
     qk, vv, mixed, planes, w_qkv, w_out, in_sem, out_sem, w_sem) = rest
    at = places()
    weights = [
        pltpu.make_async_copy(wq_ref.at[layer], w_qkv.at[0:192], w_sem.at[0]),
        pltpu.make_async_copy(wk_ref.at[layer], w_qkv.at[192:256], w_sem.at[1]),
        pltpu.make_async_copy(wv_ref.at[layer], w_qkv.at[256:320], w_sem.at[2]),
        pltpu.make_async_copy(wv_ref.at[layer], w_qkv.at[320:384], w_sem.at[3]),
        pltpu.make_async_copy(wo_ref.at[layer], w_out.at[0:192], w_sem.at[4])]
    for item in weights:
        item.start()
    w_out[192:256, :] = jnp.zeros((64, D), BF16)

    def plane_span(pos):
        return pl.ds(pick(pos, ORDER_RS, at) * SEQS, SEQS)

    def load(pos):
        slot = lax.rem(pos, SLOTS)
        return pltpu.make_async_copy(cache_ref.at[layer, :, plane_span(pos)], planes.at[slot], in_sem.at[slot])

    def store(pos):
        slot = lax.rem(pos, SLOTS)
        return pltpu.make_async_copy(planes.at[slot], new_ref.at[layer, :, plane_span(pos)], out_sem.at[slot])

    load(jnp.int32(0)).start()
    load(jnp.int32(1)).start()
    entry_barrier(at)
    gather = Gather(at, u_ref, ubuf, ag_send, ag_recv)
    scatter = Scatter(at, tbuf, rbuf, rs_send, rs_recv)
    gather.start(0, 2)
    ubuf[at["me"]] = u_ref[...]
    for item in weights:
        item.wait()

    def body(pos, carry):
        gather.before(pos, ORDER_RS)
        blk = pick(pos, ORDER_RS, at)

        @pl.when(pos >= 2)
        def _():
            store(pos - 2).wait()

        @pl.when(pos < N - 2)
        def _():
            load(pos + 2).start()

        out = lax.dot_general(ubuf[blk], w_qkv[...], (((1,), (1,)), ((), ())), preferred_element_type=F32)
        cos = cos_ref[blk]
        sin = sin_ref[blk]
        low = lax.rem(lax.broadcasted_iota(jnp.int32, (ROWS, 128), 1), HEAD) < HEAD // 2
        for half in range(2):
            part = out[:, half * 128:(half + 1) * 128]
            swapped = jnp.where(low, pltpu.roll(part, 128 - HEAD // 2, 1), pltpu.roll(part, HEAD // 2, 1))
            qk[:, half * 128:(half + 1) * 128] = (part * cos + swapped * sin).astype(BF16).astype(F32)
        vv[...] = out[:, 256:384].astype(BF16).astype(F32)
        load(pos).wait()

        def half_block(i, carry):
            attend_half(i * HALF, start_ref, blk * SEQS, qk, vv, planes.at[lax.rem(pos, SLOTS)], mixed)
            return carry

        lax.fori_loop(0, SEQS // HALF, half_block, 0)
        store(pos).start()
        acc[...] = jnp.dot(mixed[...].astype(BF16), w_out[...], preferred_element_type=F32)
        scatter.after(pos, acc)
        return carry

    lax.fori_loop(0, N, body, 0)
    store(jnp.int32(N - 2)).wait()
    store(jnp.int32(N - 1)).wait()
    gather.finish()
    scatter.finish(acc, hidden_in, gains_ref[2 * layer + 1:2 * layer + 2, :], hidden_ref, normed_ref)


def attention(layer, u, cos, sin, start_wide, hidden, gains, weights, cache, new_cache, ident):
    args = [u, cos, sin, start_wide, hidden, gains, *weights, cache]
    in_specs = [VM] * 6 + [ANY] * 5
    aliases = {}
    if new_cache is not None:
        args.append(new_cache)
        in_specs.append(ANY)
        aliases = {11: 2}
    return pl.pallas_call(
        functools.partial(attn_kernel, layer),
        out_shape=RESIDUAL + (jax.ShapeDtypeStruct(cache.shape, BF16),),
        in_specs=in_specs, out_specs=(VM, VM, ANY),
        scratch_shapes=gather_scratch() + scatter_scratch() + [
            pltpu.VMEM((ROWS, 256), F32), pltpu.VMEM((ROWS, 128), F32), pltpu.VMEM((ROWS, 256), F32),
            pltpu.VMEM((SLOTS, 2, SEQS, HEAD, CACHE), BF16), pltpu.VMEM((384, D), BF16), pltpu.VMEM((256, D), BF16),
            pltpu.SemaphoreType.DMA((SLOTS,)), pltpu.SemaphoreType.DMA((SLOTS,)), pltpu.SemaphoreType.DMA((5,))],
        input_output_aliases=aliases,
        compiler_params=comm_params(ident),
    )(*args)


def moe_kernel(layer, u_ref, router_ref, ids_ref, hidden_in, gains_ref, gate_hbm, up_hbm, down_hbm, hidden_ref, normed_ref,
               ubuf, ag_send, ag_recv, acc, tbuf, rbuf, rs_send, rs_recv, gate_v, up_v, down_v, hidden, gates, w_sem):
    def load(kind, e):
        src, dst = ((gate_hbm, gate_v), (up_hbm, up_v))[kind]
        return pltpu.make_async_copy(src.at[layer, e], dst.at[e], w_sem.at[kind, e])

    down_load = pltpu.make_async_copy(down_hbm.at[layer], down_v, w_sem.at[2, 0])
    for e in range(LOCAL_EXPERTS):
        load(0, e).start()
        load(1, e).start()
    down_load.start()
    at = places()
    entry_barrier(at)
    gather = Gather(at, u_ref, ubuf, ag_send, ag_recv)
    scatter = Scatter(at, tbuf, rbuf, rs_send, rs_recv)
    gather.start(0, 2)
    ubuf[at["me"]] = u_ref[...]
    lane = lax.broadcasted_iota(jnp.int32, (ROWS, EXPERTS), 1)

    def route(blk):
        ids = ids_ref[blk]
        chosen = lane == ids[:, 0:1]
        for j in range(1, 8):
            chosen = chosen | (lane == ids[:, j:j + 1])
        score = lax.dot_general(ubuf[blk], router_ref[layer], (((1,), (1,)), ((), ())), preferred_element_type=F32)
        masked = jnp.where(chosen, score, -jnp.inf)
        weight = jnp.exp(masked - jnp.max(masked, axis=1, keepdims=True))
        gates[...] = weight / jnp.sum(weight, axis=1, keepdims=True)

    def inner(blk, e):
        return (jnp.dot(ubuf[blk], gate_v[e], preferred_element_type=F32),
                jnp.dot(ubuf[blk], up_v[e], preferred_element_type=F32))

    def activate(e, gate_act, up_act):
        share = jnp.sum(jnp.where(lane == at["me"] * LOCAL_EXPERTS + e, gates[...], 0.0), axis=1, keepdims=True)
        z = gate_act * jax.nn.sigmoid(gate_act) * up_act * share
        start = e * FF if isinstance(e, int) else pl.multiple_of(e * FF, FF)
        hidden[:, pl.ds(start, FF)] = z.astype(BF16)

    def down():
        for c in range(D // 512):
            cols = slice(c * 512, c * 512 + 512)
            acc[:, cols] = jnp.dot(hidden[...], down_v[:, cols], preferred_element_type=F32)

    def first_expert(e, carry):
        load(0, e).wait()
        load(1, e).wait()
        activate(e, *inner(at["sib"], e))
        return carry

    gather.before(jnp.int32(0), ORDER_RS)
    route(at["sib"])
    lax.fori_loop(0, LOCAL_EXPERTS, first_expert, 0)
    down_load.wait()
    down()
    scatter.after(jnp.int32(0), acc)

    def body(pos, carry):
        gather.before(pos, ORDER_RS)
        blk = pick(pos, ORDER_RS, at)
        acts = inner(blk, 0)
        route(blk)
        for e in range(LOCAL_EXPERTS):
            following = inner(blk, e + 1) if e + 1 < LOCAL_EXPERTS else None
            activate(e, *acts)
            acts = following
        down()
        scatter.after(pos, acc)
        return carry

    lax.fori_loop(1, N, body, 0)
    gather.finish()
    scatter.finish(acc, hidden_in, gains_ref[2 * layer + 2:2 * layer + 3, :], hidden_ref, normed_ref)


def experts(layer, u, router, ids, hidden, gains, w_gate, w_up, w_down, ident):
    width = LOCAL_EXPERTS * FF
    return pl.pallas_call(
        functools.partial(moe_kernel, layer),
        out_shape=RESIDUAL,
        in_specs=[VM] * 5 + [ANY] * 3, out_specs=(VM, VM),
        scratch_shapes=gather_scratch() + scatter_scratch() + [
            pltpu.VMEM((LOCAL_EXPERTS, D, FF), BF16), pltpu.VMEM((LOCAL_EXPERTS, D, FF), BF16),
            pltpu.VMEM((width, D), BF16), pltpu.VMEM((ROWS, width), BF16), pltpu.VMEM((ROWS, EXPERTS), F32),
            pltpu.SemaphoreType.DMA((3, LOCAL_EXPERTS))],
        compiler_params=comm_params(ident),
    )(u, router, ids, hidden, gains, w_gate, w_up, w_down.reshape(LAYERS, width, D))


TILE = 1024
TILES = VOCAB // TILE
LAST_TILE = 384


LOG2E = 1.4426950408889634


def fold(logits, column, target, stat):
    part = logits.reshape(TILE // 8, 8, ROWS)
    peak = stat[0]
    top = jnp.maximum(peak, jnp.max(part, axis=0))
    stat[0] = top
    stat[1] = stat[1] * jnp.exp2((peak - top) * (LOG2E / LOGIT_DIV)) + jnp.sum(
        jnp.exp2((part - top) * (LOG2E / LOGIT_DIV)), axis=0)
    here = target - column // 8 if isinstance(column, int) else target - lax.div(column, 8)
    picked = stat[2]
    for g in range(TILE // 8):
        picked = jnp.where(here == g, part[g], picked)
    stat[2] = picked


def head_kernel(f_ref, target_ref, embed_ref, probs_ref, last_ref, ubuf, send, recv, table, even, odd, stat, mine, theirs,
                share_send, share_recv, sem):
    def load(c):
        rows = pl.ds(pl.multiple_of(c * TILE, TILE), TILE)
        return pltpu.make_async_copy(embed_ref.at[rows], table.at[rows], sem.at[c])

    for c in range(TILES):
        load(c).start()
    at = places()
    entry_barrier(at, ORDER_AG[1:])
    gather = Gather(at, f_ref, ubuf, send, recv)
    gather.start(0, 2)
    ubuf[at["me"]] = f_ref[...]

    def tile_logits(blk, start):
        return lax.dot_general(table[pl.ds(start, TILE), :], ubuf[blk], (((1,), (1,)), ((), ())), preferred_element_type=F32)

    def group_of(blk):
        local = jnp.broadcast_to(target_ref[blk], (8, ROWS))
        sub = lax.broadcasted_iota(jnp.int32, (8, ROWS), 0)
        return jnp.where((local >= 0) & ((local & 7) == sub), local >> 3, -1 - VOCAB)

    def begin():
        stat[0] = jnp.full((8, ROWS), -1e30, F32)
        stat[1] = jnp.zeros((8, ROWS), F32)
        stat[2] = jnp.zeros((8, ROWS), F32)

    def end(blk):
        peak = stat[0]
        top = jnp.max(peak, axis=0, keepdims=True)
        mine[0, pl.ds(blk, 1), :] = top
        mine[1, pl.ds(blk, 1), :] = jnp.sum(stat[1] * jnp.exp2((peak - top) * (LOG2E / LOGIT_DIV)), axis=0, keepdims=True)
        mine[2, pl.ds(blk, 1), :] = jnp.sum(stat[2], axis=0, keepdims=True)
        last_ref[blk] = ubuf[blk, ROWS - SEQS:ROWS, :]

    def first_tile(c, carry):
        load(c).wait()
        even[...] = tile_logits(at["me"], pl.multiple_of(c * TILE, TILE))
        fold(even[...], c * TILE, group_of(at["me"]), stat)
        return carry

    begin()
    lax.fori_loop(0, TILES, first_tile, 0)
    end(at["me"])

    def body(pos, carry):
        gather.before(pos, ORDER_AG)
        blk = pick(pos, ORDER_AG, at)
        target = group_of(blk)
        begin()
        bufs = (even, odd)
        even[...] = tile_logits(blk, 0)
        for c in range(1, TILES + 1):
            if c < TILES:
                bufs[c % 2][...] = tile_logits(blk, c * TILE)
            fold(bufs[(c - 1) % 2][...], (c - 1) * TILE, target, stat)
        end(blk)
        return carry

    lax.fori_loop(1, N, body, 0)
    gather.finish()
    me = at["me"]
    copies = [pltpu.make_async_remote_copy(
        src_ref=mine, dst_ref=theirs.at[shift], send_sem=share_send.at[shift], recv_sem=share_recv.at[shift],
        device_id={"tp": lax.rem(me + shift, N)}, device_id_type=MESH) for shift in range(1, N)]
    for item in copies:
        item.start()
    theirs[0] = mine[...]
    for item in copies:
        item.wait()
    peak = functools.reduce(jnp.maximum, [theirs[i, 0] for i in range(N)])
    total = sum(theirs[i, 1] * jnp.exp2((theirs[i, 0] - peak) * (LOG2E / LOGIT_DIV)) for i in range(N))
    picked = sum(theirs[i, 2] for i in range(N))
    probs_ref[...] = (picked - peak) * (1.0 / LOGIT_DIV) - jnp.log(total)


def head(f, target, embed, ident):
    return pl.pallas_call(
        head_kernel,
        out_shape=(jax.ShapeDtypeStruct((N, ROWS), F32), jax.ShapeDtypeStruct((N, SEQS, D), BF16)),
        in_specs=[VM, VM, ANY], out_specs=(VM, VM),
        scratch_shapes=gather_scratch() + [
            pltpu.VMEM((VOCAB, D), BF16), pltpu.VMEM((TILE, ROWS), F32), pltpu.VMEM((TILE, ROWS), F32),
            pltpu.VMEM((3, 8, ROWS), F32), pltpu.VMEM((3, N, ROWS), F32), pltpu.VMEM((N, 3, N, ROWS), F32),
            pltpu.SemaphoreType.DMA((N,)), pltpu.SemaphoreType.DMA((N,)), pltpu.SemaphoreType.DMA((TILES,))],
        compiler_params=comm_params(ident),
    )(f, target, embed)


LAST_STEPS = VOCAB // LAST_TILE
PLANES = LAYERS * 2 * BATCH // LAST_STEPS
RING = 8
AHEAD = 4


def last_kernel(f_ref, embed_ref, cache_ref, logits_ref, new_ref, ring, in_sem, out_sem):
    c = pl.program_id(0)

    def load(i):
        slot = lax.rem(i, RING)
        return pltpu.make_async_copy(cache_ref.at[pl.ds(i * PLANES, PLANES)], ring.at[slot], in_sem.at[slot])

    def store(i):
        slot = lax.rem(i, RING)
        return pltpu.make_async_copy(ring.at[slot], new_ref.at[pl.ds(i * PLANES, PLANES)], out_sem.at[slot])

    @pl.when(c == 0)
    def _():
        for i in range(AHEAD):
            load(jnp.int32(i)).start()

    @pl.when((c >= RING - AHEAD) & (c < LAST_STEPS - AHEAD))
    def _():
        store(c + AHEAD - RING).wait()

    @pl.when(c < LAST_STEPS - AHEAD)
    def _():
        load(c + AHEAD).start()

    load(c).wait()
    store(c).start()
    logits_ref[...] = lax.dot_general(f_ref[...], embed_ref[...], (((1,), (1,)), ((), ())),
                                      preferred_element_type=F32) * (1.0 / LOGIT_DIV)

    @pl.when(c == LAST_STEPS - 1)
    def _():
        for i in range(LAST_STEPS - RING, LAST_STEPS):
            store(jnp.int32(i)).wait()


def last_step(f, embed, cache):
    flat = cache.reshape(LAYERS * 2 * BATCH, HEAD, CACHE)
    logits, flat = pl.pallas_call(
        last_kernel,
        out_shape=(jax.ShapeDtypeStruct((BATCH, VOCAB), F32), jax.ShapeDtypeStruct(flat.shape, BF16)),
        grid=(LAST_STEPS,),
        in_specs=[pl.BlockSpec((BATCH, D), lambda c: (0, 0)), pl.BlockSpec((LAST_TILE, D), lambda c: (c, 0)), ANY],
        out_specs=(pl.BlockSpec((BATCH, LAST_TILE), lambda c: (0, c)), ANY),
        scratch_shapes=[pltpu.VMEM((RING, PLANES, HEAD, CACHE), BF16), pltpu.SemaphoreType.DMA((RING,)),
                        pltpu.SemaphoreType.DMA((RING,))],
        compiler_params=pltpu.CompilerParams(dimension_semantics=("arbitrary",), vmem_limit_bytes=VMEM_LIMIT),
    )(f, embed, flat)
    return logits, flat.reshape(cache.shape)


def by_block(values):
    return values.reshape(N, SEQS, values.shape[1]).transpose(0, 2, 1)


def solution(mesh):
    cache_spec = P(None, None, 'dp', None, 'tp', None)
    expert_spec = P(None, 'tp', None, None)
    in_specs = (P('dp', None), P('dp'), cache_spec, P(None, None, 'dp', None), P('tp', None), P(None, None), P(None, None, 'tp'), P(None, None, 'tp'), P(None, None, 'tp'), P(None, 'tp', None), P(None, None, None), expert_spec, expert_spec, expert_spec)
    out_specs = (P('dp', None), P('dp', 'tp'), cache_spec)

    def decode_local(tokens, start_pos, kv_cache, expert_ids, embed, norm_gain, w_query, w_key, w_value, w_out, w_router, w_gate, w_up, w_down):
        shard = lax.axis_index('tp')
        cache = kv_cache.transpose(0, 1, 2, 4, 5, 3).reshape(LAYERS, 2, BATCH, HEAD, CACHE)

        ids = by_block(tokens[:, :STEPS]).reshape(N, ROWS)
        hidden, normed = embed_tokens(ids, shard, embed, norm_gain)

        pos = by_block(start_pos[:, None] + jnp.arange(STEPS)[None, :]).reshape(N, ROWS)
        inv_freq = ROPE_THETA ** (-2.0 * jnp.arange(HEAD // 2, dtype=F32) / HEAD)
        angles = pos.astype(F32)[:, :, None] * jnp.tile(inv_freq, 4)
        cos = jnp.cos(angles)
        sin = jnp.sin(angles) * jnp.where(jnp.arange(128) % HEAD < HEAD // 2, -1.0, 1.0)
        start_wide = jnp.broadcast_to(start_pos[:, None], (BATCH, 128))

        weights = [w.transpose(0, 2, 1) for w in (w_query, w_key, w_value)] + [w_out]
        router = w_router.transpose(0, 2, 1)
        routed = expert_ids.reshape(STEPS, LAYERS, N, SEQS, 8).transpose(1, 2, 0, 3, 4).reshape(LAYERS, N, ROWS, 8)

        new_cache = None
        for layer in range(LAYERS):
            hidden, normed, new_cache = attention(layer, normed, cos, sin, start_wide, hidden, norm_gain, weights, cache, new_cache,
                                                  1 + 2 * layer)
            hidden, normed = experts(layer, normed, router, routed[layer], hidden, norm_gain, w_gate, w_up, w_down, 2 + 2 * layer)

        target = by_block(tokens[:, 1:] - shard * VOCAB).reshape(N, 1, ROWS)
        log_probs, f_last = head(normed, target, embed, 5)
        logits, new_cache = last_step(f_last.reshape(BATCH, D), embed, new_cache)
        log_probs = log_probs.reshape(N, STEPS, SEQS).transpose(0, 2, 1).reshape(BATCH, STEPS)
        new_cache = new_cache.reshape(LAYERS, 2, BATCH, 1, HEAD, CACHE).transpose(0, 1, 2, 5, 3, 4)
        return log_probs, logits, new_cache

    return jax.shard_map(decode_local, mesh=mesh, in_specs=in_specs, out_specs=out_specs, check_vma=False)
```

```python
import functools

import jax
import jax.numpy as jnp
from jax import lax
from jax.experimental import pallas as pl
from jax.experimental.pallas import tpu as pltpu
from jax.sharding import PartitionSpec as P

EMBED_MULT = 12.0
ATT_SCALE = 0.015625
RESID_MULT = 0.22
LOGIT_DIV = 6.0
NORM_EPS = 1e-6
ROPE_THETA = 10000.0

D = 1536
HEAD = 64
BATCH = 512
STEPS = 4
LAYERS = 2
CACHE = 128
EXPERTS = 40
LOCAL_EXPERTS = 5
FF = 512
VOCAB = 6144
N = 8
SEQS = BATCH // N
ROWS = SEQS * STEPS
MESH = pl.DeviceIdType.MESH
F32 = jnp.float32
BF16 = jnp.bfloat16
VMEM_LIMIT = 60 * 1024 * 1024

ORDER_RS = ("sib", "bs", "a", "ds", "dg", "as", "b", "me")
ORDER_AG = ("me", "sib", "bs", "a", "ds", "dg", "as", "b")
ORDER_EMBED = ("sib", "ds", "dg", "bs", "a", "as", "b", "me")


def places():
    me = lax.axis_index("tp")
    k = lax.rem(me, 2)
    x = lax.rem(lax.div(me, 2), 2)
    y = lax.div(me, 4)
    step_x = 2 - 4 * x
    step_y = 4 - 8 * y
    a = me + step_x + k * (step_y - step_x)
    b = me + step_y + k * (step_x - step_y)
    dg = me + step_x + step_y
    s = 1 - 2 * k
    return {"me": me, "sib": me + s, "a": a, "as": a + s, "b": b, "bs": b + s, "dg": dg, "ds": dg + s}


def entry_barrier(at, names=("sib", "a", "b")):
    barrier = pltpu.get_barrier_semaphore()
    for name in names:
        pl.semaphore_signal(barrier, inc=1, device_id={"tp": at[name]}, device_id_type=MESH)
    pl.semaphore_wait(barrier, len(names))


def pick(pos, order, at):
    total = jnp.int32(0)
    for i, name in enumerate(order):
        total = total + jnp.where(pos == i, at[name], 0)
    return total


class Gather:
    def __init__(self, at, own, ubuf, send, recv):
        self.at, self.own, self.ubuf, self.send, self.recv = at, own, ubuf, send, recv

    def copy(self, src, origin, target, slot):
        return pltpu.make_async_remote_copy(
            src_ref=src, dst_ref=self.ubuf.at[origin], send_sem=self.send.at[slot], recv_sem=self.recv.at[origin],
            device_id={"tp": target}, device_id_type=MESH)

    def item(self, slot):
        at = self.at
        if slot < 3:
            return self.copy(self.own, at["me"], at[("a", "b", "sib")[slot]], slot)
        name, target = (("a", "b"), ("a", "sib"), ("b", "sib"), ("dg", "sib"))[slot - 3]
        return self.copy(self.ubuf.at[at[name]], at[name], at[target], slot)

    def start(self, *slots):
        for slot in slots:
            self.item(slot).start()

    def arrive(self, name):
        origin = self.at[name]
        self.copy(self.own, origin, self.at["sib"], 0).wait_recv()

    def before(self, pos, order):
        @pl.when(pos == order.index("sib"))
        def _():
            self.arrive("sib")

        @pl.when(pos == order.index("bs"))
        def _():
            self.arrive("a")
            self.start(3, 4, 1)
            self.arrive("bs")

        @pl.when(pos == order.index("ds"))
        def _():
            self.arrive("dg")
            self.start(6)
            self.arrive("ds")

        @pl.when(pos == order.index("as"))
        def _():
            self.arrive("b")
            self.start(5)
            self.arrive("as")

    def finish(self):
        for slot in range(7):
            self.item(slot).wait_send()


class Scatter:
    def __init__(self, at, tbuf, rbuf, send, recv):
        self.at, self.tbuf, self.rbuf, self.send, self.recv = at, tbuf, rbuf, send, recv

    def copy(self, slot, target):
        return pltpu.make_async_remote_copy(
            src_ref=self.tbuf.at[slot], dst_ref=self.rbuf.at[slot], send_sem=self.send.at[slot],
            recv_sem=self.recv.at[slot], device_id={"tp": target}, device_id_type=MESH)

    def arrive(self, slot):
        self.copy(slot, self.at["sib"]).wait_recv()

    def after(self, pos, acc, far_first=False):
        at = self.at

        @pl.when((pos == 0) | (pos == 1) | (pos == 3) | (pos == 5))
        def _():
            slot = lax.div(pos + 1, 2)
            self.tbuf[slot] = acc[...].astype(BF16)
            self.copy(slot, at["sib"]).start()

        @pl.when((pos == 2) | (pos == 4))
        def _():
            slot = lax.div(pos, 2)
            out = 6 - slot if far_first else slot + 3
            self.arrive(slot)
            self.tbuf[out] = (acc[...] + self.rbuf[slot].astype(F32)).astype(BF16)
            self.copy(out, at["a"]).start()

        @pl.when(pos == 6)
        def _():
            self.arrive(3)
            self.arrive(5)
            self.tbuf[6] = (acc[...] + self.rbuf[3].astype(F32) + self.rbuf[5].astype(F32)).astype(BF16)
            self.copy(6, at["b"]).start()

    def finish(self, acc, hidden_in, gain, hidden_ref, normed_ref):
        self.arrive(0)
        self.arrive(4)
        self.arrive(6)

        def chunk(c, carry):
            rows = pl.ds(pl.multiple_of(c * 32, 32), 32)
            total = acc[rows, :]
            for slot in (0, 4, 6):
                total = total + self.rbuf[slot, rows, :].astype(F32)
            total = total.astype(BF16).astype(F32)
            if hidden_in is None:
                hidden = EMBED_MULT * total
            else:
                hidden = hidden_in[rows, :] + RESID_MULT * total
            hidden_ref[rows, :] = hidden
            mean_sq = jnp.mean(hidden * hidden, axis=1, keepdims=True)
            normed_ref[rows, :] = (hidden * lax.rsqrt(mean_sq + NORM_EPS) * gain).astype(BF16)
            return carry

        lax.fori_loop(0, ROWS // 32, chunk, 0)
        for slot in range(7):
            self.copy(slot, self.at["sib"]).wait_send()


def gather_scratch():
    return [pltpu.VMEM((N, ROWS, D), BF16), pltpu.SemaphoreType.DMA((7,)), pltpu.SemaphoreType.DMA((N,))]


def scatter_scratch():
    return [pltpu.VMEM((ROWS, D), F32), pltpu.VMEM((7, ROWS, D), BF16),
            pltpu.VMEM((7, ROWS, D), BF16), pltpu.SemaphoreType.DMA((7,)), pltpu.SemaphoreType.DMA((7,))]


VM = pl.BlockSpec(memory_space=pltpu.VMEM)
RESIDUAL = (jax.ShapeDtypeStruct((ROWS, D), F32), jax.ShapeDtypeStruct((ROWS, D), BF16))
ANY = pl.BlockSpec(memory_space=pl.ANY)


def comm_params(ident):
    return pltpu.CompilerParams(collective_id=ident, has_side_effects=True, vmem_limit_bytes=VMEM_LIMIT)


CAP = 64


def pack_kernel(group_ref, place_ref, embed_ref, out_ref, buf, sem):
    def issue(d):
        for j in range(CAP):
            pltpu.make_async_copy(embed_ref.at[group_ref[d * CAP + j]], buf.at[d, j], sem.at[d]).start()

    def place(d):
        pltpu.make_async_copy(embed_ref.at[0:CAP], buf.at[d], sem.at[d]).wait()
        lane = lax.broadcasted_iota(jnp.int32, (CAP, 8 * CAP), 1)
        one_hot = jnp.where(lane == place_ref[d], 1.0, 0.0).astype(BF16)
        out_ref[d] = jnp.dot(one_hot, buf[d].reshape(8 * CAP, D), preferred_element_type=F32).astype(BF16)

    def body(d, carry):
        issue(d + 2)
        place(d)
        return carry

    def first(d, carry):
        issue(d)
        return carry

    def last(d, carry):
        place(d)
        return carry

    lax.fori_loop(0, 2, first, 0)
    lax.fori_loop(0, N - 2, body, 0)
    lax.fori_loop(N - 2, N, last, 0)


def pack_rows(owned, embed):
    group = lax.div(owned, 8).reshape(-1)
    place = (8 * jnp.arange(CAP) + lax.rem(owned, 8)).reshape(N, CAP, 1)
    return pl.pallas_call(
        pack_kernel,
        out_shape=jax.ShapeDtypeStruct((N, CAP, D), BF16),
        grid_spec=pltpu.PrefetchScalarGridSpec(
            num_scalar_prefetch=1, grid=(1,),
            in_specs=[pl.BlockSpec((N, CAP, 1), lambda i, *_: (0, 0, 0)), ANY],
            out_specs=pl.BlockSpec((N, CAP, D), lambda i, *_: (0, 0, 0)),
            scratch_shapes=[pltpu.VMEM((N, CAP, 8, D), BF16), pltpu.SemaphoreType.DMA((N,))]),
        compiler_params=pltpu.CompilerParams(vmem_limit_bytes=VMEM_LIMIT),
    )(group, place, embed.reshape(VOCAB // 8, 8, D))


def exchange_kernel(packed_ref, slot_ref, gains_ref, hidden_ref, normed_ref, held, send, recv):
    me = lax.axis_index("tp")
    barrier = pltpu.get_barrier_semaphore()
    for shift in range(1, N):
        pl.semaphore_signal(barrier, inc=1, device_id={"tp": lax.rem(me + shift, N)}, device_id_type=MESH)
    pl.semaphore_wait(barrier, N - 1)

    def copy(target, origin, shift):
        return pltpu.make_async_remote_copy(
            src_ref=packed_ref.at[target], dst_ref=held.at[origin], send_sem=send.at[shift], recv_sem=recv.at[shift],
            device_id={"tp": target}, device_id_type=MESH)

    for shift in range(1, N):
        copy(lax.rem(me + shift, N), me, shift).start()
    held[me] = packed_ref[me]
    for shift in range(1, N):
        copy(lax.rem(me + shift, N), lax.rem(me + N - shift, N), shift).wait()

    def chunk(c, carry):
        rows = pl.ds(pl.multiple_of(c * 64, 64), 64)
        lane = lax.broadcasted_iota(jnp.int32, (64, N * CAP), 1)
        one_hot = jnp.where(lane == slot_ref[rows, :], 1.0, 0.0).astype(BF16)
        hidden = EMBED_MULT * jnp.dot(one_hot, held[...].reshape(N * CAP, D), preferred_element_type=F32)
        hidden_ref[rows, :] = hidden
        mean_sq = jnp.mean(hidden * hidden, axis=1, keepdims=True)
        normed_ref[rows, :] = (hidden * lax.rsqrt(mean_sq + NORM_EPS) * gains_ref[0:1, :]).astype(BF16)
        return carry

    lax.fori_loop(0, ROWS // 64, chunk, 0)


def exchange_rows(packed, slot, gains, ident):
    return pl.pallas_call(
        exchange_kernel,
        out_shape=RESIDUAL,
        in_specs=[VM] * 3, out_specs=(VM, VM),
        scratch_shapes=[pltpu.VMEM((N, CAP, D), BF16), pltpu.SemaphoreType.DMA((N,)), pltpu.SemaphoreType.DMA((N,))],
        compiler_params=comm_params(ident),
    )(packed, slot, gains)


def embed_tokens(ids, shard, embed, gains):
    owner = lax.div(ids, VOCAB)
    earlier = jnp.arange(ROWS)[:, None] > jnp.arange(ROWS)[None, :]
    rank = jnp.sum(((owner[:, :, None] == owner[:, None, :]) & earlier).astype(jnp.int32), axis=2)
    local = ids - shard * VOCAB

    def packed(gains):
        mine = jnp.where(owner == shard, rank, -1)
        hit = mine[:, None, :] == jnp.arange(CAP)[None, :, None]
        owned = jnp.sum(jnp.where(hit, local[:, None, :], 0), axis=2)
        slot = lax.dynamic_index_in_dim(owner * CAP + rank, shard, 0, keepdims=False)
        return exchange_rows(pack_rows(owned, embed), slot[:, None], gains, 0)

    def general(gains):
        flat = local.reshape(-1)
        inside = (flat >= 0) & (flat < VOCAB)
        rows = jnp.take(embed, jnp.clip(flat, 0, VOCAB - 1), axis=0)
        return embed_sum(jnp.where(inside[:, None], rows, jnp.zeros_like(rows)), gains, 6)

    return lax.cond(jnp.max(rank) < CAP, packed, general, gains)


def embed_kernel(rows_ref, gains_ref, hidden_ref, normed_ref, acc, tbuf, rbuf, send, recv):
    at = places()
    entry_barrier(at)
    scatter = Scatter(at, tbuf, rbuf, send, recv)

    def body(pos, carry):
        acc[...] = rows_ref[pick(pos, ORDER_EMBED, at)].astype(F32)
        scatter.after(pos, acc, far_first=True)
        return carry

    lax.fori_loop(0, N, body, 0)
    scatter.finish(acc, None, gains_ref[0:1, :], hidden_ref, normed_ref)


def embed_sum(rows, gains, ident):
    return pl.pallas_call(
        embed_kernel,
        out_shape=RESIDUAL,
        in_specs=[VM, VM], out_specs=(VM, VM),
        scratch_shapes=scatter_scratch(),
        compiler_params=comm_params(ident),
    )(rows.reshape(N, ROWS, D), gains)


HALF = 32
SLOTS = 4


def attend_half(base, start_ref, first_seq, qk, vv, planes, mixed_out):
    lane = lax.broadcasted_iota(jnp.int32, (8, 128), 1)
    row = lax.broadcasted_iota(jnp.int32, (8, 128), 0)
    first = lane < HEAD
    own = [(2 * j + lax.div(lane, HEAD)) == row for j in range(4)]
    groups = range(HALF // 8)

    def spread(twice):
        return jnp.concatenate([jnp.where(own[j], twice, 0.0) for j in range(4)], axis=1)

    starts = [start_ref[pl.ds(pl.multiple_of(first_seq + base + 8 * g, 8), 8), :] for g in groups]
    query, updates = [], []
    for g in groups:
        queries, keys, vals, hot = [], [], [], []
        for s in range(STEPS):
            span = pl.ds(pl.multiple_of(s * SEQS + base + 8 * g, 8), 8)
            left, right = qk[span, 0:128], qk[span, 128:256]
            left_r, right_r = pltpu.roll(left, HEAD, 1), pltpu.roll(right, HEAD, 1)
            queries += [spread(jnp.where(first, left, left_r)), spread(jnp.where(first, left_r, left)),
                        spread(jnp.where(first, right, right_r))]
            keys.append(spread(jnp.where(first, right_r, right)))
            vals.append(spread(vv[span, :]))
            hot.append(jnp.where(lane == starts[g] + s, 1.0, 0.0))
        query.append(jnp.concatenate(queries, axis=0).astype(BF16))
        hot_all = jnp.concatenate(hot, axis=0).astype(BF16)
        updates.append([
            lax.dot_general(jnp.concatenate(entry, axis=0).astype(BF16), hot_all, (((0,), (0,)), ((), ())),
                            preferred_element_type=F32) for entry in (keys, vals)])
    for g in groups:
        span = pl.ds(base + 8 * g, 8)
        fresh = jnp.where((lane >= starts[g]) & (lane < starts[g] + STEPS), 1.0, 0.0)
        fresh = jnp.broadcast_to(fresh[:, None, :], (8, HEAD, 128)) > 0.5
        for kind in range(2):
            old = planes[kind, span].astype(F32)
            planes[kind, span] = jnp.where(fresh, updates[g][kind].reshape(8, HEAD, 128), old).astype(BF16)
    scores = [jnp.dot(query[g], planes[0, pl.ds(base + 8 * g, 8)].reshape(8 * HEAD, 128), preferred_element_type=F32)
              for g in groups]
    probs = []
    for g in groups:
        valid = [jnp.where(lane <= starts[g] + s, 0.0, -jnp.inf) for s in range(STEPS)]
        score = scores[g] * ATT_SCALE + jnp.concatenate([valid[s] for s in range(STEPS) for h in range(3)], axis=0)
        weight = jnp.exp(score - jnp.max(score, axis=1, keepdims=True))
        probs.append((weight / jnp.sum(weight, axis=1, keepdims=True)).astype(BF16))
    mixed = [lax.dot_general(probs[g], planes[1, pl.ds(base + 8 * g, 8)].reshape(8 * HEAD, 128),
                             (((1,), (1,)), ((), ())), preferred_element_type=F32) for g in groups]
    for g in groups:
        for s in range(STEPS):
            span = pl.ds(pl.multiple_of(s * SEQS + base + 8 * g, 8), 8)
            heads = []
            for h in range(3):
                part = mixed[g][8 * (3 * s + h):8 * (3 * s + h) + 8, :]
                total = sum(jnp.where(own[j], part[:, 128 * j:128 * j + 128], 0.0) for j in range(4))
                heads.append(total + pltpu.roll(total, HEAD, 1))
            mixed_out[span, 0:128] = jnp.where(first, heads[0], heads[1])
            mixed_out[span, 128:256] = heads[2]


def attn_kernel(layer, u_ref, table_ref, start_ref, gains_ref, hidden_hbm, wq_ref, wk_ref, wv_ref, wo_ref, cache_ref,
                *rest):
    if layer > 0:
        rest = rest[1:]
    (hidden_ref, normed_ref, new_ref, ubuf, ag_send, ag_recv, acc, tbuf, rbuf, rs_send, rs_recv,
     qk, vv, mixed, planes, w_qkv, w_out, hidden_in, in_sem, out_sem, w_sem) = rest
    at = places()
    weights = [
        pltpu.make_async_copy(wq_ref.at[layer], w_qkv.at[0:192], w_sem.at[0]),
        pltpu.make_async_copy(wk_ref.at[layer], w_qkv.at[192:256], w_sem.at[1]),
        pltpu.make_async_copy(wv_ref.at[layer], w_qkv.at[256:320], w_sem.at[2]),
        pltpu.make_async_copy(wv_ref.at[layer], w_qkv.at[320:384], w_sem.at[3]),
        pltpu.make_async_copy(wo_ref.at[layer], w_out.at[0:192], w_sem.at[4])]
    for item in weights:
        item.start()
    residual = pltpu.make_async_copy(hidden_hbm, hidden_in, w_sem.at[5])
    residual.start()
    w_out[192:256, :] = jnp.zeros((64, D), BF16)

    def plane_span(pos):
        return pl.ds(pick(pos, ORDER_RS, at) * SEQS, SEQS)

    def load(pos):
        slot = lax.rem(pos, SLOTS)
        return pltpu.make_async_copy(cache_ref.at[layer, :, plane_span(pos)], planes.at[slot], in_sem.at[slot])

    def store(pos):
        slot = lax.rem(pos, SLOTS)
        return pltpu.make_async_copy(planes.at[slot], new_ref.at[layer, :, plane_span(pos)], out_sem.at[slot])

    load(jnp.int32(0)).start()
    load(jnp.int32(1)).start()
    entry_barrier(at)
    gather = Gather(at, u_ref, ubuf, ag_send, ag_recv)
    scatter = Scatter(at, tbuf, rbuf, rs_send, rs_recv)
    gather.start(0, 2)
    ubuf[at["me"]] = u_ref[...]
    for item in weights:
        item.wait()

    def body(pos, carry):
        gather.before(pos, ORDER_RS)
        blk = pick(pos, ORDER_RS, at)

        @pl.when(pos >= 2)
        def _():
            store(pos - 2).wait()

        @pl.when(pos < N - 2)
        def _():
            load(pos + 2).start()

        out = lax.dot_general(ubuf[blk], w_qkv[...], (((1,), (1,)), ((), ())), preferred_element_type=F32)
        start = start_ref[pl.ds(pl.multiple_of(blk * SEQS, SEQS), SEQS), :]
        lane = lax.broadcasted_iota(jnp.int32, (SEQS, 128), 1)
        hot = jnp.concatenate([jnp.where(lane == start + s, 1.0, 0.0) for s in range(STEPS)], axis=0)
        turn = jnp.dot(hot, table_ref[...], precision=lax.Precision.HIGHEST, preferred_element_type=F32)
        cos = turn[:, 0:128]
        sin = turn[:, 128:256]
        low = lax.rem(lax.broadcasted_iota(jnp.int32, (ROWS, 128), 1), HEAD) < HEAD // 2
        for half in range(2):
            part = out[:, half * 128:(half + 1) * 128]
            swapped = jnp.where(low, pltpu.roll(part, 128 - HEAD // 2, 1), pltpu.roll(part, HEAD // 2, 1))
            qk[:, half * 128:(half + 1) * 128] = (part * cos + swapped * sin).astype(BF16).astype(F32)
        vv[...] = out[:, 256:384].astype(BF16).astype(F32)
        load(pos).wait()

        def half_block(i, carry):
            attend_half(i * HALF, start_ref, blk * SEQS, qk, vv, planes.at[lax.rem(pos, SLOTS)], mixed)
            return carry

        lax.fori_loop(0, SEQS // HALF, half_block, 0)
        store(pos).start()
        acc[...] = jnp.dot(mixed[...].astype(BF16), w_out[...], preferred_element_type=F32)
        scatter.after(pos, acc)
        return carry

    lax.fori_loop(0, N, body, 0)
    store(jnp.int32(N - 2)).wait()
    store(jnp.int32(N - 1)).wait()
    gather.finish()
    residual.wait()
    scatter.finish(acc, hidden_in, gains_ref[2 * layer + 1:2 * layer + 2, :], hidden_ref, normed_ref)


def attention(layer, u, table, start_wide, hidden, gains, weights, cache, new_cache, ident):
    args = [u, table, start_wide, gains, hidden, *weights, cache]
    in_specs = [VM] * 4 + [ANY] * 6
    aliases = {}
    if new_cache is not None:
        args.append(new_cache)
        in_specs.append(ANY)
        aliases = {10: 2}
    return pl.pallas_call(
        functools.partial(attn_kernel, layer),
        out_shape=RESIDUAL + (jax.ShapeDtypeStruct(cache.shape, BF16),),
        in_specs=in_specs, out_specs=(VM, VM, ANY),
        scratch_shapes=gather_scratch() + scatter_scratch() + [
            pltpu.VMEM((ROWS, 256), F32), pltpu.VMEM((ROWS, 128), F32), pltpu.VMEM((ROWS, 256), F32),
            pltpu.VMEM((SLOTS, 2, SEQS, HEAD, CACHE), BF16), pltpu.VMEM((384, D), BF16), pltpu.VMEM((256, D), BF16),
            pltpu.VMEM((ROWS, D), F32), pltpu.SemaphoreType.DMA((SLOTS,)), pltpu.SemaphoreType.DMA((SLOTS,)),
            pltpu.SemaphoreType.DMA((6,))],
        input_output_aliases=aliases,
        compiler_params=comm_params(ident),
    )(*args)


def moe_kernel(layer, u_ref, router_ref, ids_ref, gains_ref, hidden_hbm, gate_hbm, up_hbm, down_hbm, hidden_ref, normed_ref,
               ubuf, ag_send, ag_recv, acc, tbuf, rbuf, rs_send, rs_recv, gate_v, up_v, down_v, hidden, gates, hidden_in, w_sem):
    def load(kind, e):
        src, dst = ((gate_hbm, gate_v), (up_hbm, up_v))[kind]
        return pltpu.make_async_copy(src.at[layer, e], dst.at[e], w_sem.at[kind, e])

    down_load = pltpu.make_async_copy(down_hbm.at[layer], down_v, w_sem.at[2, 0])
    for e in range(LOCAL_EXPERTS):
        load(0, e).start()
        load(1, e).start()
    down_load.start()
    residual = pltpu.make_async_copy(hidden_hbm, hidden_in, w_sem.at[2, 1])
    residual.start()
    at = places()
    entry_barrier(at)
    gather = Gather(at, u_ref, ubuf, ag_send, ag_recv)
    scatter = Scatter(at, tbuf, rbuf, rs_send, rs_recv)
    gather.start(0, 2)
    ubuf[at["me"]] = u_ref[...]
    lane = lax.broadcasted_iota(jnp.int32, (ROWS, EXPERTS), 1)

    def route(blk):
        ids = ids_ref[blk]
        chosen = lane == ids[:, 0:1]
        for j in range(1, 8):
            chosen = chosen | (lane == ids[:, j:j + 1])
        score = lax.dot_general(ubuf[blk], router_ref[layer], (((1,), (1,)), ((), ())), preferred_element_type=F32)
        masked = jnp.where(chosen, score, -jnp.inf)
        weight = jnp.exp(masked - jnp.max(masked, axis=1, keepdims=True))
        gates[...] = weight / jnp.sum(weight, axis=1, keepdims=True)

    def inner(blk, e):
        return (jnp.dot(ubuf[blk], gate_v[e], preferred_element_type=F32),
                jnp.dot(ubuf[blk], up_v[e], preferred_element_type=F32))

    def activate(e, gate_act, up_act):
        share = jnp.sum(jnp.where(lane == at["me"] * LOCAL_EXPERTS + e, gates[...], 0.0), axis=1, keepdims=True)
        z = gate_act * jax.nn.sigmoid(gate_act) * up_act * share
        start = e * FF if isinstance(e, int) else pl.multiple_of(e * FF, FF)
        hidden[:, pl.ds(start, FF)] = z.astype(BF16)

    def down():
        for c in range(D // 512):
            cols = slice(c * 512, c * 512 + 512)
            acc[:, cols] = jnp.dot(hidden[...], down_v[:, cols], preferred_element_type=F32)

    def first_expert(e, carry):
        load(0, e).wait()
        load(1, e).wait()
        activate(e, *inner(at["sib"], e))
        return carry

    gather.before(jnp.int32(0), ORDER_RS)
    route(at["sib"])
    lax.fori_loop(0, LOCAL_EXPERTS, first_expert, 0)
    down_load.wait()
    down()
    scatter.after(jnp.int32(0), acc)

    def body(pos, carry):
        gather.before(pos, ORDER_RS)
        blk = pick(pos, ORDER_RS, at)
        acts = inner(blk, 0)
        route(blk)
        for e in range(LOCAL_EXPERTS):
            following = inner(blk, e + 1) if e + 1 < LOCAL_EXPERTS else None
            activate(e, *acts)
            acts = following
        down()
        scatter.after(pos, acc)
        return carry

    lax.fori_loop(1, N, body, 0)
    gather.finish()
    residual.wait()
    scatter.finish(acc, hidden_in, gains_ref[2 * layer + 2:2 * layer + 3, :], hidden_ref, normed_ref)


def experts(layer, u, router, ids, hidden, gains, w_gate, w_up, w_down, ident):
    width = LOCAL_EXPERTS * FF
    return pl.pallas_call(
        functools.partial(moe_kernel, layer),
        out_shape=RESIDUAL,
        in_specs=[VM] * 4 + [ANY] * 4, out_specs=(VM, VM),
        scratch_shapes=gather_scratch() + scatter_scratch() + [
            pltpu.VMEM((LOCAL_EXPERTS, D, FF), BF16), pltpu.VMEM((LOCAL_EXPERTS, D, FF), BF16),
            pltpu.VMEM((width, D), BF16), pltpu.VMEM((ROWS, width), BF16), pltpu.VMEM((ROWS, EXPERTS), F32),
            pltpu.VMEM((ROWS, D), F32),
            pltpu.SemaphoreType.DMA((3, LOCAL_EXPERTS))],
        compiler_params=comm_params(ident),
    )(u, router, ids, gains, hidden, w_gate, w_up, w_down.reshape(LAYERS, width, D))


TILE = 512
TILES = VOCAB // TILE
LAST_TILE = 384


LOG2E = 1.4426950408889634


def fold(logits, column, target, stat):
    part = logits.reshape(TILE // 8, 8, ROWS)
    peak = stat[0]
    top = jnp.maximum(peak, jnp.max(part, axis=0))
    stat[0] = top
    stat[1] = stat[1] * jnp.exp2((peak - top) * (LOG2E / LOGIT_DIV)) + jnp.sum(
        jnp.exp2((part - top) * (LOG2E / LOGIT_DIV)), axis=0)
    here = target - column // 8 if isinstance(column, int) else target - lax.div(column, 8)
    picked = stat[2]
    for g in range(TILE // 8):
        picked = jnp.where(here == g, part[g], picked)
    stat[2] = picked


def head_kernel(f_ref, target_ref, embed_ref, probs_ref, last_ref, ubuf, send, recv, table, even, odd, stat, mine, theirs,
                share_send, share_recv, sem):
    def load(c):
        rows = pl.ds(pl.multiple_of(c * TILE, TILE), TILE)
        return pltpu.make_async_copy(embed_ref.at[rows], table.at[rows], sem.at[c])

    for c in range(TILES):
        load(c).start()
    at = places()
    entry_barrier(at, ORDER_AG[1:])
    gather = Gather(at, f_ref, ubuf, send, recv)
    gather.start(0, 2)
    ubuf[at["me"]] = f_ref[...]

    def tile_logits(blk, start):
        return lax.dot_general(table[pl.ds(start, TILE), :], ubuf[blk], (((1,), (1,)), ((), ())), preferred_element_type=F32)

    def group_of(blk):
        local = jnp.broadcast_to(target_ref[blk], (8, ROWS))
        sub = lax.broadcasted_iota(jnp.int32, (8, ROWS), 0)
        return jnp.where((local >= 0) & ((local & 7) == sub), local >> 3, -1 - VOCAB)

    def begin():
        stat[0] = jnp.full((8, ROWS), -1e30, F32)
        stat[1] = jnp.zeros((8, ROWS), F32)
        stat[2] = jnp.zeros((8, ROWS), F32)

    def end(blk):
        peak = stat[0]
        top = jnp.max(peak, axis=0, keepdims=True)
        mine[0, pl.ds(blk, 1), :] = top
        mine[1, pl.ds(blk, 1), :] = jnp.sum(stat[1] * jnp.exp2((peak - top) * (LOG2E / LOGIT_DIV)), axis=0, keepdims=True)
        mine[2, pl.ds(blk, 1), :] = jnp.sum(stat[2], axis=0, keepdims=True)
        last_ref[blk] = ubuf[blk, ROWS - SEQS:ROWS, :]

    def first_tiles(i, carry):
        group = group_of(at["me"])
        bufs = (even, odd)
        for j in range(2):
            load(2 * i + j).wait()
            bufs[j][...] = tile_logits(at["me"], pl.multiple_of((2 * i + j) * TILE, TILE))
        for j in range(2):
            fold(bufs[j][...], (2 * i + j) * TILE, group, stat)
        return carry

    begin()
    lax.fori_loop(0, TILES // 2, first_tiles, 0)
    end(at["me"])

    def body(pos, carry):
        gather.before(pos, ORDER_AG)
        blk = pick(pos, ORDER_AG, at)
        target = group_of(blk)
        begin()
        bufs = (even, odd)
        even[...] = tile_logits(blk, 0)
        for c in range(1, TILES + 1):
            if c < TILES:
                bufs[c % 2][...] = tile_logits(blk, c * TILE)
            fold(bufs[(c - 1) % 2][...], (c - 1) * TILE, target, stat)
        end(blk)
        return carry

    lax.fori_loop(1, N, body, 0)
    gather.finish()
    me = at["me"]
    copies = [pltpu.make_async_remote_copy(
        src_ref=mine, dst_ref=theirs.at[shift], send_sem=share_send.at[shift], recv_sem=share_recv.at[shift],
        device_id={"tp": lax.rem(me + shift, N)}, device_id_type=MESH) for shift in range(1, N)]
    for item in copies:
        item.start()
    theirs[0] = mine[...]
    for item in copies:
        item.wait()
    peak = functools.reduce(jnp.maximum, [theirs[i, 0] for i in range(N)])
    total = sum(theirs[i, 1] * jnp.exp2((theirs[i, 0] - peak) * (LOG2E / LOGIT_DIV)) for i in range(N))
    picked = sum(theirs[i, 2] for i in range(N))
    probs_ref[...] = (picked - peak) * (1.0 / LOGIT_DIV) - jnp.log(total)


def head(f, target, embed, ident):
    return pl.pallas_call(
        head_kernel,
        out_shape=(jax.ShapeDtypeStruct((N, ROWS), F32), jax.ShapeDtypeStruct((N, SEQS, D), BF16)),
        in_specs=[VM, VM, ANY], out_specs=(VM, VM),
        scratch_shapes=gather_scratch() + [
            pltpu.VMEM((VOCAB, D), BF16), pltpu.VMEM((TILE, ROWS), F32), pltpu.VMEM((TILE, ROWS), F32),
            pltpu.VMEM((3, 8, ROWS), F32), pltpu.VMEM((3, N, ROWS), F32), pltpu.VMEM((N, 3, N, ROWS), F32),
            pltpu.SemaphoreType.DMA((N,)), pltpu.SemaphoreType.DMA((N,)), pltpu.SemaphoreType.DMA((TILES,))],
        compiler_params=comm_params(ident),
    )(f, target, embed)


LAST_STEPS = VOCAB // LAST_TILE
PLANES = LAYERS * 2 * BATCH // LAST_STEPS
RING = 8
AHEAD = 4


def last_kernel(f_ref, embed_ref, cache_ref, logits_ref, new_ref, ring, in_sem, out_sem):
    c = pl.program_id(0)

    def load(i):
        slot = lax.rem(i, RING)
        return pltpu.make_async_copy(cache_ref.at[pl.ds(i * PLANES, PLANES)], ring.at[slot], in_sem.at[slot])

    def store(i):
        slot = lax.rem(i, RING)
        return pltpu.make_async_copy(ring.at[slot], new_ref.at[pl.ds(i * PLANES, PLANES)], out_sem.at[slot])

    @pl.when(c == 0)
    def _():
        for i in range(AHEAD):
            load(jnp.int32(i)).start()

    @pl.when((c >= RING - AHEAD) & (c < LAST_STEPS - AHEAD))
    def _():
        store(c + AHEAD - RING).wait()

    @pl.when(c < LAST_STEPS - AHEAD)
    def _():
        load(c + AHEAD).start()

    load(c).wait()
    store(c).start()
    logits_ref[...] = lax.dot_general(f_ref[...], embed_ref[...], (((1,), (1,)), ((), ())),
                                      preferred_element_type=F32) * (1.0 / LOGIT_DIV)

    @pl.when(c == LAST_STEPS - 1)
    def _():
        for i in range(LAST_STEPS - RING, LAST_STEPS):
            store(jnp.int32(i)).wait()


def last_step(f, embed, cache):
    flat = cache.reshape(LAYERS * 2 * BATCH, HEAD, CACHE)
    logits, flat = pl.pallas_call(
        last_kernel,
        out_shape=(jax.ShapeDtypeStruct((BATCH, VOCAB), F32), jax.ShapeDtypeStruct(flat.shape, BF16)),
        grid=(LAST_STEPS,),
        in_specs=[pl.BlockSpec((BATCH, D), lambda c: (0, 0)), pl.BlockSpec((LAST_TILE, D), lambda c: (c, 0)), ANY],
        out_specs=(pl.BlockSpec((BATCH, LAST_TILE), lambda c: (0, c)), ANY),
        scratch_shapes=[pltpu.VMEM((RING, PLANES, HEAD, CACHE), BF16), pltpu.SemaphoreType.DMA((RING,)),
                        pltpu.SemaphoreType.DMA((RING,))],
        compiler_params=pltpu.CompilerParams(dimension_semantics=("arbitrary",), vmem_limit_bytes=VMEM_LIMIT),
    )(f, embed, flat)
    return logits, flat.reshape(cache.shape)


def by_block(values):
    return values.reshape(N, SEQS, values.shape[1]).transpose(0, 2, 1)


def solution(mesh):
    cache_spec = P(None, None, 'dp', None, 'tp', None)
    expert_spec = P(None, 'tp', None, None)
    in_specs = (P('dp', None), P('dp'), cache_spec, P(None, None, 'dp', None), P('tp', None), P(None, None), P(None, None, 'tp'), P(None, None, 'tp'), P(None, None, 'tp'), P(None, 'tp', None), P(None, None, None), expert_spec, expert_spec, expert_spec)
    out_specs = (P('dp', None), P('dp', 'tp'), cache_spec)

    def decode_local(tokens, start_pos, kv_cache, expert_ids, embed, norm_gain, w_query, w_key, w_value, w_out, w_router, w_gate, w_up, w_down):
        shard = lax.axis_index('tp')
        cache = kv_cache.transpose(0, 1, 2, 4, 5, 3).reshape(LAYERS, 2, BATCH, HEAD, CACHE)

        ids = by_block(tokens[:, :STEPS]).reshape(N, ROWS)
        hidden, normed = embed_tokens(ids, shard, embed, norm_gain)

        inv_freq = ROPE_THETA ** (-2.0 * jnp.arange(HEAD // 2, dtype=F32) / HEAD)
        angles = jnp.arange(CACHE, dtype=F32)[:, None] * jnp.tile(inv_freq, 4)
        sign = jnp.where(jnp.arange(128) % HEAD < HEAD // 2, -1.0, 1.0)
        table = jnp.concatenate([jnp.cos(angles), jnp.sin(angles) * sign], axis=1)
        start_wide = jnp.broadcast_to(start_pos[:, None], (BATCH, 128))

        weights = [w.transpose(0, 2, 1) for w in (w_query, w_key, w_value)] + [w_out]
        router = w_router.transpose(0, 2, 1)
        routed = expert_ids.reshape(STEPS, LAYERS, N, SEQS, 8).transpose(1, 2, 0, 3, 4).reshape(LAYERS, N, ROWS, 8)

        new_cache = None
        for layer in range(LAYERS):
            hidden, normed, new_cache = attention(layer, normed, table, start_wide, hidden, norm_gain, weights, cache, new_cache,
                                                  1 + 2 * layer)
            hidden, normed = experts(layer, normed, router, routed[layer], hidden, norm_gain, w_gate, w_up, w_down, 2 + 2 * layer)

        target = by_block(tokens[:, 1:] - shard * VOCAB).reshape(N, 1, ROWS)
        log_probs, f_last = head(normed, target, embed, 5)
        logits, new_cache = last_step(f_last.reshape(BATCH, D), embed, new_cache)
        log_probs = log_probs.reshape(N, STEPS, SEQS).transpose(0, 2, 1).reshape(BATCH, STEPS)
        new_cache = new_cache.reshape(LAYERS, 2, BATCH, 1, HEAD, CACHE).transpose(0, 1, 2, 5, 3, 4)
        return log_probs, logits, new_cache

    return jax.shard_map(decode_local, mesh=mesh, in_specs=in_specs, out_specs=out_specs, check_vma=False)
```

```python
import functools

import jax
import jax.numpy as jnp
from jax import lax
from jax.experimental import pallas as pl
from jax.experimental.pallas import tpu as pltpu
from jax.sharding import PartitionSpec as P

EMBED_MULT = 12.0
ATT_SCALE = 0.015625
RESID_MULT = 0.22
LOGIT_DIV = 6.0
NORM_EPS = 1e-6
ROPE_THETA = 10000.0

D = 1536
HEAD = 64
BATCH = 512
STEPS = 4
LAYERS = 2
CACHE = 128
EXPERTS = 40
LOCAL_EXPERTS = 5
FF = 512
VOCAB = 6144
N = 8
SEQS = BATCH // N
ROWS = SEQS * STEPS
MESH = pl.DeviceIdType.MESH
F32 = jnp.float32
BF16 = jnp.bfloat16
VMEM_LIMIT = 60 * 1024 * 1024

ORDER_RS = ("sib", "bs", "a", "ds", "dg", "as", "b", "me")
ORDER_AG = ("me", "sib", "bs", "a", "ds", "dg", "as", "b")
ORDER_EMBED = ("sib", "ds", "dg", "bs", "a", "as", "b", "me")


def places():
    me = lax.axis_index("tp")
    k = lax.rem(me, 2)
    x = lax.rem(lax.div(me, 2), 2)
    y = lax.div(me, 4)
    step_x = 2 - 4 * x
    step_y = 4 - 8 * y
    a = me + step_x + k * (step_y - step_x)
    b = me + step_y + k * (step_x - step_y)
    dg = me + step_x + step_y
    s = 1 - 2 * k
    return {"me": me, "sib": me + s, "a": a, "as": a + s, "b": b, "bs": b + s, "dg": dg, "ds": dg + s}


def entry_barrier(at, names=("sib", "a", "b")):
    barrier = pltpu.get_barrier_semaphore()
    for name in names:
        pl.semaphore_signal(barrier, inc=1, device_id={"tp": at[name]}, device_id_type=MESH)
    pl.semaphore_wait(barrier, len(names))


def pick(pos, order, at):
    total = jnp.int32(0)
    for i, name in enumerate(order):
        total = total + jnp.where(pos == i, at[name], 0)
    return total


class Gather:
    def __init__(self, at, own, ubuf, send, recv):
        self.at, self.own, self.ubuf, self.send, self.recv = at, own, ubuf, send, recv

    def copy(self, src, origin, target, slot):
        return pltpu.make_async_remote_copy(
            src_ref=src, dst_ref=self.ubuf.at[origin], send_sem=self.send.at[slot], recv_sem=self.recv.at[origin],
            device_id={"tp": target}, device_id_type=MESH)

    def item(self, slot):
        at = self.at
        if slot < 3:
            return self.copy(self.own, at["me"], at[("a", "b", "sib")[slot]], slot)
        name, target = (("a", "b"), ("a", "sib"), ("b", "sib"), ("dg", "sib"))[slot - 3]
        return self.copy(self.ubuf.at[at[name]], at[name], at[target], slot)

    def start(self, *slots):
        for slot in slots:
            self.item(slot).start()

    def arrive(self, name):
        origin = self.at[name]
        self.copy(self.own, origin, self.at["sib"], 0).wait_recv()

    def before(self, pos, order):
        @pl.when(pos == order.index("sib"))
        def _():
            self.arrive("sib")

        @pl.when(pos == order.index("bs"))
        def _():
            self.arrive("a")
            self.start(3, 4, 1)
            self.arrive("bs")

        @pl.when(pos == order.index("ds"))
        def _():
            self.arrive("dg")
            self.start(6)
            self.arrive("ds")

        @pl.when(pos == order.index("as"))
        def _():
            self.arrive("b")
            self.start(5)
            self.arrive("as")

    def finish(self):
        for slot in range(7):
            self.item(slot).wait_send()


class Scatter:
    def __init__(self, at, tbuf, rbuf, send, recv):
        self.at, self.tbuf, self.rbuf, self.send, self.recv = at, tbuf, rbuf, send, recv

    def copy(self, slot, target):
        return pltpu.make_async_remote_copy(
            src_ref=self.tbuf.at[slot], dst_ref=self.rbuf.at[slot], send_sem=self.send.at[slot],
            recv_sem=self.recv.at[slot], device_id={"tp": target}, device_id_type=MESH)

    def arrive(self, slot):
        self.copy(slot, self.at["sib"]).wait_recv()

    def after(self, pos, acc, far_first=False):
        at = self.at

        @pl.when((pos == 0) | (pos == 1) | (pos == 3) | (pos == 5))
        def _():
            slot = lax.div(pos + 1, 2)
            self.tbuf[slot] = acc[...].astype(BF16)
            self.copy(slot, at["sib"]).start()

        @pl.when((pos == 2) | (pos == 4))
        def _():
            slot = lax.div(pos, 2)
            out = 6 - slot if far_first else slot + 3
            self.arrive(slot)
            self.tbuf[out] = (acc[...] + self.rbuf[slot].astype(F32)).astype(BF16)
            self.copy(out, at["a"]).start()

        @pl.when(pos == 6)
        def _():
            self.arrive(3)
            self.arrive(5)
            self.tbuf[6] = (acc[...] + self.rbuf[3].astype(F32) + self.rbuf[5].astype(F32)).astype(BF16)
            self.copy(6, at["b"]).start()

    def finish(self, acc, hidden_in, gain, hidden_ref, normed_ref):
        self.arrive(0)
        self.arrive(4)
        self.arrive(6)

        def chunk(c, carry):
            rows = pl.ds(pl.multiple_of(c * 32, 32), 32)
            total = acc[rows, :]
            for slot in (0, 4, 6):
                total = total + self.rbuf[slot, rows, :].astype(F32)
            total = total.astype(BF16).astype(F32)
            if hidden_in is None:
                hidden = EMBED_MULT * total
            else:
                hidden = hidden_in[rows, :] + RESID_MULT * total
            hidden_ref[rows, :] = hidden
            mean_sq = jnp.mean(hidden * hidden, axis=1, keepdims=True)
            normed_ref[rows, :] = (hidden * lax.rsqrt(mean_sq + NORM_EPS) * gain).astype(BF16)
            return carry

        lax.fori_loop(0, ROWS // 32, chunk, 0)
        for slot in range(7):
            self.copy(slot, self.at["sib"]).wait_send()


def gather_scratch():
    return [pltpu.VMEM((N, ROWS, D), BF16), pltpu.SemaphoreType.DMA((7,)), pltpu.SemaphoreType.DMA((N,))]


def scatter_scratch():
    return [pltpu.VMEM((ROWS, D), F32), pltpu.VMEM((7, ROWS, D), BF16),
            pltpu.VMEM((7, ROWS, D), BF16), pltpu.SemaphoreType.DMA((7,)), pltpu.SemaphoreType.DMA((7,))]


VM = pl.BlockSpec(memory_space=pltpu.VMEM)
RESIDUAL = (jax.ShapeDtypeStruct((ROWS, D), F32), jax.ShapeDtypeStruct((ROWS, D), BF16))
ANY = pl.BlockSpec(memory_space=pl.ANY)


def comm_params(ident):
    return pltpu.CompilerParams(collective_id=ident, has_side_effects=True, vmem_limit_bytes=VMEM_LIMIT)


CAP = 64


def pack_kernel(count_ref, group_ref, place_ref, embed_ref, out_ref, buf, sem):
    def copy(group, d, j):
        return pltpu.make_async_copy(embed_ref.at[group], buf.at[d, j], sem.at[d])

    def issue(d, carry):
        def eight(i, carry):
            for j in range(8):
                copy(group_ref[d * CAP + 8 * i + j], d, 8 * i + j).start()
            return carry

        lax.fori_loop(0, count_ref[d], eight, 0)
        return carry

    def place(d, carry):
        def eight(i, carry):
            pltpu.make_async_copy(embed_ref.at[0:8], buf.at[d, pl.ds(8 * i, 8)], sem.at[d]).wait()
            return carry

        def blank(i, carry):
            buf[d, pl.ds(8 * i, 8)] = jnp.zeros((8, 8, D), BF16)
            return carry

        lax.fori_loop(count_ref[d], CAP // 8, blank, 0)
        lax.fori_loop(0, count_ref[d], eight, 0)
        lane = lax.broadcasted_iota(jnp.int32, (CAP, 8 * CAP), 1)
        one_hot = jnp.where(lane == place_ref[d], 1.0, 0.0).astype(BF16)
        out_ref[d] = jnp.dot(one_hot, buf[d].reshape(8 * CAP, D), preferred_element_type=F32).astype(BF16)
        return carry

    lax.fori_loop(0, N, issue, 0)
    lax.fori_loop(0, N, place, 0)


def pack_rows(count, owned, embed):
    group = lax.div(owned, 8).reshape(-1)
    place = (8 * jnp.arange(CAP) + lax.rem(owned, 8)).reshape(N, CAP, 1)
    return pl.pallas_call(
        pack_kernel,
        out_shape=jax.ShapeDtypeStruct((N, CAP, D), BF16),
        grid_spec=pltpu.PrefetchScalarGridSpec(
            num_scalar_prefetch=2, grid=(1,),
            in_specs=[pl.BlockSpec((N, CAP, 1), lambda i, *_: (0, 0, 0)), ANY],
            out_specs=pl.BlockSpec((N, CAP, D), lambda i, *_: (0, 0, 0)),
            scratch_shapes=[pltpu.VMEM((N, CAP, 8, D), BF16), pltpu.SemaphoreType.DMA((N,))]),
        compiler_params=pltpu.CompilerParams(vmem_limit_bytes=VMEM_LIMIT),
    )(count, group, place, embed.reshape(VOCAB // 8, 8, D))


def exchange_kernel(packed_ref, slot_ref, gains_ref, hidden_ref, normed_ref, held, send, recv):
    me = lax.axis_index("tp")
    barrier = pltpu.get_barrier_semaphore()
    for shift in range(1, N):
        pl.semaphore_signal(barrier, inc=1, device_id={"tp": lax.rem(me + shift, N)}, device_id_type=MESH)
    pl.semaphore_wait(barrier, N - 1)

    def copy(target, origin, shift):
        return pltpu.make_async_remote_copy(
            src_ref=packed_ref.at[target], dst_ref=held.at[origin], send_sem=send.at[shift], recv_sem=recv.at[shift],
            device_id={"tp": target}, device_id_type=MESH)

    for shift in range(1, N):
        copy(lax.rem(me + shift, N), me, shift).start()
    held[me] = packed_ref[me]
    for shift in range(1, N):
        copy(lax.rem(me + shift, N), lax.rem(me + N - shift, N), shift).wait()

    def chunk(c, carry):
        rows = pl.ds(pl.multiple_of(c * 64, 64), 64)
        lane = lax.broadcasted_iota(jnp.int32, (64, N * CAP), 1)
        one_hot = jnp.where(lane == slot_ref[rows, :], 1.0, 0.0).astype(BF16)
        hidden = EMBED_MULT * jnp.dot(one_hot, held[...].reshape(N * CAP, D), preferred_element_type=F32)
        hidden_ref[rows, :] = hidden
        mean_sq = jnp.mean(hidden * hidden, axis=1, keepdims=True)
        normed_ref[rows, :] = (hidden * lax.rsqrt(mean_sq + NORM_EPS) * gains_ref[0:1, :]).astype(BF16)
        return carry

    lax.fori_loop(0, ROWS // 64, chunk, 0)


def exchange_rows(packed, slot, gains, ident):
    return pl.pallas_call(
        exchange_kernel,
        out_shape=RESIDUAL,
        in_specs=[VM] * 3, out_specs=(VM, VM),
        scratch_shapes=[pltpu.VMEM((N, CAP, D), BF16), pltpu.SemaphoreType.DMA((N,)), pltpu.SemaphoreType.DMA((N,))],
        compiler_params=comm_params(ident),
    )(packed, slot, gains)


def embed_tokens(ids, shard, embed, gains):
    owner = lax.div(ids, VOCAB)
    earlier = jnp.arange(ROWS)[:, None] > jnp.arange(ROWS)[None, :]
    rank = jnp.sum(((owner[:, :, None] == owner[:, None, :]) & earlier).astype(jnp.int32), axis=2)
    local = ids - shard * VOCAB

    def packed(gains):
        mine = jnp.where(owner == shard, rank, -1)
        hit = mine[:, None, :] == jnp.arange(CAP)[None, :, None]
        owned = jnp.sum(jnp.where(hit, local[:, None, :], 0), axis=2)
        slot = lax.dynamic_index_in_dim(owner * CAP + rank, shard, 0, keepdims=False)
        count = lax.div(jnp.max(mine, axis=1) + 8, 8)
        return exchange_rows(pack_rows(count, owned, embed), slot[:, None], gains, 0)

    def general(gains):
        flat = local.reshape(-1)
        inside = (flat >= 0) & (flat < VOCAB)
        rows = jnp.take(embed, jnp.clip(flat, 0, VOCAB - 1), axis=0)
        return embed_sum(jnp.where(inside[:, None], rows, jnp.zeros_like(rows)), gains, 6)

    return lax.cond(jnp.max(rank) < CAP, packed, general, gains)


def embed_kernel(rows_ref, gains_ref, hidden_ref, normed_ref, acc, tbuf, rbuf, send, recv):
    at = places()
    entry_barrier(at)
    scatter = Scatter(at, tbuf, rbuf, send, recv)

    def body(pos, carry):
        acc[...] = rows_ref[pick(pos, ORDER_EMBED, at)].astype(F32)
        scatter.after(pos, acc, far_first=True)
        return carry

    lax.fori_loop(0, N, body, 0)
    scatter.finish(acc, None, gains_ref[0:1, :], hidden_ref, normed_ref)


def embed_sum(rows, gains, ident):
    return pl.pallas_call(
        embed_kernel,
        out_shape=RESIDUAL,
        in_specs=[VM, VM], out_specs=(VM, VM),
        scratch_shapes=scatter_scratch(),
        compiler_params=comm_params(ident),
    )(rows.reshape(N, ROWS, D), gains)


HALF = 32
SLOTS = 4


def attend_half(base, start_ref, first_seq, qk, vv, planes, mixed_out):
    lane = lax.broadcasted_iota(jnp.int32, (8, 128), 1)
    row = lax.broadcasted_iota(jnp.int32, (8, 128), 0)
    first = lane < HEAD
    own = [(2 * j + lax.div(lane, HEAD)) == row for j in range(4)]
    groups = range(HALF // 8)

    def spread(twice):
        return jnp.concatenate([jnp.where(own[j], twice, 0.0) for j in range(4)], axis=1)

    starts = [start_ref[pl.ds(pl.multiple_of(first_seq + base + 8 * g, 8), 8), :] for g in groups]
    query, updates = [], []
    for g in groups:
        queries, keys, vals, hot = [], [], [], []
        for s in range(STEPS):
            span = pl.ds(pl.multiple_of(s * SEQS + base + 8 * g, 8), 8)
            left, right = qk[span, 0:128], qk[span, 128:256]
            left_r, right_r = pltpu.roll(left, HEAD, 1), pltpu.roll(right, HEAD, 1)
            queries += [spread(jnp.where(first, left, left_r)), spread(jnp.where(first, left_r, left)),
                        spread(jnp.where(first, right, right_r))]
            keys.append(spread(jnp.where(first, right_r, right)))
            vals.append(spread(vv[span, :]))
            hot.append(jnp.where(lane == starts[g] + s, 1.0, 0.0))
        query.append(jnp.concatenate(queries, axis=0).astype(BF16))
        hot_all = jnp.concatenate(hot, axis=0).astype(BF16)
        updates.append([
            lax.dot_general(jnp.concatenate(entry, axis=0).astype(BF16), hot_all, (((0,), (0,)), ((), ())),
                            preferred_element_type=F32) for entry in (keys, vals)])
    for g in groups:
        span = pl.ds(base + 8 * g, 8)
        fresh = jnp.where((lane >= starts[g]) & (lane < starts[g] + STEPS), 1.0, 0.0)
        fresh = jnp.broadcast_to(fresh[:, None, :], (8, HEAD, 128)) > 0.5
        for kind in range(2):
            old = planes[kind, span].astype(F32)
            planes[kind, span] = jnp.where(fresh, updates[g][kind].reshape(8, HEAD, 128), old).astype(BF16)
    scores = [jnp.dot(query[g], planes[0, pl.ds(base + 8 * g, 8)].reshape(8 * HEAD, 128), preferred_element_type=F32)
              for g in groups]
    probs = []
    for g in groups:
        valid = [jnp.where(lane <= starts[g] + s, 0.0, -jnp.inf) for s in range(STEPS)]
        score = scores[g] * ATT_SCALE + jnp.concatenate([valid[s] for s in range(STEPS) for h in range(3)], axis=0)
        weight = jnp.exp(score - jnp.max(score, axis=1, keepdims=True))
        probs.append((weight / jnp.sum(weight, axis=1, keepdims=True)).astype(BF16))
    mixed = [lax.dot_general(probs[g], planes[1, pl.ds(base + 8 * g, 8)].reshape(8 * HEAD, 128),
                             (((1,), (1,)), ((), ())), preferred_element_type=F32) for g in groups]
    for g in groups:
        for s in range(STEPS):
            span = pl.ds(pl.multiple_of(s * SEQS + base + 8 * g, 8), 8)
            heads = []
            for h in range(3):
                part = mixed[g][8 * (3 * s + h):8 * (3 * s + h) + 8, :]
                total = sum(jnp.where(own[j], part[:, 128 * j:128 * j + 128], 0.0) for j in range(4))
                heads.append(total + pltpu.roll(total, HEAD, 1))
            mixed_out[span, 0:128] = jnp.where(first, heads[0], heads[1])
            mixed_out[span, 128:256] = heads[2]


def attn_kernel(layer, u_ref, table_ref, start_ref, gains_ref, hidden_hbm, wq_ref, wk_ref, wv_ref, wo_ref, cache_ref,
                *rest):
    if layer > 0:
        rest = rest[1:]
    (hidden_ref, normed_ref, new_ref, ubuf, ag_send, ag_recv, acc, tbuf, rbuf, rs_send, rs_recv,
     qk, vv, mixed, planes, w_qkv, w_out, hidden_in, in_sem, out_sem, w_sem) = rest
    at = places()
    weights = [
        pltpu.make_async_copy(wq_ref.at[layer], w_qkv.at[0:192], w_sem.at[0]),
        pltpu.make_async_copy(wk_ref.at[layer], w_qkv.at[192:256], w_sem.at[1]),
        pltpu.make_async_copy(wv_ref.at[layer], w_qkv.at[256:320], w_sem.at[2]),
        pltpu.make_async_copy(wv_ref.at[layer], w_qkv.at[320:384], w_sem.at[3]),
        pltpu.make_async_copy(wo_ref.at[layer], w_out.at[0:192], w_sem.at[4])]
    for item in weights:
        item.start()
    residual = pltpu.make_async_copy(hidden_hbm, hidden_in, w_sem.at[5])
    residual.start()
    w_out[192:256, :] = jnp.zeros((64, D), BF16)

    def plane_span(pos):
        return pl.ds(pick(pos, ORDER_RS, at) * SEQS, SEQS)

    def load(pos):
        slot = lax.rem(pos, SLOTS)
        return pltpu.make_async_copy(cache_ref.at[layer, :, plane_span(pos)], planes.at[slot], in_sem.at[slot])

    def store(pos):
        slot = lax.rem(pos, SLOTS)
        return pltpu.make_async_copy(planes.at[slot], new_ref.at[layer, :, plane_span(pos)], out_sem.at[slot])

    load(jnp.int32(0)).start()
    load(jnp.int32(1)).start()
    entry_barrier(at)
    gather = Gather(at, u_ref, ubuf, ag_send, ag_recv)
    scatter = Scatter(at, tbuf, rbuf, rs_send, rs_recv)
    gather.start(0, 2)
    ubuf[at["me"]] = u_ref[...]
    for item in weights:
        item.wait()

    def body(pos, carry):
        gather.before(pos, ORDER_RS)
        blk = pick(pos, ORDER_RS, at)

        @pl.when(pos >= 2)
        def _():
            store(pos - 2).wait()

        @pl.when(pos < N - 2)
        def _():
            load(pos + 2).start()

        out = lax.dot_general(ubuf[blk], w_qkv[...], (((1,), (1,)), ((), ())), preferred_element_type=F32)
        start = start_ref[pl.ds(pl.multiple_of(blk * SEQS, SEQS), SEQS), :]
        lane = lax.broadcasted_iota(jnp.int32, (SEQS, 128), 1)
        hot = jnp.concatenate([jnp.where(lane == start + s, 1.0, 0.0) for s in range(STEPS)], axis=0)
        turn = jnp.dot(hot, table_ref[...], precision=lax.Precision.HIGHEST, preferred_element_type=F32)
        cos = turn[:, 0:128]
        sin = turn[:, 128:256]
        low = lax.rem(lax.broadcasted_iota(jnp.int32, (ROWS, 128), 1), HEAD) < HEAD // 2
        for half in range(2):
            part = out[:, half * 128:(half + 1) * 128]
            swapped = jnp.where(low, pltpu.roll(part, 128 - HEAD // 2, 1), pltpu.roll(part, HEAD // 2, 1))
            qk[:, half * 128:(half + 1) * 128] = (part * cos + swapped * sin).astype(BF16).astype(F32)
        vv[...] = out[:, 256:384].astype(BF16).astype(F32)
        load(pos).wait()

        def half_block(i, carry):
            attend_half(i * HALF, start_ref, blk * SEQS, qk, vv, planes.at[lax.rem(pos, SLOTS)], mixed)
            return carry

        lax.fori_loop(0, SEQS // HALF, half_block, 0)
        store(pos).start()
        acc[...] = jnp.dot(mixed[...].astype(BF16), w_out[...], preferred_element_type=F32)
        scatter.after(pos, acc)
        return carry

    lax.fori_loop(0, N, body, 0)
    store(jnp.int32(N - 2)).wait()
    store(jnp.int32(N - 1)).wait()
    gather.finish()
    residual.wait()
    scatter.finish(acc, hidden_in, gains_ref[2 * layer + 1:2 * layer + 2, :], hidden_ref, normed_ref)


def attention(layer, u, table, start_wide, hidden, gains, weights, cache, new_cache, ident):
    args = [u, table, start_wide, gains, hidden, *weights, cache]
    in_specs = [VM] * 4 + [ANY] * 6
    aliases = {}
    if new_cache is not None:
        args.append(new_cache)
        in_specs.append(ANY)
        aliases = {10: 2}
    return pl.pallas_call(
        functools.partial(attn_kernel, layer),
        out_shape=RESIDUAL + (jax.ShapeDtypeStruct(cache.shape, BF16),),
        in_specs=in_specs, out_specs=(VM, VM, ANY),
        scratch_shapes=gather_scratch() + scatter_scratch() + [
            pltpu.VMEM((ROWS, 256), F32), pltpu.VMEM((ROWS, 128), F32), pltpu.VMEM((ROWS, 256), F32),
            pltpu.VMEM((SLOTS, 2, SEQS, HEAD, CACHE), BF16), pltpu.VMEM((384, D), BF16), pltpu.VMEM((256, D), BF16),
            pltpu.VMEM((ROWS, D), F32), pltpu.SemaphoreType.DMA((SLOTS,)), pltpu.SemaphoreType.DMA((SLOTS,)),
            pltpu.SemaphoreType.DMA((6,))],
        input_output_aliases=aliases,
        compiler_params=comm_params(ident),
    )(*args)


def moe_kernel(layer, u_ref, router_ref, ids_ref, gains_ref, hidden_hbm, gate_hbm, up_hbm, down_hbm, hidden_ref, normed_ref,
               ubuf, ag_send, ag_recv, acc, tbuf, rbuf, rs_send, rs_recv, gate_v, up_v, down_v, hidden, gates, hidden_in, w_sem):
    def load(kind, e):
        src, dst = ((gate_hbm, gate_v), (up_hbm, up_v))[kind]
        return pltpu.make_async_copy(src.at[layer, e], dst.at[e], w_sem.at[kind, e])

    down_load = pltpu.make_async_copy(down_hbm.at[layer], down_v, w_sem.at[2, 0])
    for e in range(LOCAL_EXPERTS):
        load(0, e).start()
        load(1, e).start()
    down_load.start()
    residual = pltpu.make_async_copy(hidden_hbm, hidden_in, w_sem.at[2, 1])
    residual.start()
    at = places()
    entry_barrier(at)
    gather = Gather(at, u_ref, ubuf, ag_send, ag_recv)
    scatter = Scatter(at, tbuf, rbuf, rs_send, rs_recv)
    gather.start(0, 2)
    ubuf[at["me"]] = u_ref[...]
    lane = lax.broadcasted_iota(jnp.int32, (ROWS, EXPERTS), 1)

    def route(blk):
        ids = ids_ref[blk]
        chosen = lane == ids[:, 0:1]
        for j in range(1, 8):
            chosen = chosen | (lane == ids[:, j:j + 1])
        score = lax.dot_general(ubuf[blk], router_ref[layer], (((1,), (1,)), ((), ())), preferred_element_type=F32)
        masked = jnp.where(chosen, score, -jnp.inf)
        weight = jnp.exp(masked - jnp.max(masked, axis=1, keepdims=True))
        gates[...] = weight / jnp.sum(weight, axis=1, keepdims=True)

    def inner(blk, e):
        return (jnp.dot(ubuf[blk], gate_v[e], preferred_element_type=F32),
                jnp.dot(ubuf[blk], up_v[e], preferred_element_type=F32))

    def activate(e, gate_act, up_act):
        share = jnp.sum(jnp.where(lane == at["me"] * LOCAL_EXPERTS + e, gates[...], 0.0), axis=1, keepdims=True)
        half = 0.5 * gate_act
        z = (half * jnp.tanh(half) + half) * up_act * share
        start = e * FF if isinstance(e, int) else pl.multiple_of(e * FF, FF)
        hidden[:, pl.ds(start, FF)] = z.astype(BF16)

    def down(start):
        cols = pl.ds(start, 512)
        acc[:, cols] = jnp.dot(hidden[...], down_v[:, cols], preferred_element_type=F32)

    def first_expert(e, carry):
        load(0, e).wait()
        load(1, e).wait()
        activate(e, *inner(at["sib"], e))
        return carry

    gather.before(jnp.int32(0), ORDER_RS)
    route(at["sib"])
    lax.fori_loop(0, LOCAL_EXPERTS, first_expert, 0)
    down_load.wait()

    def first_down(c, carry):
        down(pl.multiple_of(c * 512, 512))
        return carry

    lax.fori_loop(0, D // 512, first_down, 0)
    scatter.after(jnp.int32(0), acc)

    def body(pos, carry):
        gather.before(pos, ORDER_RS)
        blk = pick(pos, ORDER_RS, at)
        acts = inner(blk, 0)
        route(blk)
        for e in range(LOCAL_EXPERTS):
            following = inner(blk, e + 1) if e + 1 < LOCAL_EXPERTS else None
            activate(e, *acts)
            acts = following
        for c in range(D // 512):
            down(c * 512)
        scatter.after(pos, acc)
        return carry

    lax.fori_loop(1, N, body, 0)
    gather.finish()
    residual.wait()
    scatter.finish(acc, hidden_in, gains_ref[2 * layer + 2:2 * layer + 3, :], hidden_ref, normed_ref)


def experts(layer, u, router, ids, hidden, gains, w_gate, w_up, w_down, ident):
    width = LOCAL_EXPERTS * FF
    return pl.pallas_call(
        functools.partial(moe_kernel, layer),
        out_shape=RESIDUAL,
        in_specs=[VM] * 4 + [ANY] * 4, out_specs=(VM, VM),
        scratch_shapes=gather_scratch() + scatter_scratch() + [
            pltpu.VMEM((LOCAL_EXPERTS, D, FF), BF16), pltpu.VMEM((LOCAL_EXPERTS, D, FF), BF16),
            pltpu.VMEM((width, D), BF16), pltpu.VMEM((ROWS, width), BF16), pltpu.VMEM((ROWS, EXPERTS), F32),
            pltpu.VMEM((ROWS, D), F32),
            pltpu.SemaphoreType.DMA((3, LOCAL_EXPERTS))],
        compiler_params=comm_params(ident),
    )(u, router, ids, gains, hidden, w_gate, w_up, w_down.reshape(LAYERS, width, D))


TILE = 1024
TILES = VOCAB // TILE
LAST_TILE = 384


def fold(logits, column, target, stat):
    part = logits.reshape(TILE // 8, 8, ROWS)
    peak = stat[0]
    top = jnp.maximum(peak, jnp.max(part, axis=0))
    stat[0] = top
    stat[1] = stat[1] * jnp.exp((peak - top) * (1.0 / LOGIT_DIV)) + jnp.sum(
        jnp.exp((part - top) * (1.0 / LOGIT_DIV)), axis=0)
    here = target - column // 8 if isinstance(column, int) else target - lax.div(column, 8)
    picked = stat[2]
    for g in range(TILE // 8):
        picked = jnp.where(here == g, part[g], picked)
    stat[2] = picked


def head_kernel(f_ref, target_ref, embed_ref, probs_ref, last_ref, ubuf, send, recv, table, even, odd, stat, mine, theirs,
                share_send, share_recv, sem):
    def load(c):
        rows = pl.ds(pl.multiple_of(c * TILE, TILE), TILE)
        return pltpu.make_async_copy(embed_ref.at[rows], table.at[rows], sem.at[c])

    for c in range(TILES):
        load(c).start()
    at = places()
    entry_barrier(at, ORDER_AG[1:])
    gather = Gather(at, f_ref, ubuf, send, recv)
    gather.start(0, 2)
    ubuf[at["me"]] = f_ref[...]

    def tile_logits(blk, start):
        return lax.dot_general(table[pl.ds(start, TILE), :], ubuf[blk], (((1,), (1,)), ((), ())), preferred_element_type=F32)

    def group_of(blk):
        local = jnp.broadcast_to(target_ref[blk], (8, ROWS))
        sub = lax.broadcasted_iota(jnp.int32, (8, ROWS), 0)
        return jnp.where((local >= 0) & ((local & 7) == sub), local >> 3, -1 - VOCAB)

    def begin():
        stat[0] = jnp.full((8, ROWS), -1e30, F32)
        stat[1] = jnp.zeros((8, ROWS), F32)
        stat[2] = jnp.zeros((8, ROWS), F32)

    def end(blk):
        peak = stat[0]
        top = jnp.max(peak, axis=0, keepdims=True)
        mine[0, pl.ds(blk, 1), :] = top
        mine[1, pl.ds(blk, 1), :] = jnp.sum(stat[1] * jnp.exp((peak - top) * (1.0 / LOGIT_DIV)), axis=0, keepdims=True)
        mine[2, pl.ds(blk, 1), :] = jnp.sum(stat[2], axis=0, keepdims=True)
        last_ref[blk] = ubuf[blk, ROWS - SEQS:ROWS, :]

    def first_tile(c, carry):
        load(c).wait()
        even[...] = tile_logits(at["me"], pl.multiple_of(c * TILE, TILE))
        fold(even[...], c * TILE, group_of(at["me"]), stat)
        return carry

    begin()
    lax.fori_loop(0, TILES, first_tile, 0)
    end(at["me"])

    def body(pos, carry):
        gather.before(pos, ORDER_AG)
        blk = pick(pos, ORDER_AG, at)
        target = group_of(blk)
        begin()
        bufs = (even, odd)
        even[...] = tile_logits(blk, 0)
        for c in range(1, TILES + 1):
            if c < TILES:
                bufs[c % 2][...] = tile_logits(blk, c * TILE)
            fold(bufs[(c - 1) % 2][...], (c - 1) * TILE, target, stat)
        end(blk)
        return carry

    lax.fori_loop(1, N, body, 0)
    gather.finish()
    me = at["me"]
    copies = [pltpu.make_async_remote_copy(
        src_ref=mine, dst_ref=theirs.at[shift], send_sem=share_send.at[shift], recv_sem=share_recv.at[shift],
        device_id={"tp": lax.rem(me + shift, N)}, device_id_type=MESH) for shift in range(1, N)]
    for item in copies:
        item.start()
    theirs[0] = mine[...]
    for item in copies:
        item.wait()
    peak = functools.reduce(jnp.maximum, [theirs[i, 0] for i in range(N)])
    total = sum(theirs[i, 1] * jnp.exp((theirs[i, 0] - peak) * (1.0 / LOGIT_DIV)) for i in range(N))
    picked = sum(theirs[i, 2] for i in range(N))
    probs_ref[...] = (picked - peak) * (1.0 / LOGIT_DIV) - jnp.log(total)


def head(f, target, embed, ident):
    return pl.pallas_call(
        head_kernel,
        out_shape=(jax.ShapeDtypeStruct((N, ROWS), F32), jax.ShapeDtypeStruct((N, SEQS, D), BF16)),
        in_specs=[VM, VM, ANY], out_specs=(VM, VM),
        scratch_shapes=gather_scratch() + [
            pltpu.VMEM((VOCAB, D), BF16), pltpu.VMEM((TILE, ROWS), F32), pltpu.VMEM((TILE, ROWS), F32),
            pltpu.VMEM((3, 8, ROWS), F32), pltpu.VMEM((3, N, ROWS), F32), pltpu.VMEM((N, 3, N, ROWS), F32),
            pltpu.SemaphoreType.DMA((N,)), pltpu.SemaphoreType.DMA((N,)), pltpu.SemaphoreType.DMA((TILES,))],
        compiler_params=comm_params(ident),
    )(f, target, embed)


LAST_STEPS = VOCAB // LAST_TILE
PLANES = LAYERS * 2 * BATCH // LAST_STEPS
RING = 8
AHEAD = 4


def last_kernel(f_ref, embed_ref, cache_ref, logits_ref, new_ref, ring, in_sem, out_sem):
    c = pl.program_id(0)

    def load(i):
        slot = lax.rem(i, RING)
        return pltpu.make_async_copy(cache_ref.at[pl.ds(i * PLANES, PLANES)], ring.at[slot], in_sem.at[slot])

    def store(i):
        slot = lax.rem(i, RING)
        return pltpu.make_async_copy(ring.at[slot], new_ref.at[pl.ds(i * PLANES, PLANES)], out_sem.at[slot])

    @pl.when(c == 0)
    def _():
        for i in range(AHEAD):
            load(jnp.int32(i)).start()

    @pl.when((c >= RING - AHEAD) & (c < LAST_STEPS - AHEAD))
    def _():
        store(c + AHEAD - RING).wait()

    @pl.when(c < LAST_STEPS - AHEAD)
    def _():
        load(c + AHEAD).start()

    load(c).wait()
    store(c).start()
    logits_ref[...] = lax.dot_general(f_ref[...], embed_ref[...], (((1,), (1,)), ((), ())),
                                      preferred_element_type=F32) * (1.0 / LOGIT_DIV)

    @pl.when(c == LAST_STEPS - 1)
    def _():
        for i in range(LAST_STEPS - RING, LAST_STEPS):
            store(jnp.int32(i)).wait()


def last_step(f, embed, cache):
    flat = cache.reshape(LAYERS * 2 * BATCH, HEAD, CACHE)
    logits, flat = pl.pallas_call(
        last_kernel,
        out_shape=(jax.ShapeDtypeStruct((BATCH, VOCAB), F32), jax.ShapeDtypeStruct(flat.shape, BF16)),
        grid=(LAST_STEPS,),
        in_specs=[pl.BlockSpec((BATCH, D), lambda c: (0, 0)), pl.BlockSpec((LAST_TILE, D), lambda c: (c, 0)), ANY],
        out_specs=(pl.BlockSpec((BATCH, LAST_TILE), lambda c: (0, c)), ANY),
        scratch_shapes=[pltpu.VMEM((RING, PLANES, HEAD, CACHE), BF16), pltpu.SemaphoreType.DMA((RING,)),
                        pltpu.SemaphoreType.DMA((RING,))],
        compiler_params=pltpu.CompilerParams(dimension_semantics=("arbitrary",), vmem_limit_bytes=VMEM_LIMIT),
    )(f, embed, flat)
    return logits, flat.reshape(cache.shape)


def by_block(values):
    return values.reshape(N, SEQS, values.shape[1]).transpose(0, 2, 1)


def solution(mesh):
    cache_spec = P(None, None, 'dp', None, 'tp', None)
    expert_spec = P(None, 'tp', None, None)
    in_specs = (P('dp', None), P('dp'), cache_spec, P(None, None, 'dp', None), P('tp', None), P(None, None), P(None, None, 'tp'), P(None, None, 'tp'), P(None, None, 'tp'), P(None, 'tp', None), P(None, None, None), expert_spec, expert_spec, expert_spec)
    out_specs = (P('dp', None), P('dp', 'tp'), cache_spec)

    def decode_local(tokens, start_pos, kv_cache, expert_ids, embed, norm_gain, w_query, w_key, w_value, w_out, w_router, w_gate, w_up, w_down):
        shard = lax.axis_index('tp')
        cache = kv_cache.transpose(0, 1, 2, 4, 5, 3).reshape(LAYERS, 2, BATCH, HEAD, CACHE)

        ids = by_block(tokens[:, :STEPS]).reshape(N, ROWS)
        hidden, normed = embed_tokens(ids, shard, embed, norm_gain)

        inv_freq = ROPE_THETA ** (-2.0 * jnp.arange(HEAD // 2, dtype=F32) / HEAD)
        angles = jnp.arange(CACHE, dtype=F32)[:, None] * jnp.tile(inv_freq, 4)
        sign = jnp.where(jnp.arange(128) % HEAD < HEAD // 2, -1.0, 1.0)
        table = jnp.concatenate([jnp.cos(angles), jnp.sin(angles) * sign], axis=1)
        start_wide = jnp.broadcast_to(start_pos[:, None], (BATCH, 128))

        weights = [w.transpose(0, 2, 1) for w in (w_query, w_key, w_value)] + [w_out]
        router = w_router.transpose(0, 2, 1)
        routed = expert_ids.reshape(STEPS, LAYERS, N, SEQS, 8).transpose(1, 2, 0, 3, 4).reshape(LAYERS, N, ROWS, 8)

        new_cache = None
        for layer in range(LAYERS):
            hidden, normed, new_cache = attention(layer, normed, table, start_wide, hidden, norm_gain, weights, cache, new_cache,
                                                  1 + 2 * layer)
            hidden, normed = experts(layer, normed, router, routed[layer], hidden, norm_gain, w_gate, w_up, w_down, 2 + 2 * layer)

        target = by_block(tokens[:, 1:] - shard * VOCAB).reshape(N, 1, ROWS)
        log_probs, f_last = head(normed, target, embed, 5)
        logits, new_cache = last_step(f_last.reshape(BATCH, D), embed, new_cache)
        log_probs = log_probs.reshape(N, STEPS, SEQS).transpose(0, 2, 1).reshape(BATCH, STEPS)
        new_cache = new_cache.reshape(LAYERS, 2, BATCH, 1, HEAD, CACHE).transpose(0, 1, 2, 5, 3, 4)
        return log_probs, logits, new_cache

    return jax.shard_map(decode_local, mesh=mesh, in_specs=in_specs, out_specs=out_specs, check_vma=False)
```

```python
import functools

import jax
import jax.numpy as jnp
from jax import lax
from jax.experimental import pallas as pl
from jax.experimental.pallas import tpu as pltpu
from jax.sharding import PartitionSpec as P

EMBED_MULT = 12.0
ATT_SCALE = 0.015625
RESID_MULT = 0.22
LOGIT_DIV = 6.0
NORM_EPS = 1e-6
ROPE_THETA = 10000.0

D = 1536
HEAD = 64
BATCH = 512
STEPS = 4
LAYERS = 2
CACHE = 128
EXPERTS = 40
LOCAL_EXPERTS = 5
FF = 512
VOCAB = 6144
N = 8
SEQS = BATCH // N
ROWS = SEQS * STEPS
MESH = pl.DeviceIdType.MESH
F32 = jnp.float32
BF16 = jnp.bfloat16
VMEM_LIMIT = 60 * 1024 * 1024

ORDER_RS = ("sib", "bs", "a", "ds", "dg", "as", "b", "me")
ORDER_AG = ("me", "sib", "bs", "a", "ds", "dg", "as", "b")
ORDER_EMBED = ("sib", "ds", "dg", "bs", "a", "as", "b", "me")


def places():
    me = lax.axis_index("tp")
    k = lax.rem(me, 2)
    x = lax.rem(lax.div(me, 2), 2)
    y = lax.div(me, 4)
    step_x = 2 - 4 * x
    step_y = 4 - 8 * y
    a = me + step_x + k * (step_y - step_x)
    b = me + step_y + k * (step_x - step_y)
    dg = me + step_x + step_y
    s = 1 - 2 * k
    return {"me": me, "sib": me + s, "a": a, "as": a + s, "b": b, "bs": b + s, "dg": dg, "ds": dg + s}


def entry_barrier(at, names=("sib", "a", "b")):
    barrier = pltpu.get_barrier_semaphore()
    for name in names:
        pl.semaphore_signal(barrier, inc=1, device_id={"tp": at[name]}, device_id_type=MESH)
    pl.semaphore_wait(barrier, len(names))


def pick(pos, order, at):
    total = jnp.int32(0)
    for i, name in enumerate(order):
        total = total + jnp.where(pos == i, at[name], 0)
    return total


class Gather:
    def __init__(self, at, own, ubuf, send, recv):
        self.at, self.own, self.ubuf, self.send, self.recv = at, own, ubuf, send, recv

    def copy(self, src, origin, target, slot):
        return pltpu.make_async_remote_copy(
            src_ref=src, dst_ref=self.ubuf.at[origin], send_sem=self.send.at[slot], recv_sem=self.recv.at[origin],
            device_id={"tp": target}, device_id_type=MESH)

    def item(self, slot):
        at = self.at
        if slot < 3:
            return self.copy(self.own, at["me"], at[("a", "b", "sib")[slot]], slot)
        name, target = (("a", "b"), ("a", "sib"), ("b", "sib"), ("dg", "sib"))[slot - 3]
        return self.copy(self.ubuf.at[at[name]], at[name], at[target], slot)

    def start(self, *slots):
        for slot in slots:
            self.item(slot).start()

    def arrive(self, name):
        origin = self.at[name]
        self.copy(self.own, origin, self.at["sib"], 0).wait_recv()

    def before(self, pos, order):
        @pl.when(pos == order.index("sib"))
        def _():
            self.arrive("sib")

        @pl.when(pos == order.index("bs"))
        def _():
            self.arrive("a")
            self.start(3, 4, 1)
            self.arrive("bs")

        @pl.when(pos == order.index("ds"))
        def _():
            self.arrive("dg")
            self.start(6)
            self.arrive("ds")

        @pl.when(pos == order.index("as"))
        def _():
            self.arrive("b")
            self.start(5)
            self.arrive("as")

    def finish(self):
        for slot in range(7):
            self.item(slot).wait_send()


class Scatter:
    def __init__(self, at, tbuf, rbuf, send, recv):
        self.at, self.tbuf, self.rbuf, self.send, self.recv = at, tbuf, rbuf, send, recv

    def copy(self, slot, target):
        return pltpu.make_async_remote_copy(
            src_ref=self.tbuf.at[slot], dst_ref=self.rbuf.at[slot], send_sem=self.send.at[slot],
            recv_sem=self.recv.at[slot], device_id={"tp": target}, device_id_type=MESH)

    def arrive(self, slot):
        self.copy(slot, self.at["sib"]).wait_recv()

    def after(self, pos, acc, far_first=False):
        at = self.at

        @pl.when((pos == 0) | (pos == 1) | (pos == 3) | (pos == 5))
        def _():
            slot = lax.div(pos + 1, 2)
            self.tbuf[slot] = acc[...].astype(BF16)
            self.copy(slot, at["sib"]).start()

        @pl.when((pos == 2) | (pos == 4))
        def _():
            slot = lax.div(pos, 2)
            out = 6 - slot if far_first else slot + 3
            self.arrive(slot)
            self.tbuf[out] = (acc[...] + self.rbuf[slot].astype(F32)).astype(BF16)
            self.copy(out, at["a"]).start()

        @pl.when(pos == 6)
        def _():
            self.arrive(3)
            self.arrive(5)
            self.tbuf[6] = (acc[...] + self.rbuf[3].astype(F32) + self.rbuf[5].astype(F32)).astype(BF16)
            self.copy(6, at["b"]).start()

    def finish(self, acc, hidden_in, gain, hidden_ref, normed_ref):
        self.arrive(0)
        self.arrive(4)
        self.arrive(6)

        def chunk(c, carry):
            rows = pl.ds(pl.multiple_of(c * 32, 32), 32)
            total = acc[rows, :]
            for slot in (0, 4, 6):
                total = total + self.rbuf[slot, rows, :].astype(F32)
            total = total.astype(BF16).astype(F32)
            if hidden_in is None:
                hidden = EMBED_MULT * total
            else:
                hidden = hidden_in[rows, :] + RESID_MULT * total
            hidden_ref[rows, :] = hidden
            mean_sq = jnp.mean(hidden * hidden, axis=1, keepdims=True)
            normed_ref[rows, :] = (hidden * lax.rsqrt(mean_sq + NORM_EPS) * gain).astype(BF16)
            return carry

        lax.fori_loop(0, ROWS // 32, chunk, 0)
        for slot in range(7):
            self.copy(slot, self.at["sib"]).wait_send()


def gather_scratch():
    return [pltpu.VMEM((N, ROWS, D), BF16), pltpu.SemaphoreType.DMA((7,)), pltpu.SemaphoreType.DMA((N,))]


def scatter_scratch():
    return [pltpu.VMEM((ROWS, D), F32), pltpu.VMEM((7, ROWS, D), BF16),
            pltpu.VMEM((7, ROWS, D), BF16), pltpu.SemaphoreType.DMA((7,)), pltpu.SemaphoreType.DMA((7,))]


VM = pl.BlockSpec(memory_space=pltpu.VMEM)
RESIDUAL = (jax.ShapeDtypeStruct((ROWS, D), F32), jax.ShapeDtypeStruct((ROWS, D), BF16))
ANY = pl.BlockSpec(memory_space=pl.ANY)


def comm_params(ident):
    return pltpu.CompilerParams(collective_id=ident, has_side_effects=True, vmem_limit_bytes=VMEM_LIMIT)


CAP = 64


def pack_kernel(count_ref, group_ref, place_ref, embed_ref, out_ref, buf, sem):
    def copy(group, d, j):
        return pltpu.make_async_copy(embed_ref.at[group], buf.at[d, j], sem.at[d])

    def issue(d, carry):
        def eight(i, carry):
            for j in range(8):
                copy(group_ref[d * CAP + 8 * i + j], d, 8 * i + j).start()
            return carry

        lax.fori_loop(0, count_ref[d], eight, 0)
        return carry

    def place(d, carry):
        def eight(i, carry):
            pltpu.make_async_copy(embed_ref.at[0:8], buf.at[d, pl.ds(8 * i, 8)], sem.at[d]).wait()
            return carry

        def blank(i, carry):
            buf[d, pl.ds(8 * i, 8)] = jnp.zeros((8, 8, D), BF16)
            return carry

        lax.fori_loop(count_ref[d], CAP // 8, blank, 0)
        lax.fori_loop(0, count_ref[d], eight, 0)
        lane = lax.broadcasted_iota(jnp.int32, (CAP, 8 * CAP), 1)
        one_hot = jnp.where(lane == place_ref[d], 1.0, 0.0).astype(BF16)
        out_ref[d] = jnp.dot(one_hot, buf[d].reshape(8 * CAP, D), preferred_element_type=F32).astype(BF16)
        return carry

    lax.fori_loop(0, N, issue, 0)
    lax.fori_loop(0, N, place, 0)


def pack_rows(count, owned, embed):
    group = lax.div(owned, 8).reshape(-1)
    place = (8 * jnp.arange(CAP) + lax.rem(owned, 8)).reshape(N, CAP, 1)
    return pl.pallas_call(
        pack_kernel,
        out_shape=jax.ShapeDtypeStruct((N, CAP, D), BF16),
        grid_spec=pltpu.PrefetchScalarGridSpec(
            num_scalar_prefetch=2, grid=(1,),
            in_specs=[pl.BlockSpec((N, CAP, 1), lambda i, *_: (0, 0, 0)), ANY],
            out_specs=pl.BlockSpec((N, CAP, D), lambda i, *_: (0, 0, 0)),
            scratch_shapes=[pltpu.VMEM((N, CAP, 8, D), BF16), pltpu.SemaphoreType.DMA((N,))]),
        compiler_params=pltpu.CompilerParams(vmem_limit_bytes=VMEM_LIMIT),
    )(count, group, place, embed.reshape(VOCAB // 8, 8, D))


def exchange_kernel(packed_ref, slot_ref, gains_ref, hidden_ref, normed_ref, held, send, recv):
    me = lax.axis_index("tp")
    barrier = pltpu.get_barrier_semaphore()
    for shift in range(1, N):
        pl.semaphore_signal(barrier, inc=1, device_id={"tp": lax.rem(me + shift, N)}, device_id_type=MESH)
    pl.semaphore_wait(barrier, N - 1)

    def copy(target, origin, shift):
        return pltpu.make_async_remote_copy(
            src_ref=packed_ref.at[target], dst_ref=held.at[origin], send_sem=send.at[shift], recv_sem=recv.at[shift],
            device_id={"tp": target}, device_id_type=MESH)

    for shift in range(1, N):
        copy(lax.rem(me + shift, N), me, shift).start()
    held[me] = packed_ref[me]
    for shift in range(1, N):
        copy(lax.rem(me + shift, N), lax.rem(me + N - shift, N), shift).wait()

    def chunk(c, carry):
        rows = pl.ds(pl.multiple_of(c * 64, 64), 64)
        lane = lax.broadcasted_iota(jnp.int32, (64, N * CAP), 1)
        one_hot = jnp.where(lane == slot_ref[rows, :], 1.0, 0.0).astype(BF16)
        hidden = EMBED_MULT * jnp.dot(one_hot, held[...].reshape(N * CAP, D), preferred_element_type=F32)
        hidden_ref[rows, :] = hidden
        mean_sq = jnp.mean(hidden * hidden, axis=1, keepdims=True)
        normed_ref[rows, :] = (hidden * lax.rsqrt(mean_sq + NORM_EPS) * gains_ref[0:1, :]).astype(BF16)
        return carry

    lax.fori_loop(0, ROWS // 64, chunk, 0)


def exchange_rows(packed, slot, gains, ident):
    return pl.pallas_call(
        exchange_kernel,
        out_shape=RESIDUAL,
        in_specs=[VM] * 3, out_specs=(VM, VM),
        scratch_shapes=[pltpu.VMEM((N, CAP, D), BF16), pltpu.SemaphoreType.DMA((N,)), pltpu.SemaphoreType.DMA((N,))],
        compiler_params=comm_params(ident),
    )(packed, slot, gains)


def embed_tokens(ids, shard, embed, gains):
    owner = lax.div(ids, VOCAB)
    earlier = jnp.arange(ROWS)[:, None] > jnp.arange(ROWS)[None, :]
    rank = jnp.sum(((owner[:, :, None] == owner[:, None, :]) & earlier).astype(jnp.int32), axis=2)
    local = ids - shard * VOCAB

    def packed(gains):
        mine = jnp.where(owner == shard, rank, -1)
        hit = mine[:, None, :] == jnp.arange(CAP)[None, :, None]
        owned = jnp.sum(jnp.where(hit, local[:, None, :], 0), axis=2)
        slot = lax.dynamic_index_in_dim(owner * CAP + rank, shard, 0, keepdims=False)
        count = lax.div(jnp.max(mine, axis=1) + 8, 8)
        return exchange_rows(pack_rows(count, owned, embed), slot[:, None], gains, 0)

    def general(gains):
        flat = local.reshape(-1)
        inside = (flat >= 0) & (flat < VOCAB)
        rows = jnp.take(embed, jnp.clip(flat, 0, VOCAB - 1), axis=0)
        return embed_sum(jnp.where(inside[:, None], rows, jnp.zeros_like(rows)), gains, 6)

    return lax.cond(jnp.max(rank) < CAP, packed, general, gains)


def embed_kernel(rows_ref, gains_ref, hidden_ref, normed_ref, acc, tbuf, rbuf, send, recv):
    at = places()
    entry_barrier(at)
    scatter = Scatter(at, tbuf, rbuf, send, recv)

    def body(pos, carry):
        acc[...] = rows_ref[pick(pos, ORDER_EMBED, at)].astype(F32)
        scatter.after(pos, acc, far_first=True)
        return carry

    lax.fori_loop(0, N, body, 0)
    scatter.finish(acc, None, gains_ref[0:1, :], hidden_ref, normed_ref)


def embed_sum(rows, gains, ident):
    return pl.pallas_call(
        embed_kernel,
        out_shape=RESIDUAL,
        in_specs=[VM, VM], out_specs=(VM, VM),
        scratch_shapes=scatter_scratch(),
        compiler_params=comm_params(ident),
    )(rows.reshape(N, ROWS, D), gains)


HALF = 32
SLOTS = 4


def attend_half(base, start_ref, first_seq, qk, vv, planes, mixed_out):
    lane = lax.broadcasted_iota(jnp.int32, (8, 128), 1)
    row = lax.broadcasted_iota(jnp.int32, (8, 128), 0)
    first = lane < HEAD
    own = [(2 * j + lax.div(lane, HEAD)) == row for j in range(4)]
    groups = range(HALF // 8)

    def spread(twice):
        return jnp.concatenate([jnp.where(own[j], twice, 0.0) for j in range(4)], axis=1)

    starts = [start_ref[pl.ds(pl.multiple_of(first_seq + base + 8 * g, 8), 8), :] for g in groups]
    query, updates = [], []
    for g in groups:
        queries, keys, vals, hot = [], [], [], []
        for s in range(STEPS):
            span = pl.ds(pl.multiple_of(s * SEQS + base + 8 * g, 8), 8)
            left, right = qk[span, 0:128], qk[span, 128:256]
            left_r, right_r = pltpu.roll(left, HEAD, 1), pltpu.roll(right, HEAD, 1)
            queries += [spread(jnp.where(first, left, left_r)), spread(jnp.where(first, left_r, left)),
                        spread(jnp.where(first, right, right_r))]
            keys.append(spread(jnp.where(first, right_r, right)))
            vals.append(spread(vv[span, :]))
            hot.append(jnp.where(lane == starts[g] + s, 1.0, 0.0))
        query.append(jnp.concatenate(queries, axis=0).astype(BF16))
        hot_all = jnp.concatenate(hot, axis=0).astype(BF16)
        updates.append([
            lax.dot_general(jnp.concatenate(entry, axis=0).astype(BF16), hot_all, (((0,), (0,)), ((), ())),
                            preferred_element_type=F32) for entry in (keys, vals)])
    for g in groups:
        span = pl.ds(base + 8 * g, 8)
        fresh = jnp.where((lane >= starts[g]) & (lane < starts[g] + STEPS), 1.0, 0.0)
        fresh = jnp.broadcast_to(fresh[:, None, :], (8, HEAD, 128)) > 0.5
        for kind in range(2):
            old = planes[kind, span].astype(F32)
            planes[kind, span] = jnp.where(fresh, updates[g][kind].reshape(8, HEAD, 128), old).astype(BF16)
    scores = [jnp.dot(query[g], planes[0, pl.ds(base + 8 * g, 8)].reshape(8 * HEAD, 128), preferred_element_type=F32)
              for g in groups]
    probs = []
    for g in groups:
        valid = [jnp.where(lane <= starts[g] + s, 0.0, -jnp.inf) for s in range(STEPS)]
        score = scores[g] * ATT_SCALE + jnp.concatenate([valid[s] for s in range(STEPS) for h in range(3)], axis=0)
        weight = jnp.exp(score - jnp.max(score, axis=1, keepdims=True))
        probs.append((weight / jnp.sum(weight, axis=1, keepdims=True)).astype(BF16))
    mixed = [lax.dot_general(probs[g], planes[1, pl.ds(base + 8 * g, 8)].reshape(8 * HEAD, 128),
                             (((1,), (1,)), ((), ())), preferred_element_type=F32) for g in groups]
    for g in groups:
        for s in range(STEPS):
            span = pl.ds(pl.multiple_of(s * SEQS + base + 8 * g, 8), 8)
            heads = []
            for h in range(3):
                part = mixed[g][8 * (3 * s + h):8 * (3 * s + h) + 8, :]
                total = sum(jnp.where(own[j], part[:, 128 * j:128 * j + 128], 0.0) for j in range(4))
                heads.append(total + pltpu.roll(total, HEAD, 1))
            mixed_out[span, 0:128] = jnp.where(first, heads[0], heads[1])
            mixed_out[span, 128:256] = heads[2]


def attn_kernel(layer, u_ref, table_ref, start_ref, gains_ref, hidden_hbm, wq_ref, wk_ref, wv_ref, wo_ref, cache_ref,
                *rest):
    if layer > 0:
        rest = rest[1:]
    (hidden_ref, normed_ref, new_ref, ubuf, ag_send, ag_recv, acc, tbuf, rbuf, rs_send, rs_recv,
     qk, vv, mixed, planes, w_qkv, w_out, hidden_in, in_sem, out_sem, w_sem) = rest
    at = places()
    weights = [
        pltpu.make_async_copy(wq_ref.at[layer], w_qkv.at[0:192], w_sem.at[0]),
        pltpu.make_async_copy(wk_ref.at[layer], w_qkv.at[192:256], w_sem.at[1]),
        pltpu.make_async_copy(wv_ref.at[layer], w_qkv.at[256:320], w_sem.at[2]),
        pltpu.make_async_copy(wv_ref.at[layer], w_qkv.at[320:384], w_sem.at[3]),
        pltpu.make_async_copy(wo_ref.at[layer], w_out.at[0:192], w_sem.at[4])]
    for item in weights:
        item.start()
    residual = pltpu.make_async_copy(hidden_hbm, hidden_in, w_sem.at[5])
    residual.start()
    w_out[192:256, :] = jnp.zeros((64, D), BF16)

    def plane_span(pos):
        return pl.ds(pick(pos, ORDER_RS, at) * SEQS, SEQS)

    def load(pos):
        slot = lax.rem(pos, SLOTS)
        return pltpu.make_async_copy(cache_ref.at[layer, :, plane_span(pos)], planes.at[slot], in_sem.at[slot])

    def store(pos):
        slot = lax.rem(pos, SLOTS)
        return pltpu.make_async_copy(planes.at[slot], new_ref.at[layer, :, plane_span(pos)], out_sem.at[slot])

    load(jnp.int32(0)).start()
    load(jnp.int32(1)).start()
    entry_barrier(at)
    gather = Gather(at, u_ref, ubuf, ag_send, ag_recv)
    scatter = Scatter(at, tbuf, rbuf, rs_send, rs_recv)
    gather.start(0, 2)
    ubuf[at["me"]] = u_ref[...]
    for item in weights:
        item.wait()

    def body(pos, carry):
        gather.before(pos, ORDER_RS)
        blk = pick(pos, ORDER_RS, at)

        @pl.when(pos >= 2)
        def _():
            store(pos - 2).wait()

        @pl.when(pos < N - 2)
        def _():
            load(pos + 2).start()

        out = lax.dot_general(ubuf[blk], w_qkv[...], (((1,), (1,)), ((), ())), preferred_element_type=F32)
        start = start_ref[pl.ds(pl.multiple_of(blk * SEQS, SEQS), SEQS), :]
        lane = lax.broadcasted_iota(jnp.int32, (SEQS, 128), 1)
        hot = jnp.concatenate([jnp.where(lane == start + s, 1.0, 0.0) for s in range(STEPS)], axis=0)
        turn = jnp.dot(hot, table_ref[...], precision=lax.Precision.HIGHEST, preferred_element_type=F32)
        cos = turn[:, 0:128]
        sin = turn[:, 128:256]
        low = lax.rem(lax.broadcasted_iota(jnp.int32, (ROWS, 128), 1), HEAD) < HEAD // 2
        for half in range(2):
            part = out[:, half * 128:(half + 1) * 128]
            swapped = jnp.where(low, pltpu.roll(part, 128 - HEAD // 2, 1), pltpu.roll(part, HEAD // 2, 1))
            qk[:, half * 128:(half + 1) * 128] = (part * cos + swapped * sin).astype(BF16).astype(F32)
        vv[...] = out[:, 256:384].astype(BF16).astype(F32)
        load(pos).wait()

        def half_block(i, carry):
            attend_half(i * HALF, start_ref, blk * SEQS, qk, vv, planes.at[lax.rem(pos, SLOTS)], mixed)
            return carry

        lax.fori_loop(0, SEQS // HALF, half_block, 0)
        store(pos).start()
        acc[...] = jnp.dot(mixed[...].astype(BF16), w_out[...], preferred_element_type=F32)
        scatter.after(pos, acc)
        return carry

    lax.fori_loop(0, N, body, 0)
    store(jnp.int32(N - 2)).wait()
    store(jnp.int32(N - 1)).wait()
    gather.finish()
    residual.wait()
    scatter.finish(acc, hidden_in, gains_ref[2 * layer + 1:2 * layer + 2, :], hidden_ref, normed_ref)


def attention(layer, u, table, start_wide, hidden, gains, weights, cache, new_cache, ident):
    args = [u, table, start_wide, gains, hidden, *weights, cache]
    in_specs = [VM] * 4 + [ANY] * 6
    aliases = {}
    if new_cache is not None:
        args.append(new_cache)
        in_specs.append(ANY)
        aliases = {10: 2}
    return pl.pallas_call(
        functools.partial(attn_kernel, layer),
        out_shape=RESIDUAL + (jax.ShapeDtypeStruct(cache.shape, BF16),),
        in_specs=in_specs, out_specs=(VM, VM, ANY),
        scratch_shapes=gather_scratch() + scatter_scratch() + [
            pltpu.VMEM((ROWS, 256), F32), pltpu.VMEM((ROWS, 128), F32), pltpu.VMEM((ROWS, 256), F32),
            pltpu.VMEM((SLOTS, 2, SEQS, HEAD, CACHE), BF16), pltpu.VMEM((384, D), BF16), pltpu.VMEM((256, D), BF16),
            pltpu.VMEM((ROWS, D), F32), pltpu.SemaphoreType.DMA((SLOTS,)), pltpu.SemaphoreType.DMA((SLOTS,)),
            pltpu.SemaphoreType.DMA((6,))],
        input_output_aliases=aliases,
        compiler_params=comm_params(ident),
    )(*args)


def moe_kernel(layer, u_ref, router_ref, ids_ref, gains_ref, hidden_hbm, gate_hbm, up_hbm, down_hbm, hidden_ref, normed_ref,
               ubuf, ag_send, ag_recv, acc, tbuf, rbuf, rs_send, rs_recv, gate_v, up_v, down_v, hidden, gates, hidden_in, w_sem):
    def load(kind, e):
        src, dst = ((gate_hbm, gate_v), (up_hbm, up_v))[kind]
        return pltpu.make_async_copy(src.at[layer, e], dst.at[e], w_sem.at[kind, e])

    down_load = pltpu.make_async_copy(down_hbm.at[layer], down_v, w_sem.at[2, 0])
    for e in range(LOCAL_EXPERTS):
        load(0, e).start()
        load(1, e).start()
    down_load.start()
    residual = pltpu.make_async_copy(hidden_hbm, hidden_in, w_sem.at[2, 1])
    residual.start()
    at = places()
    entry_barrier(at)
    gather = Gather(at, u_ref, ubuf, ag_send, ag_recv)
    scatter = Scatter(at, tbuf, rbuf, rs_send, rs_recv)
    gather.start(0, 2)
    ubuf[at["me"]] = u_ref[...]
    lane = lax.broadcasted_iota(jnp.int32, (ROWS, EXPERTS), 1)

    def route(blk):
        ids = ids_ref[blk]
        chosen = lane == ids[:, 0:1]
        for j in range(1, 8):
            chosen = chosen | (lane == ids[:, j:j + 1])
        score = lax.dot_general(ubuf[blk], router_ref[layer], (((1,), (1,)), ((), ())), preferred_element_type=F32)
        masked = jnp.where(chosen, score, -jnp.inf)
        weight = jnp.exp(masked - jnp.max(masked, axis=1, keepdims=True))
        gates[...] = weight / jnp.sum(weight, axis=1, keepdims=True)

    def inner(blk, e):
        return (jnp.dot(ubuf[blk], gate_v[e], preferred_element_type=F32),
                jnp.dot(ubuf[blk], up_v[e], preferred_element_type=F32))

    def activate(e, gate_act, up_act):
        share = jnp.sum(jnp.where(lane == at["me"] * LOCAL_EXPERTS + e, gates[...], 0.0), axis=1, keepdims=True)
        z = gate_act * jax.nn.sigmoid(gate_act) * up_act * share
        start = e * FF if isinstance(e, int) else pl.multiple_of(e * FF, FF)
        hidden[:, pl.ds(start, FF)] = z.astype(BF16)

    def down(start):
        cols = pl.ds(start, 512)
        acc[:, cols] = jnp.dot(hidden[...], down_v[:, cols], preferred_element_type=F32)

    def first_expert(e, carry):
        load(0, e).wait()
        load(1, e).wait()
        activate(e, *inner(at["sib"], e))
        return carry

    gather.before(jnp.int32(0), ORDER_RS)
    route(at["sib"])
    lax.fori_loop(0, LOCAL_EXPERTS, first_expert, 0)
    down_load.wait()

    def first_down(c, carry):
        down(pl.multiple_of(c * 512, 512))
        return carry

    lax.fori_loop(0, D // 512, first_down, 0)
    scatter.after(jnp.int32(0), acc)

    def body(pos, carry):
        gather.before(pos, ORDER_RS)
        blk = pick(pos, ORDER_RS, at)
        acts = inner(blk, 0)
        route(blk)
        for e in range(LOCAL_EXPERTS):
            following = inner(blk, e + 1) if e + 1 < LOCAL_EXPERTS else None
            activate(e, *acts)
            acts = following
        for c in range(D // 512):
            down(c * 512)
        scatter.after(pos, acc)
        return carry

    lax.fori_loop(1, N, body, 0)
    gather.finish()
    residual.wait()
    scatter.finish(acc, hidden_in, gains_ref[2 * layer + 2:2 * layer + 3, :], hidden_ref, normed_ref)


def experts(layer, u, router, ids, hidden, gains, w_gate, w_up, w_down, ident):
    width = LOCAL_EXPERTS * FF
    return pl.pallas_call(
        functools.partial(moe_kernel, layer),
        out_shape=RESIDUAL,
        in_specs=[VM] * 4 + [ANY] * 4, out_specs=(VM, VM),
        scratch_shapes=gather_scratch() + scatter_scratch() + [
            pltpu.VMEM((LOCAL_EXPERTS, D, FF), BF16), pltpu.VMEM((LOCAL_EXPERTS, D, FF), BF16),
            pltpu.VMEM((width, D), BF16), pltpu.VMEM((ROWS, width), BF16), pltpu.VMEM((ROWS, EXPERTS), F32),
            pltpu.VMEM((ROWS, D), F32),
            pltpu.SemaphoreType.DMA((3, LOCAL_EXPERTS))],
        compiler_params=comm_params(ident),
    )(u, router, ids, gains, hidden, w_gate, w_up, w_down.reshape(LAYERS, width, D))


TILE = 1024
TILES = VOCAB // TILE
LAST_TILE = 384


def fold(logits, column, target, stat):
    part = logits.reshape(TILE // 8, 8, ROWS)
    peak = stat[0]
    top = jnp.maximum(peak, jnp.max(part, axis=0))
    stat[0] = top
    stat[1] = stat[1] * jnp.exp((peak - top) * (1.0 / LOGIT_DIV)) + jnp.sum(
        jnp.exp((part - top) * (1.0 / LOGIT_DIV)), axis=0)
    here = target - column // 8 if isinstance(column, int) else target - lax.div(column, 8)
    picked = stat[2]
    for g in range(TILE // 8):
        picked = jnp.where(here == g, part[g], picked)
    stat[2] = picked


def head_kernel(f_ref, target_ref, embed_ref, probs_ref, last_ref, ubuf, send, recv, table, tile_ref, stat, mine, theirs,
                share_send, share_recv, sem):
    def load(c):
        rows = pl.ds(pl.multiple_of(c * TILE, TILE), TILE)
        return pltpu.make_async_copy(embed_ref.at[rows], table.at[rows], sem.at[c])

    for c in range(TILES):
        load(c).start()
    at = places()
    entry_barrier(at, ORDER_AG[1:])
    gather = Gather(at, f_ref, ubuf, send, recv)
    gather.start(0, 2)
    ubuf[at["me"]] = f_ref[...]

    def tile_logits(blk, start):
        return lax.dot_general(table[pl.ds(start, TILE), :], ubuf[blk], (((1,), (1,)), ((), ())), preferred_element_type=F32)

    def group_of(blk):
        local = jnp.broadcast_to(target_ref[blk], (8, ROWS))
        sub = lax.broadcasted_iota(jnp.int32, (8, ROWS), 0)
        return jnp.where((local >= 0) & ((local & 7) == sub), local >> 3, -1 - VOCAB)

    def begin():
        stat[0] = jnp.full((8, ROWS), -1e30, F32)
        stat[1] = jnp.zeros((8, ROWS), F32)
        stat[2] = jnp.zeros((8, ROWS), F32)

    def end(blk):
        peak = stat[0]
        top = jnp.max(peak, axis=0, keepdims=True)
        mine[0, pl.ds(blk, 1), :] = top
        mine[1, pl.ds(blk, 1), :] = jnp.sum(stat[1] * jnp.exp((peak - top) * (1.0 / LOGIT_DIV)), axis=0, keepdims=True)
        mine[2, pl.ds(blk, 1), :] = jnp.sum(stat[2], axis=0, keepdims=True)
        last_ref[blk] = ubuf[blk, ROWS - SEQS:ROWS, :]

    def first_tile(c, carry):
        load(c).wait()
        tile_ref[...] = tile_logits(at["me"], pl.multiple_of(c * TILE, TILE))
        fold(tile_ref[...], c * TILE, group_of(at["me"]), stat)
        return carry

    begin()
    lax.fori_loop(0, TILES, first_tile, 0)
    end(at["me"])

    def body(pos, carry):
        gather.before(pos, ORDER_AG)
        blk = pick(pos, ORDER_AG, at)
        target = group_of(blk)
        begin()
        tile = tile_logits(blk, 0)
        for c in range(TILES):
            following = tile_logits(blk, (c + 1) * TILE) if c + 1 < TILES else None
            fold(tile, c * TILE, target, stat)
            tile = following
        end(blk)
        return carry

    lax.fori_loop(1, N, body, 0)
    gather.finish()
    me = at["me"]
    copies = [pltpu.make_async_remote_copy(
        src_ref=mine, dst_ref=theirs.at[shift], send_sem=share_send.at[shift], recv_sem=share_recv.at[shift],
        device_id={"tp": lax.rem(me + shift, N)}, device_id_type=MESH) for shift in range(1, N)]
    for item in copies:
        item.start()
    theirs[0] = mine[...]
    for item in copies:
        item.wait()
    peak = functools.reduce(jnp.maximum, [theirs[i, 0] for i in range(N)])
    total = sum(theirs[i, 1] * jnp.exp((theirs[i, 0] - peak) * (1.0 / LOGIT_DIV)) for i in range(N))
    picked = sum(theirs[i, 2] for i in range(N))
    probs_ref[...] = (picked - peak) * (1.0 / LOGIT_DIV) - jnp.log(total)


def head(f, target, embed, ident):
    return pl.pallas_call(
        head_kernel,
        out_shape=(jax.ShapeDtypeStruct((N, ROWS), F32), jax.ShapeDtypeStruct((N, SEQS, D), BF16)),
        in_specs=[VM, VM, ANY], out_specs=(VM, VM),
        scratch_shapes=gather_scratch() + [
            pltpu.VMEM((VOCAB, D), BF16), pltpu.VMEM((TILE, ROWS), F32),
            pltpu.VMEM((3, 8, ROWS), F32), pltpu.VMEM((3, N, ROWS), F32), pltpu.VMEM((N, 3, N, ROWS), F32),
            pltpu.SemaphoreType.DMA((N,)), pltpu.SemaphoreType.DMA((N,)), pltpu.SemaphoreType.DMA((TILES,))],
        compiler_params=comm_params(ident),
    )(f, target, embed)


LAST_STEPS = VOCAB // LAST_TILE
PLANES = LAYERS * 2 * BATCH // LAST_STEPS
RING = 8
AHEAD = 4


def last_kernel(f_ref, embed_ref, cache_ref, logits_ref, new_ref, ring, in_sem, out_sem):
    c = pl.program_id(0)

    def load(i):
        slot = lax.rem(i, RING)
        return pltpu.make_async_copy(cache_ref.at[pl.ds(i * PLANES, PLANES)], ring.at[slot], in_sem.at[slot])

    def store(i):
        slot = lax.rem(i, RING)
        return pltpu.make_async_copy(ring.at[slot], new_ref.at[pl.ds(i * PLANES, PLANES)], out_sem.at[slot])

    @pl.when(c == 0)
    def _():
        for i in range(AHEAD):
            load(jnp.int32(i)).start()

    @pl.when((c >= RING - AHEAD) & (c < LAST_STEPS - AHEAD))
    def _():
        store(c + AHEAD - RING).wait()

    @pl.when(c < LAST_STEPS - AHEAD)
    def _():
        load(c + AHEAD).start()

    load(c).wait()
    store(c).start()
    logits_ref[...] = lax.dot_general(f_ref[...], embed_ref[...], (((1,), (1,)), ((), ())),
                                      preferred_element_type=F32) * (1.0 / LOGIT_DIV)

    @pl.when(c == LAST_STEPS - 1)
    def _():
        for i in range(LAST_STEPS - RING, LAST_STEPS):
            store(jnp.int32(i)).wait()


def last_step(f, embed, cache):
    flat = cache.reshape(LAYERS * 2 * BATCH, HEAD, CACHE)
    logits, flat = pl.pallas_call(
        last_kernel,
        out_shape=(jax.ShapeDtypeStruct((BATCH, VOCAB), F32), jax.ShapeDtypeStruct(flat.shape, BF16)),
        grid=(LAST_STEPS,),
        in_specs=[pl.BlockSpec((BATCH, D), lambda c: (0, 0)), pl.BlockSpec((LAST_TILE, D), lambda c: (c, 0)), ANY],
        out_specs=(pl.BlockSpec((BATCH, LAST_TILE), lambda c: (0, c)), ANY),
        scratch_shapes=[pltpu.VMEM((RING, PLANES, HEAD, CACHE), BF16), pltpu.SemaphoreType.DMA((RING,)),
                        pltpu.SemaphoreType.DMA((RING,))],
        compiler_params=pltpu.CompilerParams(dimension_semantics=("arbitrary",), vmem_limit_bytes=VMEM_LIMIT),
    )(f, embed, flat)
    return logits, flat.reshape(cache.shape)


def by_block(values):
    return values.reshape(N, SEQS, values.shape[1]).transpose(0, 2, 1)


def solution(mesh):
    cache_spec = P(None, None, 'dp', None, 'tp', None)
    expert_spec = P(None, 'tp', None, None)
    in_specs = (P('dp', None), P('dp'), cache_spec, P(None, None, 'dp', None), P('tp', None), P(None, None), P(None, None, 'tp'), P(None, None, 'tp'), P(None, None, 'tp'), P(None, 'tp', None), P(None, None, None), expert_spec, expert_spec, expert_spec)
    out_specs = (P('dp', None), P('dp', 'tp'), cache_spec)

    def decode_local(tokens, start_pos, kv_cache, expert_ids, embed, norm_gain, w_query, w_key, w_value, w_out, w_router, w_gate, w_up, w_down):
        shard = lax.axis_index('tp')
        cache = kv_cache.transpose(0, 1, 2, 4, 5, 3).reshape(LAYERS, 2, BATCH, HEAD, CACHE)

        ids = by_block(tokens[:, :STEPS]).reshape(N, ROWS)
        hidden, normed = embed_tokens(ids, shard, embed, norm_gain)

        inv_freq = ROPE_THETA ** (-2.0 * jnp.arange(HEAD // 2, dtype=F32) / HEAD)
        angles = jnp.arange(CACHE, dtype=F32)[:, None] * jnp.tile(inv_freq, 4)
        sign = jnp.where(jnp.arange(128) % HEAD < HEAD // 2, -1.0, 1.0)
        table = jnp.concatenate([jnp.cos(angles), jnp.sin(angles) * sign], axis=1)
        start_wide = jnp.broadcast_to(start_pos[:, None], (BATCH, 128))

        weights = [w.transpose(0, 2, 1) for w in (w_query, w_key, w_value)] + [w_out]
        router = w_router.transpose(0, 2, 1)
        routed = expert_ids.reshape(STEPS, LAYERS, N, SEQS, 8).transpose(1, 2, 0, 3, 4).reshape(LAYERS, N, ROWS, 8)

        new_cache = None
        for layer in range(LAYERS):
            hidden, normed, new_cache = attention(layer, normed, table, start_wide, hidden, norm_gain, weights, cache, new_cache,
                                                  1 + 2 * layer)
            hidden, normed = experts(layer, normed, router, routed[layer], hidden, norm_gain, w_gate, w_up, w_down, 2 + 2 * layer)

        target = by_block(tokens[:, 1:] - shard * VOCAB).reshape(N, 1, ROWS)
        log_probs, f_last = head(normed, target, embed, 5)
        logits, new_cache = last_step(f_last.reshape(BATCH, D), embed, new_cache)
        log_probs = log_probs.reshape(N, STEPS, SEQS).transpose(0, 2, 1).reshape(BATCH, STEPS)
        new_cache = new_cache.reshape(LAYERS, 2, BATCH, 1, HEAD, CACHE).transpose(0, 1, 2, 5, 3, 4)
        return log_probs, logits, new_cache

    return jax.shard_map(decode_local, mesh=mesh, in_specs=in_specs, out_specs=out_specs, check_vma=False)
```
